128 devices in a mesh: dp: 32 (over x, z, y_hi), mp: 4 (over y_lo, core).
Axes of the slice: x: 4, y: 4 (y_hi: 2, y_lo: 2; y = y_hi * 2 + y_lo), z: 4, core: 2. Of those that a mesh axis runs over, the one named last changes fastest.
Arguments:
- initial_state: int32 [2048], P('dp'), may hold values from 0 to 255
- actions: int32 [2048, 16], P('dp'), may hold values from 0 to 15
- next_state: int32 [256, 16], replicated, may hold values from 0 to 255
- reward_table: float32 [256, 16], replicated, may hold values from -6 to 6
- reward_scale: float32 [2048], P('dp'), may hold values from 0.5 to 4.5
- observe_table: bfloat16 [256, 1024], replicated, may hold values from -6 to 6
- gain_attn: float32 [1024], replicated, may hold values from 0.5 to 1.5
- w_query: bfloat16 [1024, 1024], P(None, 'mp'), may hold values from -0.1875 to 0.1875
- w_key: bfloat16 [1024, 1024], P(None, 'mp'), may hold values from -0.1875 to 0.1875
- w_value: bfloat16 [1024, 1024], P(None, 'mp'), may hold values from -0.1875 to 0.1875
- w_out: bfloat16 [1024, 1024], P('mp'), may hold values from -0.1875 to 0.1875
- gain_mlp: float32 [1024], replicated, may hold values from 0.5 to 1.5
- w_up: bfloat16 [1024, 4096], P(None, 'mp'), may hold values from -0.1875 to 0.1875
- w_down: bfloat16 [4096, 1024], P('mp'), may hold values from -0.09375 to 0.09375
- gain_final: float32 [1024], replicated, may hold values from 0.5 to 1.5
- actor_head: bfloat16 [1024, 16], replicated, may hold values from -0.1875 to 0.1875
- critic_head: bfloat16 [1024], replicated, may hold values from -0.1875 to 0.1875
Outputs:
- grad_query: float32 [1024, 1024], P('dp', 'mp')
- grad_key: float32 [1024, 1024], P('dp', 'mp')
- grad_value: float32 [1024, 1024], P('dp', 'mp')
- grad_out: float32 [1024, 1024], P('mp', 'dp')
- grad_up: float32 [1024, 4096], P('dp', 'mp')
- grad_down: float32 [4096, 1024], P('mp', 'dp')
- grad_gain_attn: float32 [1024], P(('dp', 'mp'))
- grad_gain_mlp: float32 [1024], P('dp')
- grad_gain_final: float32 [1024], P('dp')
- grad_actor: float32 [1024, 16], P('dp')
- grad_critic: float32 [1024], P('dp')
The draws below stay inside these ranges and needn't reach their ends.
All inputs are finite; a program needn't handle non-finite values.
Results may differ from the reference program's by a relative error of at most 0.015.
Values sent between devices are 32-bit elements; how exact they have to be, the bound alone decides.
A program may use at most 128 MiB of HBM per device.

```python
import math
import jax
import jax.numpy as jnp
from jax import lax

D = 1024
FF = 4096
HEAD_DIM = 128
STATES = 256
ACTIONS = 16
STEPS = 16
ENVS = 2048


def draw_reward_scale(key, part):
    ramp = jnp.exp(jnp.log(3.0) * jnp.arange(ENVS, dtype=jnp.float32) / ENVS)
    rough = jax.random.uniform(key, (ENVS,), jnp.float32, 0.5, 1.5)
    return ramp * rough


def plant(drawn, key, low, top_value):
    dims = drawn.shape
    index_at = [jax.random.randint(jax.random.fold_in(key, axis), (), 0, dims[axis]) for axis in range(len(dims))]
    drawn = drawn.at[tuple(index_at)].set(low)
    longest = dims.index(max(dims))
    index_at[longest] = (index_at[longest] + 1) % dims[longest]
    return drawn.at[tuple(index_at)].set(top_value)


def level_of(own_key, shape, pieces, smallest, largest):
    factor_of = 1.0
    for position, blocks in pieces:
        steps = jax.random.uniform(jax.random.fold_in(jax.random.fold_in(own_key, 6), position), (blocks,), jnp.float32, smallest / len(pieces), largest / len(pieces))
        factor_of = factor_of * jnp.repeat(jnp.exp(steps), shape[position] // blocks).reshape((-1,) + (1,) * (len(shape) - 1 - position))
    return factor_of


def normal_values(key, extent, width, reach, pieces=(), kind=jnp.bfloat16):
    factor_of = level_of(key, extent, pieces, -0.22, 0.18) if pieces else 1.0
    result = jax.random.normal(key, extent, jnp.float32) * width * factor_of
    return jnp.minimum(jnp.maximum(result, -reach), reach).astype(kind)


def setup_inputs(seed: int = 0) -> dict:
    streams_of = jax.random.split(jax.random.key(seed), 18)
    return {
        "initial_state": plant(jax.random.randint(streams_of[0], (ENVS,), 0, STATES), jax.random.fold_in(streams_of[0], 1), 0, STATES - 1).astype(jnp.int32),
        "actions": plant(jax.random.randint(streams_of[1], (ENVS, STEPS), 0, ACTIONS), jax.random.fold_in(streams_of[1], 1), 0, ACTIONS - 1).astype(jnp.int32),
        "next_state": plant(jax.random.randint(streams_of[2], (STATES, ACTIONS), 0, STATES), jax.random.fold_in(streams_of[2], 1), 0, STATES - 1).astype(jnp.int32),
        "reward_table": normal_values(streams_of[3], (STATES, ACTIONS), 1.0, 6.0, (), jnp.float32),
        "reward_scale": draw_reward_scale(jax.random.fold_in(streams_of[17], 71), 0),
        "observe_table": normal_values(streams_of[5], (STATES, D), 1.0, 6.0),
        "gain_attn": jnp.clip(1.0 + 0.1 * jax.random.normal(streams_of[6], (D,), jnp.float32), 0.5, 1.5),
        "w_query": normal_values(streams_of[7], (D, D), D ** -0.5, 0.1875, ((1, 4),)),
        "w_key": normal_values(streams_of[8], (D, D), D ** -0.5, 0.1875, ((1, 4),)),
        "w_value": normal_values(streams_of[9], (D, D), D ** -0.5, 0.1875, ((1, 4),)),
        "w_out": normal_values(streams_of[10], (D, D), D ** -0.5, 0.1875, ((0, 4),)),
        "gain_mlp": jnp.clip(1.0 + 0.1 * jax.random.normal(streams_of[11], (D,), jnp.float32), 0.5, 1.5),
        "w_up": normal_values(streams_of[12], (D, FF), D ** -0.5, 0.1875, ((1, 4),)),
        "w_down": normal_values(streams_of[13], (FF, D), FF ** -0.5, 0.09375, ((0, 4),)),
        "gain_final": jnp.clip(1.0 + 0.1 * jax.random.normal(streams_of[14], (D,), jnp.float32), 0.5, 1.5),
        "actor_head": normal_values(streams_of[15], (D, ACTIONS), D ** -0.5, 0.1875),
        "critic_head": normal_values(streams_of[16], (D,), D ** -0.5, 0.1875),
    }


EPS = 1e-05
GAMMA = 0.9
VALUE_COEF = 0.5
ENTROPY_COEF = 0.1

def roll_states(initial_state, actions, next_state):
    flat_table = next_state.reshape(-1)
    table_width = next_state.shape[1]
    cell_ids = jnp.arange(flat_table.shape[0], dtype=jnp.int32)

    def advance(current, action):
        flat_index = (current * table_width + action).astype(jnp.int32)
        chosen = lax.optimization_barrier(jnp.sum(jnp.where(flat_index[:, None] == cell_ids[None, :], flat_table[None, :], 0), axis=1))
        return (chosen.astype(jnp.int32), current)
    unused, visited = lax.scan(advance, initial_state.astype(jnp.int32), jnp.transpose(actions))
    return jnp.transpose(visited)

def state_tables(states, actions, reward_table, reward_scale, observe_table):
    state_count = reward_table.shape[0]
    state_match = states.reshape(-1)[:, None] == jnp.arange(state_count, dtype=jnp.int32)[None, :]
    reward_rows = jnp.dot(state_match.astype(jnp.float32), reward_table, precision=lax.Precision.HIGHEST, preferred_element_type=jnp.float32)
    chosen = actions.reshape(-1)[:, None] == jnp.arange(reward_table.shape[1], dtype=jnp.int32)[None, :]
    rewards = lax.optimization_barrier(jnp.sum(jnp.where(chosen, reward_rows, 0.0), axis=1)).reshape(states.shape) * reward_scale[:, None]
    embedded = jnp.dot(state_match.astype(jnp.bfloat16), observe_table, preferred_element_type=jnp.float32)
    return (rewards, embedded)

def normalize(inputs, gain):
    inverse_rms = lax.rsqrt(lax.optimization_barrier(jnp.mean(inputs * inputs, axis=-1, keepdims=True)) + EPS)
    return (inputs * inverse_rms * gain, inverse_rms)

def norm_back(inputs, inverse_rms, gain, upstream):
    weighted = upstream * gain
    return inverse_rms * weighted - inputs * inverse_rms ** 3 * lax.optimization_barrier(jnp.mean(inputs * weighted, axis=-1, keepdims=True))

def discount(rewards, critic_grid):

    def backward_step(running, reward):
        running = reward + GAMMA * running
        return (running, running)
    unused, totals = lax.scan(backward_step, critic_grid[:, -1], jnp.transpose(rewards), reverse=True)
    return jnp.transpose(totals)

def policy_terms(logits, critic_out, returns, normed, actions, factor):
    logp = logits - jnp.log(lax.optimization_barrier(jnp.sum(jnp.exp(logits), axis=1, keepdims=True)))
    chance = jnp.exp(logp)
    entropy = -lax.optimization_barrier(jnp.sum(chance * logp, axis=1, keepdims=True))
    picked = (actions.reshape(-1)[:, None] == jnp.arange(logits.shape[1], dtype=jnp.int32)[None, :]).astype(jnp.float32)
    d_logits = factor * (-normed.reshape(-1)[:, None] * (picked - chance) + ENTROPY_COEF * chance * (logp + entropy))
    d_value = factor * VALUE_COEF * (critic_out - returns.reshape(-1))
    return (d_logits.astype(jnp.bfloat16), d_value.astype(jnp.bfloat16))

def product(left, right):
    return jnp.dot(left, right, preferred_element_type=jnp.float32)

def across(left, right):
    return jnp.dot(left.T, right, preferred_element_type=jnp.float32)

def heads_view(rows_array):
    return rows_array.reshape(rows_array.shape[0] // STEPS, STEPS, -1, HEAD_DIM).astype(jnp.float32)

def attend(queries, key_rows, value_rows):
    q_heads, k_heads, v_heads = (heads_view(queries), heads_view(key_rows), heads_view(value_rows))
    scores = jnp.einsum('eqhd,ekhd->ehqk', q_heads, k_heads) / math.sqrt(HEAD_DIM)
    causal = jnp.arange(STEPS)[:, None] >= jnp.arange(STEPS)[None, :]
    weights = jnp.where(causal, jnp.exp(scores), 0.0)
    attn_probs = weights / lax.optimization_barrier(jnp.sum(weights, axis=-1, keepdims=True))
    probs_low = attn_probs.astype(jnp.bfloat16)
    mixed_rows = jnp.einsum('ehqk,ekhd->eqhd', probs_low.astype(jnp.float32), v_heads)
    return (mixed_rows.astype(jnp.bfloat16).reshape(queries.shape), attn_probs, probs_low)

def attend_back(queries, key_rows, value_rows, attn_probs, probs_low, d_mixed):
    q_heads, k_heads, v_heads = (heads_view(queries), heads_view(key_rows), heads_view(value_rows))
    d_heads = heads_view(d_mixed)
    d_probs = jnp.einsum('eqhd,ekhd->ehqk', d_heads, v_heads)
    d_values = jnp.einsum('ehqk,eqhd->ekhd', probs_low.astype(jnp.float32), d_heads).astype(jnp.bfloat16)
    d_scores = (attn_probs * (d_probs - lax.optimization_barrier(jnp.sum(attn_probs * d_probs, axis=-1, keepdims=True))) / math.sqrt(HEAD_DIM)).astype(jnp.bfloat16)
    d_queries = jnp.einsum('ehqk,ekhd->eqhd', d_scores.astype(jnp.float32), k_heads).astype(jnp.bfloat16)
    d_keys = jnp.einsum('ehqk,eqhd->ekhd', d_scores.astype(jnp.float32), q_heads).astype(jnp.bfloat16)
    return (d_queries.reshape(queries.shape), d_keys.reshape(queries.shape), d_values.reshape(queries.shape))

def reference(initial_state, actions, next_state, reward_table, reward_scale, observe_table, gain_attn, w_query, w_key, w_value, w_out, gain_mlp, w_up, w_down, gain_final, actor_head, critic_head):
    states = roll_states(initial_state, actions, next_state)
    rewards, x_zero = state_tables(states, actions, reward_table, reward_scale, observe_table)
    h_one, n_one = normalize(x_zero, gain_attn)
    h_one = h_one.astype(jnp.bfloat16)
    queries = product(h_one, w_query).astype(jnp.bfloat16)
    key_rows = product(h_one, w_key).astype(jnp.bfloat16)
    value_rows = product(h_one, w_value).astype(jnp.bfloat16)
    mixed_rows, attn_probs, probs_low = attend(queries, key_rows, value_rows)
    x_one = x_zero + product(mixed_rows, w_out)
    h_two, n_two = normalize(x_one, gain_mlp)
    h_two = h_two.astype(jnp.bfloat16)
    up_rows = product(h_two, w_up)
    hidden = jax.nn.silu(up_rows).astype(jnp.bfloat16)
    x_two = x_one + product(hidden, w_down)
    final_rows, n_fin = normalize(x_two, gain_final)
    final_rows = final_rows.astype(jnp.bfloat16)
    logits = product(final_rows, actor_head)
    critic_out = jnp.dot(final_rows, critic_head, preferred_element_type=jnp.float32)
    env_count = actions.shape[0]
    critic_grid = critic_out.reshape(env_count, STEPS)
    returns = discount(rewards, critic_grid)
    advantage = returns - critic_grid
    token_total = advantage.size
    adv_mean = jnp.sum(advantage) / token_total
    spread = jnp.sum((advantage - adv_mean) ** 2) / token_total
    normed = (advantage - adv_mean) * lax.rsqrt(spread + EPS)
    d_logits, d_value = policy_terms(logits, critic_out, returns, normed, actions, 1.0 / math.sqrt(token_total))
    grad_actor = across(final_rows, d_logits)
    grad_critic = jnp.dot(d_value, final_rows, preferred_element_type=jnp.float32)
    d_final = product(d_logits, actor_head.T) + d_value[:, None].astype(jnp.float32) * critic_head.astype(jnp.float32)[None, :]
    grad_final = lax.optimization_barrier(jnp.sum(d_final * x_two * n_fin, axis=0))
    dx_two = norm_back(x_two, n_fin, gain_final, d_final)
    dx_two_low = dx_two.astype(jnp.bfloat16)
    grad_down = across(hidden, dx_two_low)
    d_hidden = product(dx_two_low, w_down.T).astype(jnp.bfloat16)
    sigmoid_up = jax.nn.sigmoid(up_rows)
    d_up = (d_hidden.astype(jnp.float32) * sigmoid_up * (1.0 + up_rows * (1.0 - sigmoid_up))).astype(jnp.bfloat16)
    grad_up = across(h_two, d_up)
    d_h_two = product(d_up, w_up.T)
    grad_mlp = lax.optimization_barrier(jnp.sum(d_h_two * x_one * n_two, axis=0))
    dx_one = dx_two + norm_back(x_one, n_two, gain_mlp, d_h_two)
    dx_one_low = dx_one.astype(jnp.bfloat16)
    grad_out = across(mixed_rows, dx_one_low)
    d_mixed = product(dx_one_low, w_out.T).astype(jnp.bfloat16)
    d_queries, d_keys, d_values = attend_back(queries, key_rows, value_rows, attn_probs, probs_low, d_mixed)
    grad_query = across(h_one, d_queries)
    grad_key = across(h_one, d_keys)
    grad_value = across(h_one, d_values)
    d_h_one = product(d_queries, w_query.T) + product(d_keys, w_key.T) + product(d_values, w_value.T)
    grad_attn = lax.optimization_barrier(jnp.sum(d_h_one * x_zero * n_one, axis=0))
    return (grad_query, grad_key, grad_value, grad_out, grad_up, grad_down, grad_attn, grad_mlp, grad_final, grad_actor, grad_critic)
```

```python
import functools
import math

import jax
import jax.numpy as jnp
from jax import lax
from jax.experimental import pallas as pl
from jax.experimental.pallas import tpu as pltpu
from jax.sharding import PartitionSpec as P

HEAD_DIM = 128
STEPS = 16
EPS = 1e-05
GAMMA = 0.9
VALUE_COEF = 0.5
ENTROPY_COEF = 0.1
MESH = pl.DeviceIdType.MESH
VMEM = pl.BlockSpec(memory_space=pltpu.VMEM)
F32 = jnp.float32
BF16 = jnp.bfloat16


def place():
    d, m = lax.axis_index("dp"), lax.axis_index("mp")
    return d, m, m % 2, m // 2


def partners():
    d, m, c, l = place()
    over = m + 2 - 4 * l
    return (d, m + 1 - 2 * c), (d, over), (d + 1 - 2 * (d % 2), over)


def greet(devices):
    barrier = pltpu.get_barrier_semaphore()
    for dev in devices:
        pl.semaphore_signal(barrier, inc=1, device_id=dev, device_id_type=MESH)
    pl.semaphore_wait(barrier, len(devices))


def remote(src, dst, send, recv, dev):
    return pltpu.make_async_remote_copy(
        src_ref=src, dst_ref=dst, send_sem=send, recv_sem=recv, device_id=dev, device_id_type=MESH
    )


def rows(start, size):
    return pl.ds(pl.multiple_of(start, size), size)


def by_blocks(total, block, body):
    lax.fori_loop(0, total // block, lambda i, z: (body(pl.multiple_of(i * block, block)), z)[1], 0)


def part_sums(p_ref, near, far, near_s, near_r, far_s, far_r, finish):
    d, m, c, l = place()
    core, *over = partners()
    step = 128
    first = []
    for k in range(2):
        blk = (1 - l) if k == 0 else l
        for h in range(2):
            cp = remote(
                p_ref.at[rows(h * 512 + (1 - c) * 256 + blk * step, step)],
                near.at[h, k], near_s.at[h, k], near_r.at[h, k], core,
            )
            cp.start()
            first.append(cp)

    def add_mine(h, k, blk):
        base = h * 512 + c * 256 + blk * step

        def body(i):
            near[h, k, pl.ds(i, 32), :] += p_ref[rows(base + i, 32), :]

        by_blocks(step, 32, body)

    second = []
    for h in range(2):
        first[h].wait_recv()
        add_mine(h, 0, 1 - l)
        cp = remote(near.at[h, 0], far.at[h], far_s.at[h], far_r.at[h], over[h])
        cp.start()
        second.append(cp)
    for h in range(2):
        first[2 + h].wait_recv()
        add_mine(h, 1, l)
    for h in range(2):
        second[h].wait_recv()
        finish(h)
    for cp in first + second:
        cp.wait_send()


def part_gather(q_ref, whole, out_ref, over_s, over_r, core_s, core_r):
    d, m, c, l = place()
    core, *over = partners()
    sent, incoming = [], []
    mine = [h * 512 + c * 256 + l * 128 for h in range(2)]
    yours = [h * 512 + c * 256 + (1 - l) * 128 for h in range(2)]
    for k in range(2):
        for h in range(2):
            cp = remote(
                q_ref.at[pl.ds(h * 128 + k * 64, 64)], whole.at[rows(mine[h] + k * 64, 64)],
                over_s.at[h, k], over_r.at[h, k], over[h],
            )
            cp.start()
            incoming.append((h, k, cp))
    for h in range(2):
        cp = remote(
            q_ref.at[pl.ds(h * 128, 128)], whole.at[rows(mine[h], 128)],
            core_s.at[h, 2], core_r.at[h, 2], core,
        )
        cp.start()
        sent.append(cp)

    def keep(base, size, src=None, at=0):
        def body(i):
            value = whole[rows(base + i, 32), :] if src is None else src[pl.ds(at + i, 32), :]
            out_ref[rows(base + i, 32), :] = value.astype(BF16)

        by_blocks(size, 32, body)

    for h in range(2):
        keep(mine[h], 128, q_ref, h * 128)
    for h in range(2):
        sent[h].wait_recv()
        keep(h * 512 + (1 - c) * 256 + l * 128, 128)
    for h, k, cp in incoming:
        cp.wait_recv()
        at = rows(yours[h] + k * 64, 64)
        fwd = remote(whole.at[at], whole.at[at], core_s.at[h, k], core_r.at[h, k], core)
        fwd.start()
        sent.append(fwd)
        keep(yours[h] + k * 64, 64)
    for n, (h, k, cp) in enumerate(incoming):
        sent[2 + n].wait_recv()
        keep(h * 512 + (1 - c) * 256 + (1 - l) * 128 + k * 64, 64)
    for cp in sent + [cp for _, _, cp in incoming]:
        cp.wait_send()


SUM_SCRATCH = [
    pltpu.VMEM((2, 2, 128, 1024), F32),
    pltpu.VMEM((2, 128, 1024), F32),
    pltpu.SemaphoreType.DMA((2, 2)),
    pltpu.SemaphoreType.DMA((2, 2)),
    pltpu.SemaphoreType.DMA((2,)),
    pltpu.SemaphoreType.DMA((2,)),
]
GATHER_SCRATCH = [
    pltpu.VMEM((1024, 1024), F32),
    pltpu.SemaphoreType.DMA((2, 2)),
    pltpu.SemaphoreType.DMA((2, 2)),
    pltpu.SemaphoreType.DMA((2, 3)),
    pltpu.SemaphoreType.DMA((2, 3)),
]


def params(n):
    return pltpu.CompilerParams(
        collective_id=n, has_side_effects=True, vmem_limit_bytes=60 * 1024 * 1024
    )


def attn_out_kernel(p_ref, xz_ref, gain_ref, x_ref, h_ref, near, far, *rest):
    sems, q_ref, gather = rest[:4], rest[4], rest[5:]
    greet(partners())

    def finish(h):
        def body(i):
            at = pl.ds(h * 128 + i, 32)
            x = near[h, 1, pl.ds(i, 32), :] + far[h, pl.ds(i, 32), :] + xz_ref[at, :]
            x_ref[at, :] = x
            inv = lax.rsqrt(jnp.mean(x * x, axis=-1, keepdims=True) + EPS)
            q_ref[at, :] = x * inv * gain_ref[...]

        by_blocks(128, 32, body)

    part_sums(p_ref, near, far, *sems, finish)
    part_gather(q_ref, gather[0], h_ref, *gather[1:])


def attn_out(partial, xz, gain):
    return pl.pallas_call(
        attn_out_kernel,
        out_shape=(jax.ShapeDtypeStruct((256, 1024), F32), jax.ShapeDtypeStruct((1024, 1024), BF16)),
        in_specs=[VMEM] * 3,
        out_specs=(VMEM, VMEM),
        scratch_shapes=[*SUM_SCRATCH, pltpu.VMEM((256, 1024), F32), *GATHER_SCRATCH],
        compiler_params=params(1),
        name="attn_out",
    )(partial, xz, gain.reshape(1, -1))


def mlp_out_kernel(p_ref, x_ref, o_ref, near, far, *sems):
    greet(partners())

    def finish(h):
        def body(i):
            at = pl.ds(h * 128 + i, 32)
            o_ref[at, :] = near[h, 1, pl.ds(i, 32), :] + far[h, pl.ds(i, 32), :] + x_ref[at, :]

        by_blocks(128, 32, body)

    part_sums(p_ref, near, far, *sems, finish)


def mlp_out(partial, x_one):
    return pl.pallas_call(
        mlp_out_kernel,
        out_shape=jax.ShapeDtypeStruct((256, 1024), F32),
        in_specs=[VMEM] * 2,
        out_specs=VMEM,
        scratch_shapes=SUM_SCRATCH,
        compiler_params=params(2),
        name="mlp_out",
    )(partial, x_one)


def gather_kernel(q_ref, o_ref, *rest):
    greet(partners())
    part_gather(q_ref, rest[0], o_ref, *rest[1:])


def gather_rows(own):
    return pl.pallas_call(
        gather_kernel,
        out_shape=jax.ShapeDtypeStruct((1024, 1024), BF16),
        in_specs=[VMEM],
        out_specs=VMEM,
        scratch_shapes=GATHER_SCRATCH,
        compiler_params=params(3),
        name="gather_rows",
    )(own)


def mlp_in_back_kernel(p_ref, x_ref, dx_ref, gain_ref, o_ref, g_ref, near, far, *rest):
    sems, q_ref, gather = rest[:4], rest[4], rest[5:]
    greet(partners())
    g_ref[...] = jnp.zeros_like(g_ref)

    def finish(h):
        def body(i):
            at = pl.ds(h * 128 + i, 32)
            up = near[h, 1, pl.ds(i, 32), :] + far[h, pl.ds(i, 32), :]
            x = x_ref[at, :]
            inv = lax.rsqrt(jnp.mean(x * x, axis=-1, keepdims=True) + EPS)
            weighted = up * gain_ref[...]
            back = inv * weighted - x * (inv * inv * inv) * jnp.mean(
                x * weighted, axis=-1, keepdims=True
            )
            q_ref[at, :] = dx_ref[at, :] + back
            term = up * x * inv
            g_ref[...] += term[0:8] + term[8:16] + term[16:24] + term[24:32]

        by_blocks(128, 32, body)

    part_sums(p_ref, near, far, *sems, finish)
    part_gather(q_ref, gather[0], o_ref, *gather[1:])


def mlp_in_back(partial, x_one, dx_two, gain):
    return pl.pallas_call(
        mlp_in_back_kernel,
        out_shape=(jax.ShapeDtypeStruct((1024, 1024), BF16), jax.ShapeDtypeStruct((8, 1024), F32)),
        in_specs=[VMEM] * 4,
        out_specs=(VMEM, VMEM),
        scratch_shapes=[*SUM_SCRATCH, pltpu.VMEM((256, 1024), F32), *GATHER_SCRATCH],
        compiler_params=params(4),
        name="mlp_in_back",
    )(partial, x_one, dx_two, gain.reshape(1, -1))


def axes_place():
    d, m, c, l = place()
    return d // 8, (d // 2) % 4, d % 2


def stats_kernel(t_ref, o_ref, xs, zs, ys, xsem, zsem, ysem):
    d, m, c, l = place()
    x, z, yh = axes_place()
    xdev = [(lax.rem(x + j, 4) * 8 + z * 2 + yh, m) for j in (1, 2, 3)]
    zdev = [(x * 8 + lax.rem(z + j, 4) * 2 + yh, m) for j in (1, 2, 3)]
    mine = yh * 4 + m
    ydev = []
    for j in range(1, 8):
        other = lax.rem(mine + j, 8)
        ydev.append((x * 8 + z * 2 + other // 4, other % 4))
    greet(xdev + zdev + ydev)

    def stage(slots, sems, devs, me, value):
        n = len(devs)
        slots[me] = value
        copies = []
        for j, dev in enumerate(devs):
            cp = remote(slots.at[me], slots.at[me], sems.at[0, j], sems.at[1, j], dev)
            cp.start()
            copies.append(cp)
        for cp in copies:
            cp.wait_recv()
        total = slots[0]
        for k in range(1, n + 1):
            total = total + slots[k]
        for cp in copies:
            cp.wait_send()
        return total

    value = stage(xs, xsem, xdev, x, t_ref[...])
    value = stage(zs, zsem, zdev, z, value)
    o_ref[...] = stage(ys, ysem, ydev, mine, value)


def stats_sum(tile):
    return pl.pallas_call(
        stats_kernel,
        out_shape=jax.ShapeDtypeStruct((8, 128), F32),
        in_specs=[VMEM],
        out_specs=VMEM,
        scratch_shapes=[
            pltpu.VMEM((4, 8, 128), F32),
            pltpu.VMEM((4, 8, 128), F32),
            pltpu.VMEM((8, 8, 128), F32),
            pltpu.SemaphoreType.DMA((2, 3)),
            pltpu.SemaphoreType.DMA((2, 3)),
            pltpu.SemaphoreType.DMA((2, 7)),
        ],
        compiler_params=params(5),
        name="stats_sum",
    )(tile)


class Ring:
    def __init__(self, src, bufs, sems, pos, right, left):
        self.src, self.pos, self.right, self.left = src, pos, right, left
        self.mid, self.fl, self.fr = bufs
        self.sems = sems
        self.copies = []

    def send(self, k, src, dst, dev):
        cp = remote(src, dst, self.sems.at[0, k], self.sems.at[1, k], dev)
        cp.start()
        self.copies.append(cp)

    def start(self):
        p = self.pos
        self.r, self.l, opp = lax.rem(p + 1, 4), lax.rem(p + 3, 4), lax.rem(p + 2, 4)
        self.send(0, self.src(opp, 0), self.mid.at[0], self.right)
        self.send(1, self.src(opp, 1), self.mid.at[1], self.left)
        self.send(2, self.src(self.r, 1), self.fl.at[1], self.right)
        self.send(3, self.src(self.l, 0), self.fr.at[0], self.left)

    def middle(self):
        self.copies[0].wait_recv()
        add_into(self.mid.at[0], self.src(self.r, 0))
        self.send(4, self.mid.at[0], self.fl.at[0], self.right)
        self.copies[1].wait_recv()
        add_into(self.mid.at[1], self.src(self.l, 1))
        self.send(5, self.mid.at[1], self.fr.at[1], self.left)

    def finish(self, out):
        for k in (2, 3, 4, 5):
            self.copies[k].wait_recv()
        for half in range(2):
            add_three(out(half), self.src(self.pos, half), self.fl.at[half], self.fr.at[half])

    def drain(self):
        for cp in self.copies:
            cp.wait_send()


def each_block(ref, body):
    if len(ref.shape) == 3:
        for k in range(ref.shape[0]):
            by_blocks(ref.shape[1], 8, lambda i, k=k: body((k, pl.ds(i, 8), slice(None))))
    else:
        by_blocks(ref.shape[0], 8, lambda i: body((pl.ds(i, 8), slice(None))))


def add_into(dst, src):
    def body(at):
        dst[at] += src[at]

    each_block(dst, body)


def add_three(dst, a, b, c):
    def body(at):
        dst[at] = a[at] + b[at] + c[at]

    each_block(dst, body)


def grads_kernel(orders, *refs):
    n = len(orders)
    ins, outs = refs[:n], refs[n : 2 * n]
    scratch = refs[2 * n :]
    mp_buf, mp_sem = scratch[-2:]
    d, m, c, l = place()
    x, z, yh = axes_place()

    def at_x(k):
        return (lax.rem(x + k, 4) * 8 + z * 2 + yh, m)

    def at_z(k):
        return (x * 8 + lax.rem(z + k, 4) * 2 + yh, m)

    yother = (d + 1 - 2 * yh, m)
    peers = [(d, lax.rem(m + j, 4)) for j in (1, 2, 3)]
    greet([at_x(1), at_x(3), at_z(1), at_z(3), yother] + peers)

    first, second, last = [], [], []
    for i, order in enumerate(orders):
        r1m, r1l, r1r, res1, r2m, r2l, r2r, res2, ybuf, sems1, sems2, sems3 = scratch[12 * i : 12 * i + 12]
        src = ins[i]
        if order == "xz":
            ring1 = Ring(lambda j, h, s=src: s.at[j, pl.ds(h * 2, 2)], (r1m, r1l, r1r), sems1, x, at_x(1), at_x(3))
            pos2, right2, left2 = z, at_z(1), at_z(3)
        else:
            ring1 = Ring(lambda j, h, s=src: s.at[pl.ds(h * 2, 2), j], (r1m, r1l, r1r), sems1, z, at_z(1), at_z(3))
            pos2, right2, left2 = x, at_x(1), at_x(3)
        ring2 = Ring(lambda j, h, s=res1: s.at[j, pl.ds(h * 32, 32)], (r2m, r2l, r2r), sems2, pos2, right2, left2)
        first.append((ring1, res1))
        second.append((ring2, res2))
        last.append((res2, ybuf, sems3))
    for ring, _ in first:
        ring.start()
    for ring, _ in first:
        ring.middle()
    for i in range(n):
        ring, res = first[i]
        ring.finish(lambda h, s=res: s.at[pl.ds(h * 2, 2)])
        second[i][0].start()
    for i in range(n):
        second[i][0].middle()
    tails = []
    for i in range(n):
        ring, res = second[i]
        ring.finish(lambda h, s=res: s.at[pl.ds(h * 32, 32)])
        res2, ybuf, sems3 = last[i]
        cp = remote(res2.at[rows((1 - yh) * 32, 32)], ybuf, sems3.at[0], sems3.at[1], yother)
        cp.start()
        tails.append(cp)
    for i in reversed(range(n)):
        tails[i].wait_recv()
        res2, ybuf, _ = last[i]

        def body(k, res2=res2, ybuf=ybuf, i=i):
            value = res2[rows(yh * 32 + k, 8), :] + ybuf[pl.ds(k, 8), :]
            if i == n - 1:
                mp_buf[m, pl.ds(k, 8), :] = value
            else:
                outs[i][pl.ds(k, 8), :] = value

        by_blocks(32, 8, body)
        if i == n - 1:
            shares = []
            for j, dev in enumerate(peers):
                cp = remote(mp_buf.at[m], mp_buf.at[m], mp_sem.at[0, j], mp_sem.at[1, j], dev)
                cp.start()
                shares.append(cp)
    for cp in shares:
        cp.wait_recv()
    outs[n - 1][...] = mp_buf[0] + mp_buf[1] + mp_buf[2] + mp_buf[3]
    for cp in shares + tails:
        cp.wait_send()
    for ring, _ in first + second:
        ring.drain()


def reduce_grads(arrays, orders):
    scratch = []
    for a in arrays:
        w = a.shape[1]
        scratch += [
            pltpu.VMEM((2, 2, 64, w), F32),
            pltpu.VMEM((2, 2, 64, w), F32),
            pltpu.VMEM((2, 2, 64, w), F32),
            pltpu.VMEM((4, 64, w), F32),
            pltpu.VMEM((2, 32, w), F32),
            pltpu.VMEM((2, 32, w), F32),
            pltpu.VMEM((2, 32, w), F32),
            pltpu.VMEM((64, w), F32),
            pltpu.VMEM((32, w), F32),
            pltpu.SemaphoreType.DMA((2, 6)),
            pltpu.SemaphoreType.DMA((2, 6)),
            pltpu.SemaphoreType.DMA((2,)),
        ]
    scratch += [pltpu.VMEM((4, 32, arrays[-1].shape[1]), F32), pltpu.SemaphoreType.DMA((2, 3))]
    return pl.pallas_call(
        functools.partial(grads_kernel, orders),
        out_shape=tuple(jax.ShapeDtypeStruct((32, a.shape[1]), F32) for a in arrays),
        in_specs=[VMEM] * len(arrays),
        out_specs=tuple([VMEM] * len(arrays)),
        scratch_shapes=scratch,
        compiler_params=params(6),
        name="reduce_grads",
    )(*[a.reshape(4, 4, 64, a.shape[1]) for a in arrays])


def roll_states(initial_state, actions, next_state):
    flat_table = next_state.reshape(-1)
    table_width = next_state.shape[1]
    cell_ids = jnp.arange(flat_table.shape[0], dtype=jnp.int32)

    def advance(current, action):
        flat_index = current * table_width + action
        chosen = jnp.sum(
            jnp.where(flat_index[:, None] == cell_ids[None, :], flat_table[None, :], 0), axis=1
        )
        return (chosen, current)

    unused, visited = lax.scan(advance, initial_state, jnp.transpose(actions))
    return jnp.transpose(visited)


def one_hot(ids, count, dtype):
    return (ids.reshape(-1)[:, None] == jnp.arange(count, dtype=jnp.int32)[None, :]).astype(dtype)


def reward_rows(states, actions, reward_table, reward_scale):
    found = jnp.dot(
        one_hot(states, reward_table.shape[0], F32),
        reward_table,
        precision=lax.Precision.HIGHEST,
        preferred_element_type=F32,
    )
    chosen = one_hot(actions, reward_table.shape[1], jnp.bool_)
    return jnp.sum(jnp.where(chosen, found, 0.0), axis=1).reshape(states.shape) * reward_scale[:, None]


def inverse_rms(inputs):
    return lax.rsqrt(jnp.mean(inputs * inputs, axis=-1, keepdims=True) + EPS)


def norm_back(inputs, inv, gain, upstream):
    weighted = upstream * gain
    return inv * weighted - inputs * inv**3 * jnp.mean(inputs * weighted, axis=-1, keepdims=True)


def discount(rewards, critic_grid):
    def backward_step(running, reward):
        running = reward + GAMMA * running
        return (running, running)

    unused, totals = lax.scan(
        backward_step, critic_grid[:, -1], jnp.transpose(rewards), reverse=True
    )
    return jnp.transpose(totals)


def policy_terms(logits, critic_out, returns, normed, actions, factor):
    logp = logits - jnp.log(jnp.sum(jnp.exp(logits), axis=1, keepdims=True))
    chance = jnp.exp(logp)
    entropy = -jnp.sum(chance * logp, axis=1, keepdims=True)
    picked = one_hot(actions, logits.shape[1], F32)
    d_logits = factor * (
        -normed.reshape(-1)[:, None] * (picked - chance) + ENTROPY_COEF * chance * (logp + entropy)
    )
    d_value = factor * VALUE_COEF * (critic_out - returns.reshape(-1))
    return (d_logits.astype(BF16), d_value.astype(BF16))


def product(left, right):
    return jnp.dot(left, right, preferred_element_type=F32)


def across(left, right):
    return jnp.dot(left.T, right, preferred_element_type=F32)


def heads_view(rows_array):
    return rows_array.reshape(rows_array.shape[0] // STEPS, STEPS, -1, HEAD_DIM)


def attend(queries, key_rows, value_rows):
    q_heads, k_heads, v_heads = (heads_view(queries), heads_view(key_rows), heads_view(value_rows))
    scores = jnp.einsum(
        "eqhd,ekhd->ehqk", q_heads, k_heads, preferred_element_type=F32
    ) / math.sqrt(HEAD_DIM)
    causal = jnp.arange(STEPS)[:, None] >= jnp.arange(STEPS)[None, :]
    weights = jnp.where(causal, jnp.exp(scores), 0.0)
    attn_probs = weights / jnp.sum(weights, axis=-1, keepdims=True)
    probs_low = attn_probs.astype(BF16)
    mixed_rows = jnp.einsum("ehqk,ekhd->eqhd", probs_low, v_heads, preferred_element_type=F32)
    return (mixed_rows.astype(BF16).reshape(queries.shape), attn_probs, probs_low)


def attend_back(queries, key_rows, value_rows, attn_probs, probs_low, d_mixed):
    q_heads, k_heads, v_heads = (heads_view(queries), heads_view(key_rows), heads_view(value_rows))
    d_heads = heads_view(d_mixed)
    d_probs = jnp.einsum("eqhd,ekhd->ehqk", d_heads, v_heads, preferred_element_type=F32)
    d_values = jnp.einsum("ehqk,eqhd->ekhd", probs_low, d_heads, preferred_element_type=F32).astype(BF16)
    d_scores = (
        attn_probs
        * (d_probs - jnp.sum(attn_probs * d_probs, axis=-1, keepdims=True))
        / math.sqrt(HEAD_DIM)
    ).astype(BF16)
    d_queries = jnp.einsum("ehqk,ekhd->eqhd", d_scores, k_heads, preferred_element_type=F32).astype(BF16)
    d_keys = jnp.einsum("ehqk,eqhd->ekhd", d_scores, q_heads, preferred_element_type=F32).astype(BF16)
    return (
        d_queries.reshape(queries.shape),
        d_keys.reshape(queries.shape),
        d_values.reshape(queries.shape),
    )


def shared_inputs(initial_state, actions, reward_scale):
    half = actions.shape[0] // 2
    packed = jnp.concatenate(
        [
            initial_state[half:, None].astype(F32),
            actions[half:].astype(F32),
            reward_scale[half:, None],
        ],
        axis=1,
    )
    dp, mp = lax.axis_size("dp"), lax.axis_size("mp")
    pairs = [(d * mp + m, (d ^ 1) * mp + m - 2) for d in range(dp) for m in (2, 3)]
    moved = lax.ppermute(packed, ("dp", "mp"), pairs)
    other = jnp.where(lax.axis_index("mp") < 2, moved, packed)
    return (
        jnp.concatenate([initial_state[:half], other[:, 0].astype(jnp.int32)]),
        jnp.concatenate([actions[:half], other[:, 1 : STEPS + 1].astype(jnp.int32)]),
        jnp.concatenate([reward_scale[:half], other[:, STEPS + 1]]),
    )


def owned(array, size):
    m = lax.axis_index("mp")
    at = ((m % 2) * 2 + m // 2) * size
    half = array.shape[0] // 2
    return jnp.concatenate(
        [lax.dynamic_slice_in_dim(array, h * half + at, size, 0) for h in range(2)]
    )


def per_device(
    initial_state,
    actions,
    next_state,
    reward_table,
    reward_scale,
    observe_table,
    gain_attn,
    w_query,
    w_key,
    w_value,
    w_out,
    gain_mlp,
    w_up,
    w_down,
    gain_final,
    actor_head,
    critic_head,
):
    token_total = actions.size * lax.axis_size("dp")
    initial_state, actions, reward_scale = shared_inputs(initial_state, actions, reward_scale)
    states = roll_states(initial_state, actions, next_state)

    table = observe_table.astype(F32)
    n_table = inverse_rms(table)
    h_table = (table * n_table * gain_attn).astype(BF16)
    q_table = product(h_table, w_query).astype(BF16)
    k_table = product(h_table, w_key).astype(BF16)
    v_table = product(h_table, w_value).astype(BF16)
    match = one_hot(states, table.shape[0], BF16)
    queries = product(match, q_table).astype(BF16)
    key_rows = product(match, k_table).astype(BF16)
    value_rows = product(match, v_table).astype(BF16)
    mixed_rows, attn_probs, probs_low = attend(queries, key_rows, value_rows)

    own_states, own_actions, own_scale = owned(states, 8), owned(actions, 8), owned(reward_scale, 8)
    own_zero = product(one_hot(own_states, table.shape[0], BF16), observe_table)
    x_one, h_two = attn_out(product(mixed_rows, w_out), own_zero, gain_mlp)
    up_rows = product(h_two, w_up)
    hidden = jax.nn.silu(up_rows).astype(BF16)
    x_two = mlp_out(product(hidden, w_down), x_one)

    n_fin = inverse_rms(x_two)
    final_rows = (x_two * n_fin * gain_final).astype(BF16)
    heads = jnp.concatenate(
        [actor_head, critic_head[:, None], jnp.zeros((actor_head.shape[0], 111), BF16)], axis=1
    )
    both = product(final_rows, heads)
    action_count = actor_head.shape[1]
    logits, critic_out = both[:, :action_count], both[:, action_count]
    rewards = reward_rows(own_states, own_actions, reward_table, own_scale)
    critic_grid = critic_out.reshape(rewards.shape)
    returns = discount(rewards, critic_grid)
    advantage = returns - critic_grid
    row = jnp.arange(8)[:, None]
    tile = jnp.where(row == 0, jnp.sum(advantage), jnp.sum(advantage * advantage))
    totals = stats_sum(jnp.broadcast_to(tile, (8, 128)))
    adv_mean = totals[0, 0] / token_total
    spread = totals[1, 0] / token_total - adv_mean * adv_mean
    normed = (advantage - adv_mean) * lax.rsqrt(spread + EPS)
    d_logits, d_value = policy_terms(
        logits, critic_out, returns, normed, own_actions, 1.0 / math.sqrt(token_total)
    )
    d_both = jnp.concatenate(
        [d_logits, d_value[:, None], jnp.zeros((d_value.shape[0], 111), BF16)], axis=1
    )
    grad_heads = across(final_rows, d_both)
    d_final = product(d_both, heads.T)
    grad_final = jnp.sum(d_final * x_two * n_fin, axis=0)
    dx_two = norm_back(x_two, n_fin, gain_final, d_final)
    dx_two_low = gather_rows(dx_two)

    grad_down = across(dx_two_low, hidden)
    d_hidden = jnp.dot(dx_two_low, w_down.T, preferred_element_type=F32).astype(BF16)
    sigmoid_up = jax.nn.sigmoid(up_rows)
    d_up = (
        d_hidden.astype(F32) * sigmoid_up * (1.0 + up_rows * (1.0 - sigmoid_up))
    ).astype(BF16)
    grad_up = across(h_two, d_up)
    dx_one_low, mlp_terms = mlp_in_back(product(d_up, w_up.T), x_one, dx_two, gain_mlp)

    grad_out = across(dx_one_low, mixed_rows)
    d_mixed = product(dx_one_low, w_out.T).astype(BF16)
    d_queries, d_keys, d_values = attend_back(
        queries, key_rows, value_rows, attn_probs, probs_low, d_mixed
    )
    h_one = product(match, h_table).astype(BF16)
    grad_qk = across(h_one, jnp.concatenate([d_queries, d_keys], axis=1))
    grad_value = across(h_one, d_values)
    q_sum, k_sum, v_sum = across(match, d_queries), across(match, d_keys), across(match, d_values)

    def back_sum(total, w):
        return jnp.dot(
            total, w.T.astype(F32), precision=lax.Precision.HIGHEST, preferred_element_type=F32
        )

    d_table = back_sum(q_sum, w_query) + back_sum(k_sum, w_key) + back_sum(v_sum, w_value)
    attn_term = jnp.sum(d_table * table * n_table, axis=0)

    vectors = jnp.stack([jnp.sum(mlp_terms, axis=0), grad_final, attn_term], axis=1)
    small = jnp.concatenate([grad_heads[:, : action_count + 1], vectors, jnp.zeros((1024, 108), F32)], axis=1)
    up_part, qk_part, down_part, out_part, value_part, small_part = reduce_grads(
        (grad_up, grad_qk, grad_down, grad_out, grad_value, small),
        ("xz", "xz", "zx", "zx", "zx", "xz"),
    )
    wide = w_query.shape[1]
    attn_total = lax.dynamic_slice_in_dim(
        small_part[:, action_count + 3], lax.axis_index("mp") * 8, 8, 0
    )
    return (
        qk_part[:, :wide],
        qk_part[:, wide:],
        value_part,
        out_part.T,
        up_part,
        down_part.T,
        attn_total,
        small_part[:, action_count + 1],
        small_part[:, action_count + 2],
        small_part[:, :action_count],
        small_part[:, action_count],
    )


def solution(mesh):
    return jax.shard_map(
        per_device,
        mesh=mesh,
        in_specs=(
            P("dp"),
            P("dp", None),
            P(),
            P(),
            P("dp"),
            P(),
            P(),
            P(None, "mp"),
            P(None, "mp"),
            P(None, "mp"),
            P("mp", None),
            P(),
            P(None, "mp"),
            P("mp", None),
            P(),
            P(),
            P(),
        ),
        out_specs=(
            P("dp", "mp"),
            P("dp", "mp"),
            P("dp", "mp"),
            P("mp", "dp"),
            P("dp", "mp"),
            P("mp", "dp"),
            P(("dp", "mp")),
            P("dp"),
            P("dp"),
            P("dp", None),
            P("dp"),
        ),
        check_vma=False,
    )
```

```python
import functools
import math

import jax
import jax.numpy as jnp
from jax import lax
from jax.experimental import pallas as pl
from jax.experimental.pallas import tpu as pltpu
from jax.sharding import PartitionSpec as P

HEAD_DIM = 128
STEPS = 16
EPS = 1e-05
GAMMA = 0.9
VALUE_COEF = 0.5
ENTROPY_COEF = 0.1
MESH = pl.DeviceIdType.MESH
VMEM = pl.BlockSpec(memory_space=pltpu.VMEM)
F32 = jnp.float32
BF16 = jnp.bfloat16


def place():
    d, m = lax.axis_index("dp"), lax.axis_index("mp")
    return d, m, m % 2, m // 2


def partners():
    d, m, c, l = place()
    over = m + 2 - 4 * l
    return (d, m + 1 - 2 * c), (d, over), (d + 1 - 2 * (d % 2), over)


def greet(devices):
    barrier = pltpu.get_barrier_semaphore()
    for dev in devices:
        pl.semaphore_signal(barrier, inc=1, device_id=dev, device_id_type=MESH)
    pl.semaphore_wait(barrier, len(devices))


def remote(src, dst, send, recv, dev):
    return pltpu.make_async_remote_copy(
        src_ref=src, dst_ref=dst, send_sem=send, recv_sem=recv, device_id=dev, device_id_type=MESH
    )


def rows(start, size):
    return pl.ds(pl.multiple_of(start, size), size)


def by_blocks(total, block, body):
    lax.fori_loop(0, total // block, lambda i, z: (body(pl.multiple_of(i * block, block)), z)[1], 0)


def part_sums(p_ref, near, far, near_s, near_r, far_s, far_r, finish):
    d, m, c, l = place()
    core, *over = partners()
    step = 128
    first = []
    for k in range(2):
        blk = (1 - l) if k == 0 else l
        for h in range(2):
            cp = remote(
                p_ref.at[rows(h * 512 + (1 - c) * 256 + blk * step, step)],
                near.at[h, k], near_s.at[h, k], near_r.at[h, k], core,
            )
            cp.start()
            first.append(cp)

    def add_mine(h, k, blk):
        base = h * 512 + c * 256 + blk * step

        def body(i):
            near[h, k, pl.ds(i, 32), :] += p_ref[rows(base + i, 32), :]

        by_blocks(step, 32, body)

    second = []
    for h in range(2):
        first[h].wait_recv()
        add_mine(h, 0, 1 - l)
        cp = remote(near.at[h, 0], far.at[h], far_s.at[h], far_r.at[h], over[h])
        cp.start()
        second.append(cp)
    for h in range(2):
        first[2 + h].wait_recv()
        add_mine(h, 1, l)
    for h in range(2):
        second[h].wait_recv()
        finish(h)
    for cp in first + second:
        cp.wait_send()


def part_gather(q_ref, whole, out_ref, over_s, over_r, core_s, core_r, between=None):
    d, m, c, l = place()
    core, *over = partners()
    sent, incoming = [], []
    mine = [h * 512 + c * 256 + l * 128 for h in range(2)]
    yours = [h * 512 + c * 256 + (1 - l) * 128 for h in range(2)]
    for k in range(2):
        for h in range(2):
            cp = remote(
                q_ref.at[pl.ds(h * 128 + k * 64, 64)], whole.at[rows(mine[h] + k * 64, 64)],
                over_s.at[h, k], over_r.at[h, k], over[h],
            )
            cp.start()
            incoming.append((h, k, cp))
    for h in range(2):
        cp = remote(
            q_ref.at[pl.ds(h * 128, 128)], whole.at[rows(mine[h], 128)],
            core_s.at[h, 2], core_r.at[h, 2], core,
        )
        cp.start()
        sent.append(cp)

    def keep(base, size, src=None, at=0):
        def body(i):
            value = whole[rows(base + i, 32), :] if src is None else src[pl.ds(at + i, 32), :]
            out_ref[rows(base + i, 32), :] = value.astype(BF16)

        by_blocks(size, 32, body)

    for h in range(2):
        keep(mine[h], 128, q_ref, h * 128)
    for h in range(2):
        sent[h].wait_recv()
        keep(h * 512 + (1 - c) * 256 + l * 128, 128)
    if between is not None:
        between()
    for h, k, cp in incoming:
        cp.wait_recv()
        at = rows(yours[h] + k * 64, 64)
        fwd = remote(whole.at[at], whole.at[at], core_s.at[h, k], core_r.at[h, k], core)
        fwd.start()
        sent.append(fwd)
        keep(yours[h] + k * 64, 64)
    for n, (h, k, cp) in enumerate(incoming):
        sent[2 + n].wait_recv()
        keep(h * 512 + (1 - c) * 256 + (1 - l) * 128 + k * 64, 64)
    for cp in sent + [cp for _, _, cp in incoming]:
        cp.wait_send()


SUM_SCRATCH = [
    pltpu.VMEM((2, 2, 128, 1024), F32),
    pltpu.VMEM((2, 128, 1024), F32),
    pltpu.SemaphoreType.DMA((2, 2)),
    pltpu.SemaphoreType.DMA((2, 2)),
    pltpu.SemaphoreType.DMA((2,)),
    pltpu.SemaphoreType.DMA((2,)),
]
GATHER_SCRATCH = [
    pltpu.VMEM((1024, 1024), F32),
    pltpu.SemaphoreType.DMA((2, 2)),
    pltpu.SemaphoreType.DMA((2, 2)),
    pltpu.SemaphoreType.DMA((2, 3)),
    pltpu.SemaphoreType.DMA((2, 3)),
]


def params(n):
    return pltpu.CompilerParams(
        collective_id=n, has_side_effects=True, vmem_limit_bytes=60 * 1024 * 1024
    )


def attn_out_kernel(p_ref, xz_ref, gain_ref, x_ref, h_ref, near, far, *rest):
    sems, q_ref, gather = rest[:4], rest[4], rest[5:]
    greet(partners())

    def finish(h):
        def body(i):
            at = pl.ds(h * 128 + i, 32)
            x = near[h, 1, pl.ds(i, 32), :] + far[h, pl.ds(i, 32), :] + xz_ref[at, :]
            x_ref[at, :] = x
            inv = lax.rsqrt(jnp.mean(x * x, axis=-1, keepdims=True) + EPS)
            q_ref[at, :] = x * inv * gain_ref[...]

        by_blocks(128, 32, body)

    part_sums(p_ref, near, far, *sems, finish)
    part_gather(q_ref, gather[0], h_ref, *gather[1:])


def attn_out(partial, xz, gain):
    return pl.pallas_call(
        attn_out_kernel,
        out_shape=(jax.ShapeDtypeStruct((256, 1024), F32), jax.ShapeDtypeStruct((1024, 1024), BF16)),
        in_specs=[VMEM] * 3,
        out_specs=(VMEM, VMEM),
        scratch_shapes=[*SUM_SCRATCH, pltpu.VMEM((256, 1024), F32), *GATHER_SCRATCH],
        compiler_params=params(1),
        name="attn_out",
    )(partial, xz, gain.reshape(1, -1))


SCALE = 1.0 / math.sqrt(HEAD_DIM)


def dot(left, right, contract, **kw):
    return lax.dot_general(
        left, right, ((contract[:1], contract[1:]), ((), ())), preferred_element_type=F32, **kw
    )


def iota(shape, axis):
    return lax.broadcasted_iota(jnp.int32, shape, axis)


def block_probs(q, k):
    r, s = iota((128, 128), 0), iota((128, 128), 1)
    seen = ((r // STEPS) == (s // STEPS)) & (r >= s)
    weights = jnp.where(seen, jnp.exp(dot(q, k, (1, 1)) * SCALE), 0.0)
    return weights / jnp.sum(weights, axis=-1, keepdims=True)


def front_kernel(
    init_ref, act_ref, scale_ref, next_ref, rew_ref, obs_ref, gain_ref, wq_ref, wk_ref, wv_ref, wo_ref,
    p_ref, xz_ref, qkv_ref, match_ref, mixed_ref, ht_ref, own_ref,
    r_init, r_act, r_scale, tables, st_ref, sems,
):
    d, m, c, l = place()
    far = partners()[2]
    greet([far])
    copies = []
    for n, (src, dst) in enumerate(((init_ref, r_init), (act_ref, r_act), (scale_ref, r_scale))):
        cp = remote(src, dst, sems.at[0, n], sems.at[1, n], far)
        cp.start()
        copies.append(cp)

    def table_rows(i):
        at = pl.ds(i, 32)
        x = obs_ref[at, :].astype(F32)
        inv = lax.rsqrt(jnp.mean(x * x, axis=-1, keepdims=True) + EPS)
        ht_ref[at, :] = (x * inv * gain_ref[...]).astype(BF16)

    by_blocks(256, 32, table_rows)
    for n, w in enumerate((wq_ref, wk_ref, wv_ref)):
        tables[:, n * 256 : (n + 1) * 256] = dot(ht_ref[...], w[...], (1, 0)).astype(BF16)

    for cp in copies:
        cp.wait()
    swap = 32 + 64 * (1 - jnp.where(l == 0, 1, 0))
    lane = iota((1, 64), 1)
    state = jnp.where(lane >= swap, r_init[...], init_ref[...]).astype(F32)
    scale = jnp.where(lane >= swap, r_scale[...], scale_ref[...])
    act = jnp.where(iota((64, 16), 0) >= swap, r_act[...], act_ref[...]).astype(F32)
    eye = (iota((64, 64), 0) == iota((64, 64), 1)).astype(BF16)
    act_t = dot(act.astype(BF16), eye, (0, 0))
    nexts = next_ref[...].astype(F32).astype(BF16)
    ids, kinds = iota((256, 64), 0).astype(F32), iota((16, 64), 0).astype(F32)
    for t in range(STEPS):
        st_ref[pl.ds(t, 1), :] = state
        if t + 1 < STEPS:
            hit = jnp.where(ids == state, 1.0, 0.0).astype(BF16)
            found = dot(nexts, hit, (0, 0))
            state = jnp.sum(jnp.where(kinds == act_t[t : t + 1, :], found, 0.0), axis=0, keepdims=True)

    pick_t = (iota((128, 16), 0) % STEPS == iota((128, 16), 1)).astype(BF16)
    spread = jnp.ones((64, 128), BF16)
    lanes = iota((128, 128), 1).astype(F32)

    def per_token(rows_by_env, first_env):
        here = iota((128, 64), 1) == first_env + iota((128, 64), 0) // STEPS
        mixed = jnp.where(here, dot(pick_t, rows_by_env, (1, 0)), 0.0)
        return dot(mixed.astype(BF16), spread, (1, 0))

    def block(b, carry):
        at = rows(b * 128, 128)
        ids_here = per_token(st_ref[...].astype(BF16), b * 8)
        match = jnp.concatenate(
            [jnp.where(ids_here == lanes, 1.0, 0.0), jnp.where(ids_here == lanes + 128.0, 1.0, 0.0)], axis=1
        ).astype(BF16)
        match_ref[at, :] = match
        qkv = dot(match, tables[...], (1, 0)).astype(BF16)
        qkv_ref[at, :] = qkv
        heads = []
        for h in range(2):
            q, k, v = (qkv[:, n * 256 + h * 128 : n * 256 + (h + 1) * 128] for n in range(3))
            heads.append(dot(block_probs(q, k).astype(BF16), v, (1, 0)).astype(BF16))
        mixed = jnp.concatenate(heads, axis=1)
        mixed_ref[at, :] = mixed
        p_ref[at, :] = dot(mixed, wo_ref[...], (1, 0))
        return carry

    lax.fori_loop(0, 8, block, 0)

    for h in range(2):
        q = c * 2 + l
        at = pl.ds(h * 128, 128)
        mine = match_ref[rows(h * 512 + q * 128, 128), :]
        xz_ref[at, :] = dot(mine, obs_ref[...], (1, 0))
        first_env = h * 32 + q * 8
        acts = per_token(act_t.astype(BF16), first_env)
        chosen = jnp.where(acts == lanes, 1.0, 0.0)
        found = dot(mine.astype(F32), rew_ref[...], (1, 0), precision=lax.Precision.HIGHEST)
        here = iota((128, 64), 1) == first_env + iota((128, 64), 0) // STEPS
        factor = jnp.sum(jnp.where(here, scale, 0.0), axis=1, keepdims=True)
        reward = jnp.sum(chosen[:, :16] * found, axis=1, keepdims=True) * factor
        own_ref[at, :] = jnp.where(lanes == 16.0, reward, chosen)


def front(initial_state, actions, reward_scale, next_state, reward_table, observe_table, gain, wq, wk, wv, wo):
    sd = jax.ShapeDtypeStruct
    return pl.pallas_call(
        front_kernel,
        out_shape=(
            sd((1024, 1024), F32), sd((256, 1024), F32), sd((1024, 768), BF16), sd((1024, 256), BF16),
            sd((1024, 256), BF16), sd((256, 1024), BF16), sd((256, 128), F32),
        ),
        in_specs=[VMEM] * 11,
        out_specs=tuple([VMEM] * 7),
        scratch_shapes=[
            pltpu.VMEM((1, 64), jnp.int32), pltpu.VMEM((64, 16), jnp.int32), pltpu.VMEM((1, 64), F32),
            pltpu.VMEM((256, 768), BF16), pltpu.VMEM((16, 64), F32), pltpu.SemaphoreType.DMA((2, 3)),
        ],
        compiler_params=params(7),
        name="front",
    )(
        initial_state.reshape(1, -1), actions, reward_scale.reshape(1, -1), next_state, reward_table,
        observe_table, gain.reshape(1, -1), wq, wk, wv, wo,
    )


def axes_place():
    d, m, c, l = place()
    return d // 8, (d // 2) % 4, d % 2


def stats_devices():
    d, m, c, l = place()
    x, z, yh = axes_place()
    xdev = [(lax.rem(x + j, 4) * 8 + z * 2 + yh, m) for j in (1, 2, 3)]
    zdev = [(x * 8 + lax.rem(z + j, 4) * 2 + yh, m) for j in (1, 2, 3)]
    mine = yh * 4 + m
    ydev = []
    for j in range(1, 8):
        other = lax.rem(mine + j, 8)
        ydev.append((x * 8 + z * 2 + other // 4, other % 4))
    return xdev, zdev, ydev


def sum_everywhere(value, xs, zs, ys, xsem, zsem, ysem):
    d, m, c, l = place()
    x, z, yh = axes_place()
    xdev, zdev, ydev = stats_devices()

    def stage(slots, sems, devs, me, value):
        slots[me] = value
        copies = []
        for j, dev in enumerate(devs):
            cp = remote(slots.at[me], slots.at[me], sems.at[0, j], sems.at[1, j], dev)
            cp.start()
            copies.append(cp)
        for cp in copies:
            cp.wait_recv()
        total = slots[0]
        for k in range(1, len(devs) + 1):
            total = total + slots[k]
        for cp in copies:
            cp.wait_send()
        return total

    value = stage(xs, xsem, xdev, x, value)
    value = stage(zs, zsem, zdev, z, value)
    return stage(ys, ysem, ydev, yh * 4 + m, value)


STATS_SCRATCH = [
    pltpu.VMEM((4, 8, 128), F32),
    pltpu.VMEM((4, 8, 128), F32),
    pltpu.VMEM((8, 8, 128), F32),
    pltpu.SemaphoreType.DMA((2, 3)),
    pltpu.SemaphoreType.DMA((2, 3)),
    pltpu.SemaphoreType.DMA((2, 7)),
]


def fold8(term):
    total = term[0:8]
    for k in range(1, term.shape[0] // 8):
        total = total + term[8 * k : 8 * k + 8]
    return total


def loss_kernel(
    token_total, p_ref, x_ref, own_ref, heads_ref, gain_ref,
    dx_ref, low_ref, gh_ref, g_ref,
    near, far, s0, s1, s2, s3, xs, zs, ys, xsem, zsem, ysem, x2_ref, fin_ref, df_ref, *gather,
):
    xdev, zdev, ydev = stats_devices()
    greet(xdev + zdev + ydev)

    def finish(h):
        def body(i):
            at = pl.ds(h * 128 + i, 32)
            x = near[h, 1, pl.ds(i, 32), :] + far[h, pl.ds(i, 32), :] + x_ref[at, :]
            x2_ref[at, :] = x
            inv = lax.rsqrt(jnp.mean(x * x, axis=-1, keepdims=True) + EPS)
            fin_ref[at, :] = (x * inv * gain_ref[...]).astype(BF16)

        by_blocks(128, 32, body)

    part_sums(p_ref, near, far, s0, s1, s2, s3, finish)

    lane = iota((256, 128), 1)
    both = dot(fin_ref[...], heads_ref[...], (1, 0))
    critic = jnp.sum(jnp.where(lane == 16, both, 0.0), axis=1, keepdims=True)
    own = own_ref[...]
    reward = jnp.sum(jnp.where(lane == 16, own, 0.0), axis=1, keepdims=True)
    step = iota((256, 128), 0) % STEPS
    base = reward + jnp.where(step == STEPS - 1, GAMMA * critic, 0.0)
    r, s = iota((256, 256), 0), iota((256, 256), 1)
    ahead = ((r // STEPS) == (s // STEPS)) & (s >= r)
    decay = jnp.where(ahead, jnp.exp((s - r).astype(F32) * math.log(GAMMA)), 0.0)
    returns = dot(decay, base, (1, 0), precision=lax.Precision.HIGHEST)
    advantage = returns - critic
    sums = jnp.sum(advantage, axis=0, keepdims=True)
    squares = jnp.sum(advantage * advantage, axis=0, keepdims=True)
    tile = jnp.where(iota((8, 128), 0) == 0, sums, squares)
    totals = sum_everywhere(tile, xs, zs, ys, xsem, zsem, ysem)
    mean = totals[0:1, :] * (1.0 / token_total)
    spread = totals[1:2, :] * (1.0 / token_total) - mean * mean
    normed = (advantage - mean) * lax.rsqrt(spread + EPS)

    real = lane < 16
    logits = jnp.where(real, both, 0.0)
    mass = jnp.sum(jnp.where(real, jnp.exp(logits), 0.0), axis=1, keepdims=True)
    logp = jnp.where(real, logits - jnp.log(mass), 0.0)
    chance = jnp.where(real, jnp.exp(logp), 0.0)
    entropy = -jnp.sum(chance * logp, axis=1, keepdims=True)
    factor = 1.0 / math.sqrt(token_total)
    picked = jnp.where(real, own, 0.0)
    d_logits = factor * (-normed * (picked - chance) + ENTROPY_COEF * chance * (logp + entropy))
    d_value = (factor * VALUE_COEF) * (critic - returns)
    d_both = jnp.where(real, d_logits, jnp.where(lane == 16, d_value, 0.0)).astype(BF16)
    df_ref[...] = dot(d_both, heads_ref[...], (1, 1))

    g_ref[...] = jnp.zeros_like(g_ref)

    def back(i):
        at = pl.ds(i, 32)
        x, up = x2_ref[at, :], df_ref[at, :]
        inv = lax.rsqrt(jnp.mean(x * x, axis=-1, keepdims=True) + EPS)
        weighted = up * gain_ref[...]
        dx_ref[at, :] = inv * weighted - x * (inv * inv * inv) * jnp.mean(
            x * weighted, axis=-1, keepdims=True
        )
        g_ref[...] += fold8(up * x * inv)

    by_blocks(256, 32, back)
    part_gather(dx_ref, gather[0], low_ref, *gather[1:])
    gh_ref[...] = dot(fin_ref[...], d_both, (0, 0))


def loss(partial, x_one, own, heads, gain, token_total):
    sd = jax.ShapeDtypeStruct
    return pl.pallas_call(
        functools.partial(loss_kernel, token_total),
        out_shape=(sd((256, 1024), F32), sd((1024, 1024), BF16), sd((1024, 128), F32), sd((8, 1024), F32)),
        in_specs=[VMEM] * 5,
        out_specs=tuple([VMEM] * 4),
        scratch_shapes=[
            *SUM_SCRATCH, *STATS_SCRATCH, pltpu.VMEM((256, 1024), F32), pltpu.VMEM((256, 1024), BF16),
            pltpu.VMEM((256, 1024), F32), *GATHER_SCRATCH,
        ],
        compiler_params=params(2),
        name="loss",
    )(partial, x_one, own, heads, gain.reshape(1, -1))


class Ring:
    def __init__(self, src, bufs, sems, pos, right, left):
        self.src, self.pos, self.right, self.left = src, pos, right, left
        self.mid, self.fl, self.fr = bufs
        self.sems = sems
        self.copies = []

    def send(self, k, src, dst, dev):
        cp = remote(src, dst, self.sems.at[0, k], self.sems.at[1, k], dev)
        cp.start()
        self.copies.append(cp)

    def start(self):
        p = self.pos
        self.r, self.l, opp = lax.rem(p + 1, 4), lax.rem(p + 3, 4), lax.rem(p + 2, 4)
        self.send(0, self.src(opp, 0), self.mid.at[0], self.right)
        self.send(1, self.src(opp, 1), self.mid.at[1], self.left)
        self.send(2, self.src(self.r, 1), self.fl.at[1], self.right)
        self.send(3, self.src(self.l, 0), self.fr.at[0], self.left)

    def middle(self):
        self.copies[0].wait_recv()
        add_into(self.mid.at[0], self.src(self.r, 0))
        self.send(4, self.mid.at[0], self.fl.at[0], self.right)
        self.copies[1].wait_recv()
        add_into(self.mid.at[1], self.src(self.l, 1))
        self.send(5, self.mid.at[1], self.fr.at[1], self.left)

    def finish(self, out):
        for k in (2, 3, 4, 5):
            self.copies[k].wait_recv()
        for half in range(2):
            add_three(out(half), self.src(self.pos, half), self.fl.at[half], self.fr.at[half])

    def drain(self):
        for cp in self.copies:
            cp.wait_send()


def each_block(ref, body):
    if len(ref.shape) == 3:
        for k in range(ref.shape[0]):
            by_blocks(ref.shape[1], 8, lambda i, k=k: body((k, pl.ds(i, 8), slice(None))))
    else:
        by_blocks(ref.shape[0], 8, lambda i: body((pl.ds(i, 8), slice(None))))


def add_into(dst, src):
    def body(at):
        dst[at] += src[at]

    each_block(dst, body)


def add_three(dst, a, b, c):
    def body(at):
        dst[at] = a[at] + b[at] + c[at]

    each_block(dst, body)


def ring_one(order, src, bufs, sems):
    d, m, c, l = place()
    x, z, yh = axes_place()
    if order == "xz":
        return Ring(lambda j, h: src.at[j, pl.ds(h * 2, 2)], bufs, sems, x, at_x(1), at_x(3))
    return Ring(lambda j, h: src.at[pl.ds(h * 2, 2), j], bufs, sems, z, at_z(1), at_z(3))


def ring_two(order, res, bufs, sems):
    x, z, yh = axes_place()
    src = lambda j, h: res.at[j, pl.ds(h * 32, 32)]
    if order == "xz":
        return Ring(src, bufs, sems, z, at_z(1), at_z(3))
    return Ring(src, bufs, sems, x, at_x(1), at_x(3))


def at_x(k):
    d, m, c, l = place()
    x, z, yh = axes_place()
    return (lax.rem(x + k, 4) * 8 + z * 2 + yh, m)


def at_z(k):
    d, m, c, l = place()
    x, z, yh = axes_place()
    return (x * 8 + lax.rem(z + k, 4) * 2 + yh, m)


def one_scratch(w):
    return [pltpu.VMEM((2, 2, 64, w), F32)] * 3 + [pltpu.SemaphoreType.DMA((2, 6))]


def two_scratch(w):
    return [
        *[pltpu.VMEM((2, 32, w), F32)] * 3,
        pltpu.VMEM((64, w), F32),
        pltpu.VMEM((32, w), F32),
        pltpu.SemaphoreType.DMA((2, 6)),
        pltpu.SemaphoreType.DMA((2,)),
    ]


def mlp_in_back_kernel(
    p_ref, x_ref, dx_ref, gain_ref, up_ref, down_ref, o_ref, g_ref, up_res, down_res,
    near, far, s0, s1, s2, s3, q_ref, whole, g0, g1, g2, g3, um, ul, ur, us, dm, dl, dr, ds,
):
    greet([*partners(), at_x(1), at_x(3), at_z(1), at_z(3)])
    up_ring = ring_one("xz", up_ref, (um, ul, ur), us)
    down_ring = ring_one("zx", down_ref, (dm, dl, dr), ds)
    up_ring.start()
    down_ring.start()
    g_ref[...] = jnp.zeros_like(g_ref)

    def finish(h):
        def body(i):
            at = pl.ds(h * 128 + i, 32)
            up = near[h, 1, pl.ds(i, 32), :] + far[h, pl.ds(i, 32), :]
            x = x_ref[at, :]
            inv = lax.rsqrt(jnp.mean(x * x, axis=-1, keepdims=True) + EPS)
            weighted = up * gain_ref[...]
            back = inv * weighted - x * (inv * inv * inv) * jnp.mean(
                x * weighted, axis=-1, keepdims=True
            )
            q_ref[at, :] = dx_ref[at, :] + back
            g_ref[...] += fold8(up * x * inv)

        by_blocks(128, 32, body)

    part_sums(p_ref, near, far, s0, s1, s2, s3, finish)

    def between():
        up_ring.middle()
        down_ring.middle()

    part_gather(q_ref, whole, o_ref, g0, g1, g2, g3, between)
    up_ring.finish(lambda h: up_res.at[pl.ds(h * 2, 2)])
    down_ring.finish(lambda h: down_res.at[pl.ds(h * 2, 2)])
    up_ring.drain()
    down_ring.drain()


def mlp_in_back(partial, x_one, dx_two, gain, grad_up, grad_down):
    sd = jax.ShapeDtypeStruct
    return pl.pallas_call(
        mlp_in_back_kernel,
        out_shape=(
            sd((1024, 1024), BF16), sd((8, 1024), F32), sd((4, 64, 1024), F32), sd((4, 64, 1024), F32),
        ),
        in_specs=[VMEM] * 6,
        out_specs=tuple([VMEM] * 4),
        scratch_shapes=[
            *SUM_SCRATCH, pltpu.VMEM((256, 1024), F32), *GATHER_SCRATCH, *one_scratch(1024), *one_scratch(1024),
        ],
        compiler_params=params(4),
        name="mlp_in_back",
    )(
        partial, x_one, dx_two, gain.reshape(1, -1),
        grad_up.reshape(4, 4, 64, 1024), grad_down.reshape(4, 4, 64, 1024),
    )


def halves(value):
    high = value.astype(BF16)
    return high, (value - high.astype(F32)).astype(BF16)


def attend_back_kernel(
    dx_ref, wo_ref, qkv_ref, match_ref, ht_ref, obs_ref, wq_ref, wk_ref, wv_ref, gh_ref, gf_ref, gm_ref,
    qk_ref, v_ref, small_ref, sums, dt_ref, vec_ref,
):
    sums[...] = jnp.zeros_like(sums)

    def block(b, carry):
        at = rows(b * 128, 128)
        d_mixed = dot(dx_ref[at, :], wo_ref[...], (1, 1)).astype(BF16)
        qkv = qkv_ref[at, :]
        parts = [[], [], []]
        for h in range(2):
            q, k, v = (qkv[:, n * 256 + h * 128 : n * 256 + (h + 1) * 128] for n in range(3))
            up = d_mixed[:, h * 128 : (h + 1) * 128]
            probs = block_probs(q, k)
            d_probs = dot(up, v, (1, 1))
            parts[2].append(dot(probs.astype(BF16), up, (0, 0)).astype(BF16))
            d_scores = (
                probs * (d_probs - jnp.sum(probs * d_probs, axis=-1, keepdims=True)) * SCALE
            ).astype(BF16)
            parts[0].append(dot(d_scores, k, (1, 0)).astype(BF16))
            parts[1].append(dot(d_scores, q, (0, 0)).astype(BF16))
        d_qkv = jnp.concatenate([*parts[0], *parts[1], *parts[2]], axis=1)
        sums[...] += dot(match_ref[at, :], d_qkv, (0, 0))
        return carry

    lax.fori_loop(0, 8, block, 0)
    high, low = halves(sums[...])
    for i in range(4):
        cols = pl.ds(i * 256, 256)
        table = ht_ref[:, cols]
        total = dot(table, high, (0, 0)) + dot(table, low, (0, 0))
        qk_ref[cols, :] = total[:, :512]
        v_ref[cols, :] = total[:, 512:]
    dt_ref[...] = jnp.zeros_like(dt_ref)
    for n, w in enumerate((wq_ref, wk_ref, wv_ref)):
        cols = slice(n * 256, (n + 1) * 256)
        dt_ref[...] += dot(high[:, cols], w[...], (1, 1)) + dot(low[:, cols], w[...], (1, 1))
    vec_ref[0:8] = gf_ref[...]
    vec_ref[8:16] = gm_ref[...]
    vec_ref[16:32] = jnp.zeros((16, 1024), F32)

    def gain_rows(i):
        at = pl.ds(i, 32)
        x = obs_ref[at, :].astype(F32)
        inv = lax.rsqrt(jnp.mean(x * x, axis=-1, keepdims=True) + EPS)
        vec_ref[16:24] += fold8(dt_ref[at, :] * x * inv)

    by_blocks(256, 32, gain_rows)
    place_at = (iota((32, 128), 1) == 17 + iota((32, 128), 0) // 8).astype(BF16)
    vec = vec_ref[...]
    high, low = halves(vec)
    lowest = (vec - high.astype(F32) - low.astype(F32)).astype(BF16)
    small_ref[...] = gh_ref[...] + sum(dot(part, place_at, (0, 0)) for part in (high, low, lowest))


def attend_back(*args):
    sd = jax.ShapeDtypeStruct
    return pl.pallas_call(
        attend_back_kernel,
        out_shape=(sd((1024, 512), F32), sd((1024, 256), F32), sd((1024, 128), F32)),
        in_specs=[VMEM] * 12,
        out_specs=tuple([VMEM] * 3),
        scratch_shapes=[pltpu.VMEM((256, 768), F32), pltpu.VMEM((256, 1024), F32), pltpu.VMEM((32, 1024), F32)],
        compiler_params=pltpu.CompilerParams(vmem_limit_bytes=60 * 1024 * 1024),
        name="attend_back",
    )(*args)


FIRST = ("xz", "zx", "zx", "xz")
SECOND = ("xz", "zx") + FIRST


def grads_kernel(*refs):
    ins, outs, scratch = refs[:6], refs[6:12], refs[12:]
    mp_buf, mp_sem = scratch[-2:]
    d, m, c, l = place()
    x, z, yh = axes_place()
    yother = (d + 1 - 2 * yh, m)
    peers = [(d, lax.rem(m + j, 4)) for j in (1, 2, 3)]
    greet([at_x(1), at_x(3), at_z(1), at_z(3), yother] + peers)

    first, second, results = [], [], [ins[0], ins[1]]
    for i, order in enumerate(FIRST):
        mid, fl, fr, sems, res = scratch[5 * i : 5 * i + 5]
        first.append(ring_one(order, ins[2 + i], (mid, fl, fr), sems))
        results.append(res)
    at = 20
    ends = []
    for i, order in enumerate(SECOND):
        mid, fl, fr, res, ybuf, sems, ysem = scratch[at + 7 * i : at + 7 * i + 7]
        second.append(ring_two(order, results[i], (mid, fl, fr), sems))
        ends.append((res, ybuf, ysem))
    tails = []

    def send_tail(i):
        res, ybuf, ysem = ends[i]
        second[i].finish(lambda h: res.at[pl.ds(h * 32, 32)])
        cp = remote(res.at[rows((1 - yh) * 32, 32)], ybuf, ysem.at[0], ysem.at[1], yother)
        cp.start()
        tails.append(cp)

    for ring in first:
        ring.start()
    for ring in second[:2]:
        ring.start()
    for ring in first:
        ring.middle()
    for ring in second[:2]:
        ring.middle()
    for i, ring in enumerate(first):
        res = results[2 + i]
        ring.finish(lambda h, res=res: res.at[pl.ds(h * 2, 2)])
        second[2 + i].start()
    for i in range(2):
        send_tail(i)
    for ring in second[2:]:
        ring.middle()
    for i in (5, 2, 3, 4):
        send_tail(i)

    def total(i, put):
        res, ybuf, _ = ends[i]
        by_blocks(32, 8, lambda k: put(k, res[rows(yh * 32 + k, 8), :] + ybuf[pl.ds(k, 8), :]))

    def to_out(ref):
        def put(k, value):
            ref[pl.ds(k, 8), :] = value

        return put

    def to_mp(k, value):
        mp_buf[m, pl.ds(k, 8), :] = value

    shares = []
    for n, i in enumerate((0, 1, 5, 2, 3, 4)):
        tails[n].wait_recv()
        if i == 5:
            total(i, to_mp)
            for j, dev in enumerate(peers):
                cp = remote(mp_buf.at[m], mp_buf.at[m], mp_sem.at[0, j], mp_sem.at[1, j], dev)
                cp.start()
                shares.append(cp)
        else:
            total(i, to_out(outs[i]))
    for cp in shares:
        cp.wait_recv()
    outs[5][...] = mp_buf[0] + mp_buf[1] + mp_buf[2] + mp_buf[3]
    for cp in shares + tails:
        cp.wait_send()
    for ring in first + second:
        ring.drain()


def reduce_grads(up_res, down_res, qk, value, out, small):
    wide = [1024, 1024, 512, 256, 256, 128]
    scratch = []
    for w in wide[2:]:
        scratch += one_scratch(w) + [pltpu.VMEM((4, 64, w), F32)]
    for w in wide:
        scratch += two_scratch(w)
    scratch += [pltpu.VMEM((4, 32, 128), F32), pltpu.SemaphoreType.DMA((2, 3))]
    return pl.pallas_call(
        grads_kernel,
        out_shape=tuple(jax.ShapeDtypeStruct((32, w), F32) for w in wide),
        in_specs=[VMEM] * 6,
        out_specs=tuple([VMEM] * 6),
        scratch_shapes=scratch,
        compiler_params=params(6),
        name="reduce_grads",
    )(up_res, down_res, *[a.reshape(4, 4, 64, a.shape[1]) for a in (qk, value, out, small)])


def write_kernel(
    up_ref, down_ref, qk_ref, value_ref, out_ref, small_ref,
    o_q, o_k, o_v, o_out, o_up, o_down, o_attn, o_mlp, o_final, o_actor, o_critic,
):
    o_q[...] = qk_ref[:, :256]
    o_k[...] = qk_ref[:, 256:]
    o_v[...] = value_ref[...]
    o_up[...] = up_ref[...]
    o_out[...] = jnp.transpose(out_ref[...])
    o_down[...] = jnp.transpose(down_ref[...])
    o_actor[...] = small_ref[:, :16]
    flat = jnp.transpose(small_ref[...])
    o_critic[...] = flat[16:17, :]
    o_final[...] = flat[17:18, :]
    o_mlp[...] = flat[18:19, :]
    o_attn[...] = flat[19:20, :]


def write_outputs(*parts):
    sd = jax.ShapeDtypeStruct
    return pl.pallas_call(
        write_kernel,
        out_shape=(
            sd((32, 256), F32), sd((32, 256), F32), sd((32, 256), F32), sd((256, 32), F32), sd((32, 1024), F32),
            sd((1024, 32), F32), sd((1, 32), F32), sd((1, 32), F32), sd((1, 32), F32), sd((32, 16), F32),
            sd((1, 32), F32),
        ),
        in_specs=[VMEM] * 6,
        out_specs=tuple([VMEM] * 11),
        name="write_outputs",
    )(*parts)


def product(left, right):
    return jnp.dot(left, right, preferred_element_type=F32)


def across(left, right):
    return jnp.dot(left.T, right, preferred_element_type=F32)


def per_device(
    initial_state,
    actions,
    next_state,
    reward_table,
    reward_scale,
    observe_table,
    gain_attn,
    w_query,
    w_key,
    w_value,
    w_out,
    gain_mlp,
    w_up,
    w_down,
    gain_final,
    actor_head,
    critic_head,
):
    token_total = actions.size * lax.axis_size("dp")
    heads = jnp.concatenate(
        [actor_head, critic_head[:, None], jnp.zeros((actor_head.shape[0], 111), BF16)], axis=1
    )
    partial, own_zero, qkv, match, mixed, h_table, own = front(
        initial_state, actions, reward_scale, next_state, reward_table, observe_table, gain_attn,
        w_query, w_key, w_value, w_out,
    )
    x_one, h_two = attn_out(partial, own_zero, gain_mlp)
    up_rows = product(h_two, w_up)
    hidden = jax.nn.silu(up_rows).astype(BF16)
    dx_two, dx_two_low, grad_heads, final_terms = loss(
        product(hidden, w_down), x_one, own, heads, gain_final, token_total
    )
    grad_down = across(dx_two_low, hidden)
    d_hidden = jnp.dot(dx_two_low, w_down.T, preferred_element_type=F32).astype(BF16)
    sigmoid_up = jax.nn.sigmoid(up_rows)
    d_up = (
        d_hidden.astype(F32) * sigmoid_up * (1.0 + up_rows * (1.0 - sigmoid_up))
    ).astype(BF16)
    grad_up = across(h_two, d_up)
    dx_one_low, mlp_terms, up_res, down_res = mlp_in_back(
        product(d_up, w_up.T), x_one, dx_two, gain_mlp, grad_up, grad_down
    )
    grad_out = across(dx_one_low, mixed)
    grad_qk, grad_value, small = attend_back(
        dx_one_low, w_out, qkv, match, h_table, observe_table, w_query, w_key, w_value,
        grad_heads, final_terms, mlp_terms,
    )
    parts = reduce_grads(up_res, down_res, grad_qk, grad_value, grad_out, small)
    q, k, v, out, up, down, attn, mlp, final, actor, critic = write_outputs(*parts)
    attn_own = lax.dynamic_slice_in_dim(attn.reshape(-1), lax.axis_index("mp") * 8, 8, 0)
    return (
        q, k, v, out, up, down, attn_own, mlp.reshape(-1), final.reshape(-1), actor, critic.reshape(-1),
    )


def solution(mesh):
    return jax.shard_map(
        per_device,
        mesh=mesh,
        in_specs=(
            P("dp"),
            P("dp", None),
            P(),
            P(),
            P("dp"),
            P(),
            P(),
            P(None, "mp"),
            P(None, "mp"),
            P(None, "mp"),
            P("mp", None),
            P(),
            P(None, "mp"),
            P("mp", None),
            P(),
            P(),
            P(),
        ),
        out_specs=(
            P("dp", "mp"),
            P("dp", "mp"),
            P("dp", "mp"),
            P("mp", "dp"),
            P("dp", "mp"),
            P("mp", "dp"),
            P(("dp", "mp")),
            P("dp"),
            P("dp"),
            P("dp", None),
            P("dp"),
        ),
        check_vma=False,
    )
```

```python
import functools
import math

import jax
import jax.numpy as jnp
from jax import lax
from jax.experimental import pallas as pl
from jax.experimental.pallas import tpu as pltpu
from jax.sharding import PartitionSpec as P

HEAD_DIM = 128
STEPS = 16
EPS = 1e-05
GAMMA = 0.9
VALUE_COEF = 0.5
ENTROPY_COEF = 0.1
SCALE = 1.0 / math.sqrt(HEAD_DIM)
MESH = pl.DeviceIdType.MESH
VMEM = pl.BlockSpec(memory_space=pltpu.VMEM)
ANY = pl.BlockSpec(memory_space=pl.ANY)
F32 = jnp.float32
BF16 = jnp.bfloat16


def place():
    d, m = lax.axis_index("dp"), lax.axis_index("mp")
    return d, m, m % 2, m // 2


def axes_place():
    d, m, c, l = place()
    return d // 8, (d // 2) % 4, d % 2


def partners():
    d, m, c, l = place()
    over = m + 2 - 4 * l
    return (d, m + 1 - 2 * c), (d, over), (d + 1 - 2 * (d % 2), over)


def at_x(k):
    d, m, c, l = place()
    x, z, yh = axes_place()
    return (lax.rem(x + k, 4) * 8 + z * 2 + yh, m)


def at_z(k):
    d, m, c, l = place()
    x, z, yh = axes_place()
    return (x * 8 + lax.rem(z + k, 4) * 2 + yh, m)


def stats_devices():
    d, m, c, l = place()
    x, z, yh = axes_place()
    mine = yh * 4 + m
    ydev = []
    for j in range(1, 8):
        other = lax.rem(mine + j, 8)
        ydev.append((x * 8 + z * 2 + other // 4, other % 4))
    return [at_x(j) for j in (1, 2, 3)], [at_z(j) for j in (1, 2, 3)], ydev


def greet(devices):
    barrier = pltpu.get_barrier_semaphore()
    for dev in devices:
        pl.semaphore_signal(barrier, inc=1, device_id=dev, device_id_type=MESH)
    pl.semaphore_wait(barrier, len(devices))


def remote(src, dst, sems, at, dev):
    cp = pltpu.make_async_remote_copy(
        src_ref=src, dst_ref=dst, send_sem=sems.at[(0, *at)], recv_sem=sems.at[(1, *at)],
        device_id=dev, device_id_type=MESH,
    )
    cp.start()
    return cp


def rows(start, size):
    return pl.ds(pl.multiple_of(start, size), size)


def by_blocks(total, block, body):
    lax.fori_loop(0, total // block, lambda i, z: (body(pl.multiple_of(i * block, block)), z)[1], 0)


def dot(left, right, contract, **kw):
    return lax.dot_general(
        left, right, ((contract[:1], contract[1:]), ((), ())), preferred_element_type=F32, **kw
    )


def iota(shape, axis):
    return lax.broadcasted_iota(jnp.int32, shape, axis)


def fold8(term):
    total = term[0:8]
    for k in range(1, term.shape[0] // 8):
        total = total + term[8 * k : 8 * k + 8]
    return total


def inverse_rms(x):
    return lax.rsqrt(jnp.mean(x * x, axis=-1, keepdims=True) + EPS)


def norm_back(x, inv, gain, up):
    weighted = up * gain
    return inv * weighted - x * (inv * inv * inv) * jnp.mean(x * weighted, axis=-1, keepdims=True)


def block_at(h, core, low):
    return h * 512 + core * 256 + low * 128


CHUNKS = [(h, k) for k in range(2) for h in range(2)]


class Sums:
    def __init__(self, p, near_own, near_far, far, sems):
        d, m, self.c, self.l = place()
        self.core, *self.over = partners()
        self.p, self.near_own, self.near_far, self.far = p, near_own, near_far, far
        self.own_sem, self.near_sem, self.far_sem = sems
        self.own, self.near, self.sent = {}, {}, {}

    def give_own(self):
        for h in range(2):
            src = self.p.at[rows(block_at(h, 1 - self.c, self.l), 128)]
            self.own[h] = remote(src, self.near_own.at[h], self.own_sem, (h,), self.core)

    def give_far(self, k):
        for h in range(2):
            src = self.p.at[rows(block_at(h, 1 - self.c, 1 - self.l) + k * 64, 64)]
            self.near[h, k] = remote(src, self.near_far.at[h, k], self.near_sem, (h, k), self.core)

    def pass_far(self, k):
        for h in range(2):
            self.near[h, k].wait_recv()
            base = block_at(h, self.c, 1 - self.l) + k * 64

            def body(i, h=h, base=base):
                self.near_far[h, k, pl.ds(i, 32), :] += self.p[rows(base + i, 32), :]

            by_blocks(64, 32, body)
            self.sent[h, k] = remote(
                self.near_far.at[h, k], self.far.at[h, k], self.far_sem, (h, k), self.over[h]
            )

    def take_own(self):
        for h in range(2):
            self.own[h].wait_recv()

    def take(self, h, k):
        self.sent[h, k].wait_recv()

    def value(self, h, k, i):
        mine = self.p[rows(block_at(h, self.c, self.l) + k * 64 + i, 32), :]
        return mine + self.near_own[h, pl.ds(k * 64 + i, 32), :] + self.far[h, k, pl.ds(i, 32), :]

    def drain(self):
        for group in (self.own, self.near, self.sent):
            for cp in group.values():
                cp.wait_send()


class Gather:
    def __init__(self, q, whole, low, sems):
        d, m, self.c, self.l = place()
        self.core, *self.over = partners()
        self.q, self.whole, self.low = q, whole, low
        self.over_sem, self.core_sem, self.fwd_sem = sems
        self.far, self.near, self.fwd, self.left = {}, {}, {}, set()

    def keep(self, base, src=None, at=0):
        def body(i):
            value = self.whole[rows(base + i, 32), :] if src is None else src[pl.ds(at + i, 32), :]
            self.low[rows(base + i, 32), :] = value.astype(BF16)

        by_blocks(64, 32, body)

    def send(self, h, k):
        base = block_at(h, self.c, self.l) + k * 64
        src, dst = self.q.at[pl.ds(h * 128 + k * 64, 64)], self.whole.at[rows(base, 64)]
        self.far[h, k] = remote(src, dst, self.over_sem, (h, k), self.over[h])
        self.near[h, k] = remote(src, dst, self.core_sem, (h, k), self.core)
        self.keep(base, self.q, h * 128 + k * 64)

    def take_core(self, h, k):
        self.near[h, k].wait_recv()
        self.keep(block_at(h, 1 - self.c, self.l) + k * 64)

    def take_far(self, h, k):
        self.far[h, k].wait_recv()
        base = block_at(h, self.c, 1 - self.l) + k * 64
        at = self.whole.at[rows(base, 64)]
        self.fwd[h, k] = remote(at, at, self.fwd_sem, (h, k), self.core)
        self.keep(base)

    def forwarded(self, k):
        for h in range(2):
            self.fwd[h, k].wait_send()
        self.left.add(k)

    def take_fwd(self, h, k):
        self.fwd[h, k].wait_recv()
        self.keep(block_at(h, 1 - self.c, 1 - self.l) + k * 64)

    def drain(self):
        late = [cp for (h, k), cp in self.fwd.items() if k not in self.left]
        for cp in [*self.far.values(), *self.near.values(), *late]:
            cp.wait_send()


SUM_SEMS = [
    pltpu.SemaphoreType.DMA((2, 2)), pltpu.SemaphoreType.DMA((2, 2, 2)), pltpu.SemaphoreType.DMA((2, 2, 2)),
]
GATHER_SEMS = [pltpu.SemaphoreType.DMA((2, 2, 2))] * 3


def gather_work_sum(gather, sums, work):
    c, l = sums.c, sums.l
    work([(block_at(h, c, l), 128) for h in range(2)])
    for h, k in CHUNKS:
        gather.take_core(h, k)
    work([(block_at(h, 1 - c, l), 128) for h in range(2)])
    sums.give_own()
    for k in range(2):
        for h in range(2):
            gather.take_far(h, k)
        work([(block_at(h, c, 1 - l) + k * 64, 64) for h in range(2)])
        for h in range(2):
            gather.take_fwd(h, k)
        work([(block_at(h, 1 - c, 1 - l) + k * 64, 64) for h in range(2)])
        sums.give_far(k)
        gather.forwarded(k)
        sums.pass_far(k)
    sums.take_own()


def spans_of(ref, spans, cols=slice(None)):
    return jnp.concatenate([ref[rows(at, n), cols] for at, n in spans], axis=0)


def put_spans(ref, spans, cols, value):
    done = 0
    for at, n in spans:
        ref[rows(at, n), cols] = value[done : done + n]
        done += n


def sum_everywhere(value, xs, zs, ys, xsem, zsem, ysem):
    d, m, c, l = place()
    x, z, yh = axes_place()
    xdev, zdev, ydev = stats_devices()

    def stage(slots, sems, devs, me, value):
        slots[me] = value
        copies = [remote(slots.at[me], slots.at[me], sems, (j,), dev) for j, dev in enumerate(devs)]
        for cp in copies:
            cp.wait_recv()
        total = slots[0]
        for k in range(1, len(devs) + 1):
            total = total + slots[k]
        for cp in copies:
            cp.wait_send()
        return total

    value = stage(xs, xsem, xdev, x, value)
    value = stage(zs, zsem, zdev, z, value)
    return stage(ys, ysem, ydev, yh * 4 + m, value)


STATS_SCRATCH = [
    pltpu.VMEM((4, 8, 128), F32),
    pltpu.VMEM((4, 8, 128), F32),
    pltpu.VMEM((8, 8, 128), F32),
    pltpu.SemaphoreType.DMA((2, 3)),
    pltpu.SemaphoreType.DMA((2, 3)),
    pltpu.SemaphoreType.DMA((2, 7)),
]


class Ring:
    def __init__(self, src, bufs, sems, pos, right, left):
        self.src, self.pos, self.right, self.left = src, pos, right, left
        self.mid, self.fl, self.fr = bufs
        self.sems = sems
        self.copies = []

    def send(self, src, dst, dev):
        self.copies.append(remote(src, dst, self.sems, (len(self.copies),), dev))

    def start(self):
        p = self.pos
        self.r, self.l, opp = lax.rem(p + 1, 4), lax.rem(p + 3, 4), lax.rem(p + 2, 4)
        self.send(self.src(opp, 0), self.mid.at[0], self.right)
        self.send(self.src(opp, 1), self.mid.at[1], self.left)
        self.send(self.src(self.r, 1), self.fl.at[1], self.right)
        self.send(self.src(self.l, 0), self.fr.at[0], self.left)

    def middle(self):
        self.copies[0].wait_recv()
        add_into(self.mid.at[0], self.src(self.r, 0))
        self.send(self.mid.at[0], self.fl.at[0], self.right)
        self.copies[1].wait_recv()
        add_into(self.mid.at[1], self.src(self.l, 1))
        self.send(self.mid.at[1], self.fr.at[1], self.left)

    def finish(self, out):
        for k in (2, 3, 4, 5):
            self.copies[k].wait_recv()
        for half in range(2):
            add_three(out(half), self.src(self.pos, half), self.fl.at[half], self.fr.at[half])

    def drain(self):
        for cp in self.copies:
            cp.wait_send()


def each_block(ref, body):
    if len(ref.shape) == 3:
        for k in range(ref.shape[0]):
            by_blocks(ref.shape[1], 16, lambda i, k=k: body((k, pl.ds(i, 16), slice(None))))
    else:
        by_blocks(ref.shape[0], 16, lambda i: body((pl.ds(i, 16), slice(None))))


def add_into(dst, src):
    def body(at):
        dst[at] += src[at]

    each_block(dst, body)


def add_three(dst, a, b, c):
    def body(at):
        dst[at] = a[at] + b[at] + c[at]

    each_block(dst, body)


def ring_one(order, src, bufs, sems):
    x, z, yh = axes_place()
    if order == "xz":
        return Ring(lambda j, h: src.at[j, pl.ds(h * 2, 2)], bufs, sems, x, at_x(1), at_x(3))
    return Ring(lambda j, h: src.at[pl.ds(h * 2, 2), j], bufs, sems, z, at_z(1), at_z(3))


def ring_two(order, res, bufs, sems):
    x, z, yh = axes_place()

    def src(j, h):
        return res.at[j, pl.ds(h * 32, 32)]

    if order == "xz":
        return Ring(src, bufs, sems, z, at_z(1), at_z(3))
    return Ring(src, bufs, sems, x, at_x(1), at_x(3))


def one_scratch(w):
    return [pltpu.VMEM((2, 2, 64, w), F32)] * 3 + [pltpu.SemaphoreType.DMA((2, 6))]


def two_scratch(w):
    return [
        *[pltpu.VMEM((2, 32, w), F32)] * 3,
        pltpu.VMEM((64, w), F32),
        pltpu.VMEM((32, w), F32),
        pltpu.SemaphoreType.DMA((2, 6)),
        pltpu.SemaphoreType.DMA((2,)),
    ]


def params(n):
    return pltpu.CompilerParams(
        collective_id=n, has_side_effects=True, vmem_limit_bytes=63 * 1024 * 1024
    )


def block_probs(q, k):
    r, s = iota((128, 128), 0), iota((128, 128), 1)
    seen = ((r // STEPS) == (s // STEPS)) & (r >= s)
    weights = jnp.where(seen, jnp.exp(dot(q, k, (1, 1)) * SCALE), 0.0)
    return weights / jnp.sum(weights, axis=-1, keepdims=True)


def policy_kernel(
    token_total,
    init_ref, act_ref, scale_ref, next_ref, rew_ref, obs_ref, gain_attn, wq_ref, wk_ref, wv_ref, wo_ref,
    gain_mlp, gain_fin, actor_ref, critic_ref, up_hbm, down_hbm,
    qkv_ref, match_ref, mixed_ref, ht_ref, low_one, gh_ref, g_fin, g_mlp, up_res, down_res,
    r_init, r_act, r_scale, roll_sem, tables, st_ref, own_ref, head_f, heads,
    w_up, w_down, w_sem,
    p, near_own, near_far, far, whole, h_two, up_rows, hidden, low_two, d_up, x_one, dx_two, buf_a, buf_b,
    fin_ref, grad_up, grad_down, *rest,
):
    stats, rest = rest[:6], rest[6:]
    sems_a, sems_b, sems_d = rest[0:3], rest[3:6], rest[6:9]
    gs_b, gs_d, gs_e = rest[9:12], rest[12:15], rest[15:18]
    um, ul, ur, us, dm, dl, dr, ds = rest[18:26]
    d, m, c, l = place()
    weights = [
        pltpu.make_async_copy(up_hbm, w_up, w_sem.at[0]), pltpu.make_async_copy(down_hbm, w_down, w_sem.at[1]),
    ]
    for cp in weights:
        cp.start()
    xdev, zdev, ydev = stats_devices()
    greet(xdev + zdev + ydev)
    far_dev = partners()[2]
    copies = [
        remote(src, dst, roll_sem, (n,), far_dev)
        for n, (src, dst) in enumerate(((init_ref, r_init), (act_ref, r_act), (scale_ref, r_scale)))
    ]

    def table_rows(i):
        at = pl.ds(i, 32)
        x = obs_ref[at, :].astype(F32)
        ht_ref[at, :] = (x * inverse_rms(x) * gain_attn[...]).astype(BF16)

    by_blocks(256, 32, table_rows)
    for n, w in enumerate((wq_ref, wk_ref, wv_ref)):
        tables[:, n * 256 : (n + 1) * 256] = dot(ht_ref[...], w[...], (1, 0)).astype(BF16)
    head_f[...] = jnp.zeros_like(head_f)
    head_f[0:16, :] = actor_ref[...].astype(F32)
    head_f[16:17, :] = critic_ref[...].astype(F32)
    heads[...] = jnp.zeros_like(heads)
    heads[0:32, :] = head_f[...].astype(BF16)

    for cp in copies:
        cp.wait()
    swap = 32 + 64 * l
    lane = iota((1, 64), 1)
    state = jnp.where(lane >= swap, r_init[...], init_ref[...]).astype(F32)
    scale = jnp.where(lane >= swap, r_scale[...], scale_ref[...])
    act_t = jnp.where(iota((16, 64), 1) >= swap, r_act[...], act_ref[...]).astype(F32)
    nexts = next_ref[...].astype(F32).astype(BF16)
    ids, kinds = iota((256, 64), 0).astype(F32), iota((16, 64), 0).astype(F32)
    for t in range(STEPS):
        st_ref[pl.ds(t, 1), :] = state
        if t + 1 < STEPS:
            hit = jnp.where(ids == state, 1.0, 0.0).astype(BF16)
            found = dot(nexts, hit, (1, 0))
            state = jnp.sum(jnp.where(kinds == act_t[t : t + 1, :], found, 0.0), axis=0, keepdims=True)

    pick_t = (iota((128, 16), 0) % STEPS == iota((128, 16), 1)).astype(BF16)
    spread = jnp.ones((64, 128), BF16)
    lanes = iota((128, 128), 1).astype(F32)

    def per_token(rows_by_env, first_env):
        here = iota((128, 64), 1) == first_env + iota((128, 64), 0) // STEPS
        found = jnp.where(here, dot(pick_t, rows_by_env, (1, 0)), 0.0)
        return dot(found.astype(BF16), spread, (1, 0))

    def attend(core, low):
        def block(h, carry):
            at = rows(block_at(h, core, low), 128)
            ids_here = per_token(st_ref[...].astype(BF16), h * 32 + (core * 2 + low) * 8)
            match = jnp.concatenate(
                [jnp.where(ids_here == lanes, 1.0, 0.0), jnp.where(ids_here == lanes + 128.0, 1.0, 0.0)], axis=1
            ).astype(BF16)
            match_ref[at, :] = match
            qkv = dot(match, tables[...], (1, 0)).astype(BF16)
            qkv_ref[at, :] = qkv
            outs = []
            for n in range(2):
                q, k, v = (qkv[:, j * 256 + n * 128 : j * 256 + (n + 1) * 128] for j in range(3))
                outs.append(dot(block_probs(q, k).astype(BF16), v, (1, 0)).astype(BF16))
            mixed = jnp.concatenate(outs, axis=1)
            mixed_ref[at, :] = mixed
            p[at, :] = dot(mixed, wo_ref[...], (1, 0))
            return carry

        lax.fori_loop(0, 2, block, 0)

    sums = Sums(p, near_own, near_far, far, sems_a)
    attend(1 - c, 1 - l)
    sums.give_far(0)
    sums.give_far(1)
    attend(c, 1 - l)
    sums.pass_far(0)
    sums.pass_far(1)
    attend(1 - c, l)
    sums.give_own()
    attend(c, l)
    for h in range(2):
        at = pl.ds(h * 128, 128)
        mine = match_ref[rows(block_at(h, c, l), 128), :]
        x_one[at, :] = dot(mine, obs_ref[...], (1, 0))
        first_env = h * 32 + (c * 2 + l) * 8
        chosen = jnp.where(per_token(act_t.astype(BF16), first_env) == lanes, 1.0, 0.0)
        found = dot(mine.astype(F32), rew_ref[...], (1, 1), precision=lax.Precision.HIGHEST)
        here = iota((128, 64), 1) == first_env + iota((128, 64), 0) // STEPS
        factor = jnp.sum(jnp.where(here, scale, 0.0), axis=1, keepdims=True)
        reward = jnp.sum(chosen[:, :16] * found, axis=1, keepdims=True) * factor
        own_ref[at, :] = jnp.where(lanes == 16.0, reward, chosen)
    sums.take_own()

    gather = Gather(buf_a, whole, h_two, gs_b)
    for h, k in CHUNKS:
        sums.take(h, k)

        def body(i, h=h, k=k):
            at = pl.ds(h * 128 + k * 64 + i, 32)
            x = sums.value(h, k, i) + x_one[at, :]
            x_one[at, :] = x
            buf_a[at, :] = x * inverse_rms(x) * gain_mlp[...]

        by_blocks(64, 32, body)
        gather.send(h, k)
    sums.drain()
    for cp in weights:
        cp.wait()

    def forward(spans):
        def up(j):
            cols = pl.ds(j, 256)
            u = dot(spans_of(h_two, spans), w_up[:, cols], (1, 0))
            put_spans(up_rows, spans, cols, u)
            put_spans(hidden, spans, cols, (u / (1.0 + jnp.exp(-u))).astype(BF16))

        def down(j):
            cols = pl.ds(j, 256)
            put_spans(p, spans, cols, dot(spans_of(hidden, spans), w_down[:, cols], (1, 0)))

        by_blocks(1024, 256, up)
        by_blocks(1024, 256, down)

    sums = Sums(p, near_own, near_far, far, sems_b)
    gather_work_sum(gather, sums, forward)
    for h, k in CHUNKS:
        sums.take(h, k)

        def body(i, h=h, k=k):
            at = pl.ds(h * 128 + k * 64 + i, 32)
            x = sums.value(h, k, i) + x_one[at, :]
            buf_b[at, :] = x
            fin_ref[at, :] = (x * inverse_rms(x) * gain_fin[...]).astype(BF16)

        by_blocks(64, 32, body)
    gather.drain()
    sums.drain()

    lane = iota((256, 128), 1)
    both = dot(fin_ref[...], heads[...], (1, 1))
    critic = jnp.sum(jnp.where(lane == 16, both, 0.0), axis=1, keepdims=True)
    own = own_ref[...]
    reward = jnp.sum(jnp.where(lane == 16, own, 0.0), axis=1, keepdims=True)
    step = iota((256, 128), 0) % STEPS
    base = reward + jnp.where(step == STEPS - 1, GAMMA * critic, 0.0)
    r, s = iota((256, 256), 0), iota((256, 256), 1)
    ahead = ((r // STEPS) == (s // STEPS)) & (s >= r)
    decay = jnp.where(ahead, jnp.exp((s - r).astype(F32) * math.log(GAMMA)), 0.0)
    returns = dot(decay, base, (1, 0), precision=lax.Precision.HIGHEST)
    advantage = returns - critic
    tile = jnp.where(
        iota((8, 128), 0) == 0,
        jnp.sum(advantage, axis=0, keepdims=True),
        jnp.sum(advantage * advantage, axis=0, keepdims=True),
    )
    totals = sum_everywhere(tile, *stats)
    mean = totals[0:1, :] * (1.0 / token_total)
    variance = totals[1:2, :] * (1.0 / token_total) - mean * mean
    normed = (advantage - mean) * lax.rsqrt(variance + EPS)
    real = lane < 16
    logits = jnp.where(real, both, 0.0)
    mass = jnp.sum(jnp.where(real, jnp.exp(logits), 0.0), axis=1, keepdims=True)
    logp = jnp.where(real, logits - jnp.log(mass), 0.0)
    chance = jnp.where(real, jnp.exp(logp), 0.0)
    entropy = -jnp.sum(chance * logp, axis=1, keepdims=True)
    factor = 1.0 / math.sqrt(token_total)
    picked = jnp.where(real, own, 0.0)
    d_logits = factor * (-normed * (picked - chance) + ENTROPY_COEF * chance * (logp + entropy))
    d_value = (factor * VALUE_COEF) * (critic - returns)
    d_both = jnp.where(real, d_logits, jnp.where(lane == 16, d_value, 0.0)).astype(BF16)
    buf_a[...] = dot(d_both, heads[...], (1, 0))
    g_fin[...] = jnp.zeros_like(g_fin)
    g_mlp[...] = jnp.zeros_like(g_mlp)

    gather = Gather(dx_two, whole, low_two, gs_d)
    for h, k in CHUNKS:

        def body(i, h=h, k=k):
            at = pl.ds(h * 128 + k * 64 + i, 32)
            x, up = buf_b[at, :], buf_a[at, :]
            inv = inverse_rms(x)
            dx_two[at, :] = norm_back(x, inv, gain_fin[...], up)
            g_fin[...] += fold8(up * x * inv)

        by_blocks(64, 32, body)
        gather.send(h, k)
    gh_ref[...] = dot(fin_ref[...], d_both, (0, 0))

    def backward(spans):
        def up(j):
            cols = pl.ds(j, 256)
            d_hidden = dot(spans_of(low_two, spans), w_down[cols, :], (1, 1)).astype(BF16).astype(F32)
            u = spans_of(up_rows, spans, cols)
            sig = 1.0 / (1.0 + jnp.exp(-u))
            put_spans(d_up, spans, cols, (d_hidden * sig * (1.0 + u * (1.0 - sig))).astype(BF16))

        def down(j):
            cols = pl.ds(j, 256)
            put_spans(p, spans, cols, dot(spans_of(d_up, spans), w_up[cols, :], (1, 1)))

        by_blocks(1024, 256, up)
        by_blocks(1024, 256, down)

    sums = Sums(p, near_own, near_far, far, sems_d)
    gather_work_sum(gather, sums, backward)

    def weight_grad(out, left, right):
        def tile(j, carry):
            cols = rows(j * 256, 256)
            out[j] = dot(left[:, cols], right[...], (0, 0)).reshape(4, 64, 1024)
            return carry

        lax.fori_loop(0, 4, tile, 0)

    up_ring = ring_one("xz", grad_up, (um, ul, ur), us)
    down_ring = ring_one("zx", grad_down, (dm, dl, dr), ds)
    weight_grad(grad_up, h_two, d_up)
    up_ring.start()
    weight_grad(grad_down, low_two, hidden)
    down_ring.start()
    gather.drain()

    gather = Gather(buf_b, whole, low_one, gs_e)
    for h, k in CHUNKS:
        sums.take(h, k)

        def body(i, h=h, k=k):
            at = pl.ds(h * 128 + k * 64 + i, 32)
            up, x = sums.value(h, k, i), x_one[at, :]
            inv = inverse_rms(x)
            buf_b[at, :] = dx_two[at, :] + norm_back(x, inv, gain_mlp[...], up)
            g_mlp[...] += fold8(up * x * inv)

        by_blocks(64, 32, body)
        gather.send(h, k)
    sums.drain()
    for h, k in CHUNKS:
        gather.take_core(h, k)
    for h in range(2):
        gather.take_far(h, 0)
    up_ring.middle()
    down_ring.middle()
    for h in range(2):
        gather.take_far(h, 1)
    for h, k in CHUNKS:
        gather.take_fwd(h, k)
    gather.drain()
    up_ring.finish(lambda h: up_res.at[pl.ds(h * 2, 2)])
    down_ring.finish(lambda h: down_res.at[pl.ds(h * 2, 2)])
    up_ring.drain()
    down_ring.drain()


def policy(token_total, *args):
    sd, vm = jax.ShapeDtypeStruct, pltpu.VMEM
    return pl.pallas_call(
        functools.partial(policy_kernel, token_total),
        out_shape=(
            sd((1024, 768), BF16), sd((1024, 256), BF16), sd((1024, 256), BF16), sd((256, 1024), BF16),
            sd((1024, 1024), BF16), sd((1024, 128), F32), sd((8, 1024), F32), sd((8, 1024), F32),
            sd((4, 64, 1024), F32), sd((4, 64, 1024), F32),
        ),
        in_specs=[VMEM] * 15 + [ANY] * 2,
        out_specs=tuple([VMEM] * 10),
        scratch_shapes=[
            vm((1, 64), jnp.int32), vm((16, 64), jnp.int32), vm((1, 64), F32), pltpu.SemaphoreType.DMA((2, 3)),
            vm((256, 768), BF16), vm((16, 64), F32), vm((256, 128), F32), vm((32, 1024), F32), vm((128, 1024), BF16),
            vm((1024, 1024), BF16), vm((1024, 1024), BF16), pltpu.SemaphoreType.DMA((2,)),
            vm((1024, 1024), F32), vm((2, 128, 1024), F32), vm((2, 2, 64, 1024), F32), vm((2, 2, 64, 1024), F32),
            vm((1024, 1024), F32), vm((1024, 1024), BF16), vm((1024, 1024), F32), vm((1024, 1024), BF16),
            vm((1024, 1024), BF16), vm((1024, 1024), BF16),
            vm((256, 1024), F32), vm((256, 1024), F32), vm((256, 1024), F32), vm((256, 1024), F32),
            vm((256, 1024), BF16), vm((4, 4, 64, 1024), F32), vm((4, 4, 64, 1024), F32),
            *STATS_SCRATCH, *SUM_SEMS, *SUM_SEMS, *SUM_SEMS, *GATHER_SEMS, *GATHER_SEMS, *GATHER_SEMS,
            *one_scratch(1024), *one_scratch(1024),
        ],
        compiler_params=params(1),
        name="policy",
    )(*args)


def halves(value):
    high = value.astype(BF16)
    return high, (value - high.astype(F32)).astype(BF16)


def attend_back_kernel(
    dx_ref, wo_ref, qkv_ref, match_ref, ht_ref, obs_ref, wq_ref, wk_ref, wv_ref, gh_ref, gf_ref, gm_ref,
    qk_ref, v_ref, small_ref, sums, dt_ref, vec_ref,
):
    sums[...] = jnp.zeros_like(sums)

    def block(b, carry):
        at = rows(b * 128, 128)
        d_mixed = dot(dx_ref[at, :], wo_ref[...], (1, 1)).astype(BF16)
        qkv = qkv_ref[at, :]
        parts = [[], [], []]
        for h in range(2):
            q, k, v = (qkv[:, n * 256 + h * 128 : n * 256 + (h + 1) * 128] for n in range(3))
            up = d_mixed[:, h * 128 : (h + 1) * 128]
            probs = block_probs(q, k)
            d_probs = dot(up, v, (1, 1))
            parts[2].append(dot(probs.astype(BF16), up, (0, 0)).astype(BF16))
            d_scores = (
                probs * (d_probs - jnp.sum(probs * d_probs, axis=-1, keepdims=True)) * SCALE
            ).astype(BF16)
            parts[0].append(dot(d_scores, k, (1, 0)).astype(BF16))
            parts[1].append(dot(d_scores, q, (0, 0)).astype(BF16))
        d_qkv = jnp.concatenate([*parts[0], *parts[1], *parts[2]], axis=1)
        sums[...] += dot(match_ref[at, :], d_qkv, (0, 0))
        return carry

    lax.fori_loop(0, 8, block, 0)
    high, low = halves(sums[...])
    for i in range(4):
        cols = pl.ds(i * 256, 256)
        table = ht_ref[:, cols]
        total = dot(table, high, (0, 0)) + dot(table, low, (0, 0))
        qk_ref[cols, :] = total[:, :512]
        v_ref[cols, :] = total[:, 512:]
    dt_ref[...] = jnp.zeros_like(dt_ref)
    for n, w in enumerate((wq_ref, wk_ref, wv_ref)):
        cols = slice(n * 256, (n + 1) * 256)
        dt_ref[...] += dot(high[:, cols], w[...], (1, 1)) + dot(low[:, cols], w[...], (1, 1))
    vec_ref[0:8] = gf_ref[...]
    vec_ref[8:16] = gm_ref[...]
    vec_ref[16:32] = jnp.zeros((16, 1024), F32)

    def gain_rows(i):
        at = pl.ds(i, 32)
        x = obs_ref[at, :].astype(F32)
        inv = lax.rsqrt(jnp.mean(x * x, axis=-1, keepdims=True) + EPS)
        vec_ref[16:24] += fold8(dt_ref[at, :] * x * inv)

    by_blocks(256, 32, gain_rows)
    place_at = (iota((32, 128), 1) == 17 + iota((32, 128), 0) // 8).astype(BF16)
    vec = vec_ref[...]
    high, low = halves(vec)
    lowest = (vec - high.astype(F32) - low.astype(F32)).astype(BF16)
    small_ref[...] = gh_ref[...] + sum(dot(part, place_at, (0, 0)) for part in (high, low, lowest))


def attend_back(*args):
    sd = jax.ShapeDtypeStruct
    return pl.pallas_call(
        attend_back_kernel,
        out_shape=(sd((1024, 512), F32), sd((1024, 256), F32), sd((1024, 128), F32)),
        in_specs=[VMEM] * 12,
        out_specs=tuple([VMEM] * 3),
        scratch_shapes=[pltpu.VMEM((256, 768), F32), pltpu.VMEM((256, 1024), F32), pltpu.VMEM((32, 1024), F32)],
        compiler_params=pltpu.CompilerParams(vmem_limit_bytes=40 * 1024 * 1024),
        name="attend_back",
    )(*args)


FIRST = ("xz", "zx", "zx", "xz")
SECOND = ("xz", "zx") + FIRST


def grads_kernel(*refs):
    ins, outs, scratch = refs[:6], refs[6:12], refs[12:]
    mp_buf, mp_sem = scratch[-2:]
    d, m, c, l = place()
    x, z, yh = axes_place()
    yother = (d + 1 - 2 * yh, m)
    peers = [(d, lax.rem(m + j, 4)) for j in (1, 2, 3)]
    greet([at_x(1), at_x(3), at_z(1), at_z(3), yother] + peers)

    first, second, results = [], [], [ins[0], ins[1]]
    for i, order in enumerate(FIRST):
        mid, fl, fr, sems, res = scratch[5 * i : 5 * i + 5]
        first.append(ring_one(order, ins[2 + i], (mid, fl, fr), sems))
        results.append(res)
    at = 20
    ends = []
    for i, order in enumerate(SECOND):
        mid, fl, fr, res, ybuf, sems, ysem = scratch[at + 7 * i : at + 7 * i + 7]
        second.append(ring_two(order, results[i], (mid, fl, fr), sems))
        ends.append((res, ybuf, ysem))
    tails = []

    def send_tail(i):
        res, ybuf, ysem = ends[i]
        second[i].finish(lambda h: res.at[pl.ds(h * 32, 32)])
        tails.append(remote(res.at[rows((1 - yh) * 32, 32)], ybuf, ysem, (), yother))

    for ring in first:
        ring.start()
    for ring in second[:2]:
        ring.start()
    for ring in first:
        ring.middle()
    for ring in second[:2]:
        ring.middle()
    for i, ring in enumerate(first):
        res = results[2 + i]
        ring.finish(lambda h, res=res: res.at[pl.ds(h * 2, 2)])
        second[2 + i].start()
    for i in range(2):
        send_tail(i)
    for ring in second[2:]:
        ring.middle()
    for i in (5, 2, 3, 4):
        send_tail(i)

    def total(i, put):
        res, ybuf, _ = ends[i]
        by_blocks(32, 8, lambda k: put(k, res[rows(yh * 32 + k, 8), :] + ybuf[pl.ds(k, 8), :]))

    def to_out(ref):
        def put(k, value):
            ref[pl.ds(k, 8), :] = value

        return put

    def to_mp(k, value):
        mp_buf[m, pl.ds(k, 8), :] = value

    shares = []
    for n, i in enumerate((0, 1, 5, 2, 3, 4)):
        tails[n].wait_recv()
        if i == 5:
            total(i, to_mp)
            for j, dev in enumerate(peers):
                shares.append(remote(mp_buf.at[m], mp_buf.at[m], mp_sem, (j,), dev))
        else:
            total(i, to_out(outs[i]))
    for cp in shares:
        cp.wait_recv()
    outs[5][...] = mp_buf[0] + mp_buf[1] + mp_buf[2] + mp_buf[3]
    for cp in shares + tails:
        cp.wait_send()
    for ring in first + second:
        ring.drain()


def reduce_grads(up_res, down_res, qk, value, out, small):
    wide = [1024, 1024, 512, 256, 256, 128]
    scratch = []
    for w in wide[2:]:
        scratch += one_scratch(w) + [pltpu.VMEM((4, 64, w), F32)]
    for w in wide:
        scratch += two_scratch(w)
    scratch += [pltpu.VMEM((4, 32, 128), F32), pltpu.SemaphoreType.DMA((2, 3))]
    return pl.pallas_call(
        grads_kernel,
        out_shape=tuple(jax.ShapeDtypeStruct((32, w), F32) for w in wide),
        in_specs=[VMEM] * 6,
        out_specs=tuple([VMEM] * 6),
        scratch_shapes=scratch,
        compiler_params=params(6),
        name="reduce_grads",
    )(up_res, down_res, *[a.reshape(4, 4, 64, a.shape[1]) for a in (qk, value, out, small)])


def write_kernel(
    up_ref, down_ref, qk_ref, value_ref, out_ref, small_ref,
    o_q, o_k, o_v, o_out, o_up, o_down, o_actor, o_flat,
):
    o_q[...] = qk_ref[:, :256]
    o_k[...] = qk_ref[:, 256:]
    o_v[...] = value_ref[...]
    o_up[...] = up_ref[...]
    o_out[...] = out_ref[...]
    o_down[...] = down_ref[...]
    flat = jnp.transpose(small_ref[...])
    o_actor[...] = flat[:16, :]
    o_flat[...] = flat[16:24, :]


def write_outputs(*parts):
    sd = jax.ShapeDtypeStruct
    return pl.pallas_call(
        write_kernel,
        out_shape=(
            sd((32, 256), F32), sd((32, 256), F32), sd((32, 256), F32), sd((32, 256), F32), sd((32, 1024), F32),
            sd((32, 1024), F32), sd((16, 32), F32), sd((8, 32), F32),
        ),
        in_specs=[VMEM] * 6,
        out_specs=tuple([VMEM] * 8),
        name="write_outputs",
    )(*parts)


def per_device(
    initial_state,
    actions,
    next_state,
    reward_table,
    reward_scale,
    observe_table,
    gain_attn,
    w_query,
    w_key,
    w_value,
    w_out,
    gain_mlp,
    w_up,
    w_down,
    gain_final,
    actor_head,
    critic_head,
):
    token_total = actions.size * lax.axis_size("dp")

    def line(vector):
        return vector.reshape(1, -1)

    qkv, match, mixed, h_table, dx_one_low, grad_heads, final_terms, mlp_terms, up_res, down_res = policy(
        token_total,
        line(initial_state), actions.T, line(reward_scale), next_state.T, reward_table.T, observe_table,
        line(gain_attn), w_query, w_key, w_value, w_out, line(gain_mlp), line(gain_final),
        actor_head.T, line(critic_head), w_up, w_down,
    )
    grad_out = jnp.dot(dx_one_low.T, mixed, preferred_element_type=F32)
    grad_qk, grad_value, small = attend_back(
        dx_one_low, w_out, qkv, match, h_table, observe_table, w_query, w_key, w_value,
        grad_heads, final_terms, mlp_terms,
    )
    parts = reduce_grads(up_res, down_res, grad_qk, grad_value, grad_out, small)
    q, k, v, out, up, down, actor, flat = write_outputs(*parts)
    attn_own = lax.dynamic_slice_in_dim(flat[3], lax.axis_index("mp") * 8, 8, 0)
    return (q, k, v, out.T, up, down.T, attn_own, flat[2], flat[1], actor.T, flat[0])


def solution(mesh):
    return jax.shard_map(
        per_device,
        mesh=mesh,
        in_specs=(
            P("dp"),
            P("dp", None),
            P(),
            P(),
            P("dp"),
            P(),
            P(),
            P(None, "mp"),
            P(None, "mp"),
            P(None, "mp"),
            P("mp", None),
            P(),
            P(None, "mp"),
            P("mp", None),
            P(),
            P(),
            P(),
        ),
        out_specs=(
            P("dp", "mp"),
            P("dp", "mp"),
            P("dp", "mp"),
            P("mp", "dp"),
            P("dp", "mp"),
            P("mp", "dp"),
            P(("dp", "mp")),
            P("dp"),
            P("dp"),
            P("dp", None),
            P("dp"),
        ),
        check_vma=False,
    )
```

```python
import functools
import math

import jax
import jax.numpy as jnp
from jax import lax
from jax.experimental import pallas as pl
from jax.experimental.pallas import tpu as pltpu
from jax.sharding import PartitionSpec as P

HEAD_DIM = 128
STEPS = 16
EPS = 1e-05
GAMMA = 0.9
VALUE_COEF = 0.5
ENTROPY_COEF = 0.1
SCALE = 1.0 / math.sqrt(HEAD_DIM)
MESH = pl.DeviceIdType.MESH
VMEM = pl.BlockSpec(memory_space=pltpu.VMEM)
WIDE = 1024
ANY = pl.BlockSpec(memory_space=pl.ANY)
F32 = jnp.float32
BF16 = jnp.bfloat16


def place():
    d, m = lax.axis_index("dp"), lax.axis_index("mp")
    return d, m, m % 2, m // 2


def axes_place():
    d, m, c, l = place()
    return d // 8, (d // 2) % 4, d % 2


def partners():
    d, m, c, l = place()
    over = m + 2 - 4 * l
    return (d, m + 1 - 2 * c), (d, over), (d + 1 - 2 * (d % 2), over)


def at_x(k):
    d, m, c, l = place()
    x, z, yh = axes_place()
    return (lax.rem(x + k, 4) * 8 + z * 2 + yh, m)


def at_z(k):
    d, m, c, l = place()
    x, z, yh = axes_place()
    return (x * 8 + lax.rem(z + k, 4) * 2 + yh, m)


def stats_devices():
    d, m, c, l = place()
    x, z, yh = axes_place()
    mine = yh * 4 + m
    ydev = []
    for j in range(1, 8):
        other = lax.rem(mine + j, 8)
        ydev.append((x * 8 + z * 2 + other // 4, other % 4))
    return [at_x(j) for j in (1, 2, 3)], [at_z(j) for j in (1, 2, 3)], ydev


def greet(devices):
    barrier = pltpu.get_barrier_semaphore()
    for dev in devices:
        pl.semaphore_signal(barrier, inc=1, device_id=dev, device_id_type=MESH)
    pl.semaphore_wait(barrier, len(devices))


def remote(src, dst, sems, at, dev):
    cp = pltpu.make_async_remote_copy(
        src_ref=src, dst_ref=dst, send_sem=sems.at[(0, *at)], recv_sem=sems.at[(1, *at)],
        device_id=dev, device_id_type=MESH,
    )
    cp.start()
    return cp


def rows(start, size):
    return pl.ds(pl.multiple_of(start, size), size)


def by_blocks(total, block, body):
    lax.fori_loop(0, total // block, lambda i, z: (body(pl.multiple_of(i * block, block)), z)[1], 0)


def dot(left, right, contract, **kw):
    return lax.dot_general(
        left, right, ((contract[:1], contract[1:]), ((), ())), preferred_element_type=F32, **kw
    )


def iota(shape, axis):
    return lax.broadcasted_iota(jnp.int32, shape, axis)


def fold8(term):
    total = term[0:8]
    for k in range(1, term.shape[0] // 8):
        total = total + term[8 * k : 8 * k + 8]
    return total


def inverse_rms(x):
    return lax.rsqrt(jnp.mean(x * x, axis=-1, keepdims=True) + EPS)


def norm_back(x, inv, gain, up):
    weighted = up * gain
    return inv * weighted - x * (inv * inv * inv) * jnp.mean(x * weighted, axis=-1, keepdims=True)


def block_at(h, core, low):
    return h * 512 + core * 256 + low * 128


CHUNKS = [(h, k) for k in range(2) for h in range(2)]


class Sums:
    def __init__(self, p, near_own, near_far, far, sems):
        d, m, self.c, self.l = place()
        self.core, *self.over = partners()
        self.p, self.near_own, self.near_far, self.far = p, near_own, near_far, far
        self.own_sem, self.near_sem, self.far_sem = sems
        self.own, self.near, self.sent = {}, {}, {}

    def give_own(self):
        for h in range(2):
            src = self.p.at[rows(block_at(h, 1 - self.c, self.l), 128)]
            self.own[h] = remote(src, self.near_own.at[h], self.own_sem, (h,), self.core)

    def give_far(self, k):
        for h in range(2):
            src = self.p.at[rows(block_at(h, 1 - self.c, 1 - self.l) + k * 64, 64)]
            self.near[h, k] = remote(src, self.near_far.at[h, k], self.near_sem, (h, k), self.core)

    def pass_far(self, k):
        for h in range(2):
            self.near[h, k].wait_recv()
            base = block_at(h, self.c, 1 - self.l) + k * 64

            def body(i, h=h, base=base):
                self.near_far[h, k, pl.ds(i, 32), :] += self.p[rows(base + i, 32), :]

            by_blocks(64, 32, body)
            self.sent[h, k] = remote(
                self.near_far.at[h, k], self.far.at[h, k], self.far_sem, (h, k), self.over[h]
            )

    def take_own(self):
        for h in range(2):
            self.own[h].wait_recv()

    def take(self, h, k):
        self.sent[h, k].wait_recv()

    def value(self, h, k, i):
        mine = self.p[rows(block_at(h, self.c, self.l) + k * 64 + i, 32), :]
        return mine + self.near_own[h, pl.ds(k * 64 + i, 32), :] + self.far[h, k, pl.ds(i, 32), :]

    def drain(self):
        for group in (self.own, self.near, self.sent):
            for cp in group.values():
                cp.wait_send()


class Gather:
    def __init__(self, q, whole, low, sems):
        d, m, self.c, self.l = place()
        self.core, *self.over = partners()
        self.q, self.whole, self.low = q, whole, low
        self.over_sem, self.core_sem, self.fwd_sem = sems
        self.far, self.near, self.fwd, self.left = {}, {}, {}, set()

    def keep(self, base, src=None, at=0):
        def body(i):
            value = self.whole[rows(base + i, 32), :] if src is None else src[pl.ds(at + i, 32), :]
            self.low[rows(base + i, 32), :] = value.astype(BF16)

        by_blocks(64, 32, body)

    def send(self, h, k):
        base = block_at(h, self.c, self.l) + k * 64
        src, dst = self.q.at[pl.ds(h * 128 + k * 64, 64)], self.whole.at[rows(base, 64)]
        self.far[h, k] = remote(src, dst, self.over_sem, (h, k), self.over[h])
        self.near[h, k] = remote(src, dst, self.core_sem, (h, k), self.core)
        self.keep(base, self.q, h * 128 + k * 64)

    def take_core(self, h, k):
        self.near[h, k].wait_recv()
        self.keep(block_at(h, 1 - self.c, self.l) + k * 64)

    def take_far(self, h, k):
        self.far[h, k].wait_recv()
        base = block_at(h, self.c, 1 - self.l) + k * 64
        at = self.whole.at[rows(base, 64)]
        self.fwd[h, k] = remote(at, at, self.fwd_sem, (h, k), self.core)
        self.keep(base)

    def forwarded(self, k):
        for h in range(2):
            self.fwd[h, k].wait_send()
        self.left.add(k)

    def take_fwd(self, h, k):
        self.fwd[h, k].wait_recv()
        self.keep(block_at(h, 1 - self.c, 1 - self.l) + k * 64)

    def drain(self):
        late = [cp for (h, k), cp in self.fwd.items() if k not in self.left]
        for cp in [*self.far.values(), *self.near.values(), *late]:
            cp.wait_send()


SUM_SEMS = [
    pltpu.SemaphoreType.DMA((2, 2)), pltpu.SemaphoreType.DMA((2, 2, 2)), pltpu.SemaphoreType.DMA((2, 2, 2)),
]
GATHER_SEMS = [pltpu.SemaphoreType.DMA((2, 2, 2))] * 3


def gather_work_sum(gather, sums, work):
    c, l = sums.c, sums.l
    work([(block_at(h, c, l), 128) for h in range(2)])
    for h, k in CHUNKS:
        gather.take_core(h, k)
    work([(block_at(h, 1 - c, l), 128) for h in range(2)])
    sums.give_own()
    for k in range(2):
        for h in range(2):
            gather.take_far(h, k)
        work([(block_at(h, c, 1 - l) + k * 64, 64) for h in range(2)])
        for h in range(2):
            gather.take_fwd(h, k)
        work([(block_at(h, 1 - c, 1 - l) + k * 64, 64) for h in range(2)])
        sums.give_far(k)
        gather.forwarded(k)
        sums.pass_far(k)
    sums.take_own()


def spans_of(ref, spans, cols=slice(None)):
    return jnp.concatenate([ref[rows(at, n), cols] for at, n in spans], axis=0)


def put_spans(ref, spans, cols, value):
    done = 0
    for at, n in spans:
        ref[rows(at, n), cols] = value[done : done + n]
        done += n


def sum_everywhere(value, xs, zs, ys, xsem, zsem, ysem):
    d, m, c, l = place()
    x, z, yh = axes_place()
    xdev, zdev, ydev = stats_devices()

    def stage(slots, sems, devs, me, value):
        slots[me] = value
        copies = [remote(slots.at[me], slots.at[me], sems, (j,), dev) for j, dev in enumerate(devs)]
        for cp in copies:
            cp.wait_recv()
        total = slots[0]
        for k in range(1, len(devs) + 1):
            total = total + slots[k]
        for cp in copies:
            cp.wait_send()
        return total

    value = stage(xs, xsem, xdev, x, value)
    value = stage(zs, zsem, zdev, z, value)
    return stage(ys, ysem, ydev, yh * 4 + m, value)


STATS_SCRATCH = [
    pltpu.VMEM((4, 8, 128), F32),
    pltpu.VMEM((4, 8, 128), F32),
    pltpu.VMEM((8, 8, 128), F32),
    pltpu.SemaphoreType.DMA((2, 3)),
    pltpu.SemaphoreType.DMA((2, 3)),
    pltpu.SemaphoreType.DMA((2, 7)),
]


class Ring:
    def __init__(self, src, bufs, sems, pos, right, left):
        self.src, self.pos, self.right, self.left = src, pos, right, left
        self.mid, self.fl, self.fr = bufs
        self.sems = sems
        self.copies = []

    def send(self, src, dst, dev):
        self.copies.append(remote(src, dst, self.sems, (len(self.copies),), dev))

    def start(self):
        p = self.pos
        self.r, self.l, opp = lax.rem(p + 1, 4), lax.rem(p + 3, 4), lax.rem(p + 2, 4)
        self.send(self.src(opp, 0), self.mid.at[0], self.right)
        self.send(self.src(opp, 1), self.mid.at[1], self.left)
        self.send(self.src(self.r, 1), self.fl.at[1], self.right)
        self.send(self.src(self.l, 0), self.fr.at[0], self.left)

    def middle(self):
        self.copies[0].wait_recv()
        add_into(self.mid.at[0], self.src(self.r, 0))
        self.send(self.mid.at[0], self.fl.at[0], self.right)
        self.copies[1].wait_recv()
        add_into(self.mid.at[1], self.src(self.l, 1))
        self.send(self.mid.at[1], self.fr.at[1], self.left)

    def finish(self, out):
        for k in (2, 3, 4, 5):
            self.copies[k].wait_recv()
        for half in range(2):
            add_three(out(half), self.src(self.pos, half), self.fl.at[half], self.fr.at[half])

    def drain(self):
        for cp in self.copies:
            cp.wait_send()


def each_block(ref, body):
    if len(ref.shape) == 3:
        for k in range(ref.shape[0]):
            by_blocks(ref.shape[1], 16, lambda i, k=k: body((k, pl.ds(i, 16), slice(None))))
    else:
        by_blocks(ref.shape[0], 16, lambda i: body((pl.ds(i, 16), slice(None))))


def add_into(dst, src):
    def body(at):
        dst[at] += src[at]

    each_block(dst, body)


def add_three(dst, a, b, c):
    def body(at):
        dst[at] = a[at] + b[at] + c[at]

    each_block(dst, body)


def ring_one(order, src, bufs, sems, cols=slice(None)):
    x, z, yh = axes_place()
    every = slice(None)
    if order == "xz":
        return Ring(lambda j, h: src.at[j, pl.ds(h * 2, 2), every, cols], bufs, sems, x, at_x(1), at_x(3))
    return Ring(lambda j, h: src.at[pl.ds(h * 2, 2), j, every, cols], bufs, sems, z, at_z(1), at_z(3))


def ring_two(order, res, bufs, sems):
    x, z, yh = axes_place()

    def src(j, h):
        return res.at[j, pl.ds(h * 32, 32)]

    if order == "xz":
        return Ring(src, bufs, sems, z, at_z(1), at_z(3))
    return Ring(src, bufs, sems, x, at_x(1), at_x(3))


def one_scratch(w):
    return [pltpu.VMEM((2, 2, 64, w), F32)] * 3 + [pltpu.SemaphoreType.DMA((2, 6))]


def two_scratch(w):
    return [
        *[pltpu.VMEM((2, 32, w), F32)] * 3,
        pltpu.VMEM((64, w), F32),
        pltpu.VMEM((32, w), F32),
        pltpu.SemaphoreType.DMA((2, 6)),
        pltpu.SemaphoreType.DMA((2,)),
    ]


def params(n):
    return pltpu.CompilerParams(
        collective_id=n, has_side_effects=True, vmem_limit_bytes=63 * 1024 * 1024
    )


def block_probs(q, k):
    r, s = iota((128, 128), 0), iota((128, 128), 1)
    seen = ((r // STEPS) == (s // STEPS)) & (r >= s)
    weights = jnp.where(seen, jnp.exp(dot(q, k, (1, 1)) * SCALE), 0.0)
    return weights / jnp.sum(weights, axis=-1, keepdims=True)


def policy_kernel(
    token_total,
    init_ref, act_ref, scale_ref, next_ref, rew_ref, obs_ref, gain_attn, wq_ref, wk_ref, wv_ref, wo_ref,
    gain_mlp, gain_fin, actor_ref, critic_ref, up_hbm, down_hbm,
    qkv_out, match_out, mixed_out, ht_out, down_out, low_one, gh_ref, g_fin, g_mlp, res_a, res_b,
    qkv_ref, match_ref, mixed_ref, ht_ref, flush_sem,
    r_init, r_act, r_scale, roll_sem, tables, st_ref, own_ref, head_f, heads,
    w_up, w_down, w_sem,
    p, near_own, near_far, far, whole, h_two, up_rows, hidden, low_two, d_up, x_one, dx_two, buf_a, buf_b,
    fin_ref, grad_up, grad_down, *rest,
):
    stats, rest = rest[:6], rest[6:]
    sems_a, sems_b, sems_d = rest[0:3], rest[3:6], rest[6:9]
    gs_b, gs_d, gs_e = rest[9:12], rest[12:15], rest[15:18]
    ring_a, ring_b = rest[18:22], rest[22:26]
    flushed = []

    def flush(src, dst):
        cp = pltpu.make_async_copy(src, dst, flush_sem.at[len(flushed)])
        cp.start()
        flushed.append(cp)

    d, m, c, l = place()
    weights = [
        pltpu.make_async_copy(up_hbm, w_up, w_sem.at[0]), pltpu.make_async_copy(down_hbm, w_down, w_sem.at[1]),
    ]
    for cp in weights:
        cp.start()
    xdev, zdev, ydev = stats_devices()
    greet(xdev + zdev + ydev)
    far_dev = partners()[2]
    copies = [
        remote(src, dst, roll_sem, (n,), far_dev)
        for n, (src, dst) in enumerate(((init_ref, r_init), (act_ref, r_act), (scale_ref, r_scale)))
    ]

    def table_rows(i):
        at = pl.ds(i, 32)
        x = obs_ref[at, :].astype(F32)
        ht_ref[at, :] = (x * inverse_rms(x) * gain_attn[...]).astype(BF16)

    by_blocks(256, 32, table_rows)
    flush(ht_ref, ht_out)
    for n, w in enumerate((wq_ref, wk_ref, wv_ref)):
        tables[:, n * 256 : (n + 1) * 256] = dot(ht_ref[...], w[...], (1, 0)).astype(BF16)
    head_f[...] = jnp.zeros_like(head_f)
    head_f[0:16, :] = actor_ref[...].astype(F32)
    head_f[16:17, :] = critic_ref[...].astype(F32)
    heads[...] = jnp.zeros_like(heads)
    heads[0:32, :] = head_f[...].astype(BF16)

    for cp in copies:
        cp.wait()
    swap = 32 + 64 * l
    lane = iota((1, 64), 1)
    state = jnp.where(lane >= swap, r_init[...], init_ref[...]).astype(F32)
    scale = jnp.where(lane >= swap, r_scale[...], scale_ref[...])
    act_t = jnp.where(iota((16, 64), 1) >= swap, r_act[...], act_ref[...]).astype(F32)
    nexts = next_ref[...].astype(F32).astype(BF16)
    ids, kinds = iota((256, 64), 0).astype(F32), iota((16, 64), 0).astype(F32)
    for t in range(STEPS):
        st_ref[pl.ds(t, 1), :] = state
        if t + 1 < STEPS:
            hit = jnp.where(ids == state, 1.0, 0.0).astype(BF16)
            found = dot(nexts, hit, (1, 0))
            state = jnp.sum(jnp.where(kinds == act_t[t : t + 1, :], found, 0.0), axis=0, keepdims=True)

    pick_t = (iota((128, 16), 0) % STEPS == iota((128, 16), 1)).astype(BF16)
    spread = jnp.ones((64, 128), BF16)
    lanes = iota((128, 128), 1).astype(F32)

    def per_token(rows_by_env, first_env):
        here = iota((128, 64), 1) == first_env + iota((128, 64), 0) // STEPS
        found = jnp.where(here, dot(pick_t, rows_by_env, (1, 0)), 0.0)
        return dot(found.astype(BF16), spread, (1, 0))

    def attend(core, low):
        def block(h, carry):
            at = rows(block_at(h, core, low), 128)
            ids_here = per_token(st_ref[...].astype(BF16), h * 32 + (core * 2 + low) * 8)
            match = jnp.concatenate(
                [jnp.where(ids_here == lanes, 1.0, 0.0), jnp.where(ids_here == lanes + 128.0, 1.0, 0.0)], axis=1
            ).astype(BF16)
            match_ref[at, :] = match
            qkv = dot(match, tables[...], (1, 0)).astype(BF16)
            qkv_ref[at, :] = qkv
            outs = []
            for n in range(2):
                q, k, v = (qkv[:, j * 256 + n * 128 : j * 256 + (n + 1) * 128] for j in range(3))
                outs.append(dot(block_probs(q, k).astype(BF16), v, (1, 0)).astype(BF16))
            mixed = jnp.concatenate(outs, axis=1)
            mixed_ref[at, :] = mixed
            p[at, :] = dot(mixed, wo_ref[...], (1, 0))
            return carry

        lax.fori_loop(0, 2, block, 0)

    sums = Sums(p, near_own, near_far, far, sems_a)
    attend(1 - c, 1 - l)
    sums.give_far(0)
    sums.give_far(1)
    attend(c, 1 - l)
    sums.pass_far(0)
    sums.pass_far(1)
    attend(1 - c, l)
    sums.give_own()
    attend(c, l)
    flush(qkv_ref, qkv_out)
    flush(match_ref, match_out)
    flush(mixed_ref, mixed_out)
    for h in range(2):
        at = pl.ds(h * 128, 128)
        mine = match_ref[rows(block_at(h, c, l), 128), :]
        x_one[at, :] = dot(mine, obs_ref[...], (1, 0))
        first_env = h * 32 + (c * 2 + l) * 8
        chosen = jnp.where(per_token(act_t.astype(BF16), first_env) == lanes, 1.0, 0.0)
        found = dot(mine.astype(F32), rew_ref[...], (1, 1), precision=lax.Precision.HIGHEST)
        here = iota((128, 64), 1) == first_env + iota((128, 64), 0) // STEPS
        factor = jnp.sum(jnp.where(here, scale, 0.0), axis=1, keepdims=True)
        reward = jnp.sum(chosen[:, :16] * found, axis=1, keepdims=True) * factor
        own_ref[at, :] = jnp.where(lanes == 16.0, reward, chosen)
    sums.take_own()

    gather = Gather(buf_a, whole, h_two, gs_b)
    for h, k in CHUNKS:
        sums.take(h, k)

        def body(i, h=h, k=k):
            at = pl.ds(h * 128 + k * 64 + i, 32)
            x = sums.value(h, k, i) + x_one[at, :]
            x_one[at, :] = x
            buf_a[at, :] = x * inverse_rms(x) * gain_mlp[...]

        by_blocks(64, 32, body)
        gather.send(h, k)
    sums.drain()
    for cp in weights:
        cp.wait()

    def forward(spans):
        def up(j):
            cols = pl.ds(j, WIDE)
            u = dot(spans_of(h_two, spans), w_up[:, cols], (1, 0))
            put_spans(up_rows, spans, cols, u)
            put_spans(hidden, spans, cols, (u / (1.0 + jnp.exp(-u))).astype(BF16))

        def down(j):
            cols = pl.ds(j, WIDE)
            put_spans(p, spans, cols, dot(spans_of(hidden, spans), w_down[:, cols], (1, 0)))

        by_blocks(1024, WIDE, up)
        by_blocks(1024, WIDE, down)

    sums = Sums(p, near_own, near_far, far, sems_b)
    gather_work_sum(gather, sums, forward)
    for h, k in CHUNKS:
        sums.take(h, k)

        def body(i, h=h, k=k):
            at = pl.ds(h * 128 + k * 64 + i, 32)
            x = sums.value(h, k, i) + x_one[at, :]
            buf_b[at, :] = x
            fin_ref[at, :] = (x * inverse_rms(x) * gain_fin[...]).astype(BF16)

        by_blocks(64, 32, body)
    gather.drain()
    sums.drain()

    lane = iota((256, 128), 1)
    both = dot(fin_ref[...], heads[...], (1, 1))
    critic = jnp.sum(jnp.where(lane == 16, both, 0.0), axis=1, keepdims=True)
    own = own_ref[...]
    reward = jnp.sum(jnp.where(lane == 16, own, 0.0), axis=1, keepdims=True)
    step = iota((256, 128), 0) % STEPS
    base = reward + jnp.where(step == STEPS - 1, GAMMA * critic, 0.0)
    r, s = iota((256, 256), 0), iota((256, 256), 1)
    ahead = ((r // STEPS) == (s // STEPS)) & (s >= r)
    decay = jnp.where(ahead, jnp.exp((s - r).astype(F32) * math.log(GAMMA)), 0.0)
    returns = dot(decay, base, (1, 0), precision=lax.Precision.HIGHEST)
    advantage = returns - critic
    tile = jnp.where(
        iota((8, 128), 0) == 0,
        jnp.sum(advantage, axis=0, keepdims=True),
        jnp.sum(advantage * advantage, axis=0, keepdims=True),
    )
    totals = sum_everywhere(tile, *stats)
    mean = totals[0:1, :] * (1.0 / token_total)
    variance = totals[1:2, :] * (1.0 / token_total) - mean * mean
    normed = (advantage - mean) * lax.rsqrt(variance + EPS)
    real = lane < 16
    logits = jnp.where(real, both, 0.0)
    mass = jnp.sum(jnp.where(real, jnp.exp(logits), 0.0), axis=1, keepdims=True)
    logp = jnp.where(real, logits - jnp.log(mass), 0.0)
    chance = jnp.where(real, jnp.exp(logp), 0.0)
    entropy = -jnp.sum(chance * logp, axis=1, keepdims=True)
    factor = 1.0 / math.sqrt(token_total)
    picked = jnp.where(real, own, 0.0)
    d_logits = factor * (-normed * (picked - chance) + ENTROPY_COEF * chance * (logp + entropy))
    d_value = (factor * VALUE_COEF) * (critic - returns)
    d_both = jnp.where(real, d_logits, jnp.where(lane == 16, d_value, 0.0)).astype(BF16)
    buf_a[...] = dot(d_both, heads[...], (1, 0))
    g_fin[...] = jnp.zeros_like(g_fin)
    g_mlp[...] = jnp.zeros_like(g_mlp)

    gather = Gather(dx_two, whole, low_two, gs_d)
    for h, k in CHUNKS:

        def body(i, h=h, k=k):
            at = pl.ds(h * 128 + k * 64 + i, 32)
            x, up = buf_b[at, :], buf_a[at, :]
            inv = inverse_rms(x)
            dx_two[at, :] = norm_back(x, inv, gain_fin[...], up)
            g_fin[...] += fold8(up * x * inv)

        by_blocks(64, 32, body)
        gather.send(h, k)
    gh_ref[...] = dot(fin_ref[...], d_both, (0, 0))

    def backward(spans):
        def up(j):
            cols = pl.ds(j, WIDE)
            d_hidden = dot(spans_of(low_two, spans), w_down[cols, :], (1, 1)).astype(BF16).astype(F32)
            u = spans_of(up_rows, spans, cols)
            sig = 1.0 / (1.0 + jnp.exp(-u))
            put_spans(d_up, spans, cols, (d_hidden * sig * (1.0 + u * (1.0 - sig))).astype(BF16))

        def down(j):
            cols = pl.ds(j, WIDE)
            put_spans(p, spans, cols, dot(spans_of(d_up, spans), w_up[cols, :], (1, 1)))

        by_blocks(1024, WIDE, up)
        by_blocks(1024, WIDE, down)

    sums = Sums(p, near_own, near_far, far, sems_d)
    gather_work_sum(gather, sums, backward)

    def weight_grad(out, left, right):
        def tile(j, carry):
            cols = rows(j * 256, 256)
            out[j] = dot(left[:, cols], right[...], (0, 0)).reshape(4, 64, 1024)
            return carry

        lax.fori_loop(0, 4, tile, 0)

    rings = [
        ring_one("xz", grad_up, ring_a[:3], ring_a[3], pl.ds(0, 512)),
        ring_one("zx", grad_up, ring_b[:3], ring_b[3], pl.ds(512, 512)),
    ]
    weight_grad(grad_up, h_two, d_up)
    for ring in rings:
        ring.start()
    weight_grad(grad_down, low_two, hidden)
    flush(grad_down, down_out)
    gather.drain()

    gather = Gather(buf_b, whole, low_one, gs_e)
    for h, k in CHUNKS:
        sums.take(h, k)

        def body(i, h=h, k=k):
            at = pl.ds(h * 128 + k * 64 + i, 32)
            up, x = sums.value(h, k, i), x_one[at, :]
            inv = inverse_rms(x)
            buf_b[at, :] = dx_two[at, :] + norm_back(x, inv, gain_mlp[...], up)
            g_mlp[...] += fold8(up * x * inv)

        by_blocks(64, 32, body)
        gather.send(h, k)
    sums.drain()
    for h, k in CHUNKS:
        gather.take_core(h, k)
    for h in range(2):
        gather.take_far(h, 0)
    for ring in rings:
        ring.middle()
    for h in range(2):
        gather.take_far(h, 1)
    for h, k in CHUNKS:
        gather.take_fwd(h, k)
    gather.drain()
    for ring, res in zip(rings, (res_a, res_b)):
        ring.finish(lambda h, res=res: res.at[pl.ds(h * 2, 2)])
    for ring in rings:
        ring.drain()
    for cp in flushed:
        cp.wait()


def policy(token_total, *args):
    sd, vm = jax.ShapeDtypeStruct, pltpu.VMEM
    return pl.pallas_call(
        functools.partial(policy_kernel, token_total),
        out_shape=(
            sd((1024, 768), BF16), sd((1024, 256), BF16), sd((1024, 256), BF16), sd((256, 1024), BF16),
            sd((4, 4, 64, 1024), F32), sd((1024, 1024), BF16), sd((1024, 128), F32), sd((8, 1024), F32),
            sd((8, 1024), F32), sd((4, 64, 512), F32), sd((4, 64, 512), F32),
        ),
        in_specs=[VMEM] * 15 + [ANY] * 2,
        out_specs=tuple([ANY] * 5 + [VMEM] * 6),
        scratch_shapes=[
            vm((1024, 768), BF16), vm((1024, 256), BF16), vm((1024, 256), BF16), vm((256, 1024), BF16),
            pltpu.SemaphoreType.DMA((5,)),
            vm((1, 64), jnp.int32), vm((16, 64), jnp.int32), vm((1, 64), F32), pltpu.SemaphoreType.DMA((2, 3)),
            vm((256, 768), BF16), vm((16, 64), F32), vm((256, 128), F32), vm((32, 1024), F32), vm((128, 1024), BF16),
            vm((1024, 1024), BF16), vm((1024, 1024), BF16), pltpu.SemaphoreType.DMA((2,)),
            vm((1024, 1024), F32), vm((2, 128, 1024), F32), vm((2, 2, 64, 1024), F32), vm((2, 2, 64, 1024), F32),
            vm((1024, 1024), F32), vm((1024, 1024), BF16), vm((1024, 1024), F32), vm((1024, 1024), BF16),
            vm((1024, 1024), BF16), vm((1024, 1024), BF16),
            vm((256, 1024), F32), vm((256, 1024), F32), vm((256, 1024), F32), vm((256, 1024), F32),
            vm((256, 1024), BF16), vm((4, 4, 64, 1024), F32), vm((4, 4, 64, 1024), F32),
            *STATS_SCRATCH, *SUM_SEMS, *SUM_SEMS, *SUM_SEMS, *GATHER_SEMS, *GATHER_SEMS, *GATHER_SEMS,
            *one_scratch(512), *one_scratch(512),
        ],
        compiler_params=params(1),
        name="policy",
    )(*args)


def halves(value):
    high = value.astype(BF16)
    return high, (value - high.astype(F32)).astype(BF16)


UP_A, UP_B, DOWN_A, DOWN_B, OUT, QK, VALUE, SMALL = range(8)
ORDER = ("xz", "zx", "xz", "zx", "zx", "xz", "zx", "xz")
WIDTH = (512, 512, 512, 512, 256, 512, 256, 128)
LOADS = ((4, 4, 64, 1024), F32), ((1024, 1024), BF16), ((1024, 256), BF16), ((256, 1024), BF16), \
    ((1024, 768), BF16), ((1024, 256), BF16), ((256, 1024), BF16), ((256, 1024), BF16), \
    ((1024, 256), BF16), ((1024, 256), BF16), ((1024, 256), BF16), ((1024, 128), F32), \
    ((8, 1024), F32), ((8, 1024), F32), ((4, 64, 512), F32), ((4, 64, 512), F32)


def tail_kernel(*refs):
    n = len(LOADS)
    hbm, outs, held, rest = refs[:n], refs[n : n + 8], refs[n + 8 : 2 * n + 8], refs[2 * n + 8 :]
    load_sem, qk_ref, v_ref, out_ref, sums, dt_ref, vec_ref, mp_buf, mp_sem = rest[:9]
    rest = rest[9:]
    down_ref, dx_ref, mixed_ref, wo_ref, qkv_ref, match_ref, ht_ref, obs_ref = held[:8]
    wq_ref, wk_ref, wv_ref, small_ref, gf_ref, gm_ref, res_a, res_b = held[8:]
    loads = [pltpu.make_async_copy(a, b, load_sem.at[k]) for k, (a, b) in enumerate(zip(hbm, held))]
    for k in (14, 15, 0, *range(1, 14)):
        loads[k].start()
    d, m, c, l = place()
    x, z, yh = axes_place()
    yother = (d + 1 - 2 * yh, m)
    peers = [(d, lax.rem(m + j, 4)) for j in (1, 2, 3)]
    greet([at_x(1), at_x(3), at_z(1), at_z(3), yother] + peers)

    first, second, results, ends = {}, [], [res_a, res_b], []
    sources = {
        DOWN_A: (down_ref, pl.ds(0, 512)), DOWN_B: (down_ref, pl.ds(512, 512)), OUT: (out_ref, slice(None)),
        QK: (qk_ref, slice(None)), VALUE: (v_ref, slice(None)), SMALL: (small_ref, slice(None)),
    }
    for i in range(2, 8):
        mid, fl, fr, sems, res = rest[:5]
        rest = rest[5:]
        src, cols = sources[i]
        if i == SMALL:
            src = rest[0]
            small4 = src
            rest = rest[1:]
        first[i] = ring_one(ORDER[i], src, (mid, fl, fr), sems, cols)
        results.append(res)
    for i in range(8):
        mid, fl, fr, res, ybuf, sems, ysem = rest[:7]
        rest = rest[7:]
        second.append(ring_two(ORDER[i], results[i], (mid, fl, fr), sems))
        ends.append((res, ybuf, ysem))
    tails = {}

    def turn(i):
        first[i].finish(lambda h: results[i].at[pl.ds(h * 2, 2)])
        second[i].start()

    def send_tail(i):
        res, ybuf, ysem = ends[i]
        second[i].finish(lambda h: res.at[pl.ds(h * 32, 32)])
        tails[i] = remote(res.at[rows((1 - yh) * 32, 32)], ybuf, ysem, (), yother)

    loads[14].wait()
    loads[15].wait()
    second[UP_A].start()
    second[UP_B].start()
    loads[0].wait()
    first[DOWN_A].start()
    first[DOWN_B].start()
    for k in range(1, 14):
        loads[k].wait()

    def out_tile(j, carry):
        cols = rows(j * 256, 256)
        out_ref[j] = dot(dx_ref[:, cols], mixed_ref[...], (0, 0)).reshape(4, 64, 256)
        return carry

    lax.fori_loop(0, 4, out_tile, 0)
    first[OUT].start()
    sums[...] = jnp.zeros_like(sums)

    def block(b, carry):
        at = rows(b * 128, 128)
        d_mixed = dot(dx_ref[at, :], wo_ref[...], (1, 1)).astype(BF16)
        qkv = qkv_ref[at, :]
        parts = [[], [], []]
        for h in range(2):
            q, k, v = (qkv[:, n * 256 + h * 128 : n * 256 + (h + 1) * 128] for n in range(3))
            up = d_mixed[:, h * 128 : (h + 1) * 128]
            probs = block_probs(q, k)
            d_probs = dot(up, v, (1, 1))
            parts[2].append(dot(probs.astype(BF16), up, (0, 0)).astype(BF16))
            d_scores = (
                probs * (d_probs - jnp.sum(probs * d_probs, axis=-1, keepdims=True)) * SCALE
            ).astype(BF16)
            parts[0].append(dot(d_scores, k, (1, 0)).astype(BF16))
            parts[1].append(dot(d_scores, q, (0, 0)).astype(BF16))
        d_qkv = jnp.concatenate([*parts[0], *parts[1], *parts[2]], axis=1)
        sums[...] += dot(match_ref[at, :], d_qkv, (0, 0))
        return carry

    lax.fori_loop(0, 4, block, 0)
    for i in (UP_A, UP_B):
        second[i].middle()
    for i in (DOWN_A, DOWN_B):
        first[i].middle()
    lax.fori_loop(4, 8, block, 0)
    high, low = halves(sums[...])

    def grad_tile(j, carry):
        cols = rows(j * 256, 256)
        table = ht_ref[:, cols]
        total = dot(table, high, (0, 0)) + dot(table, low, (0, 0))
        qk_ref[j] = total[:, :512].reshape(4, 64, 512)
        v_ref[j] = total[:, 512:].reshape(4, 64, 256)
        return carry

    lax.fori_loop(0, 4, grad_tile, 0)
    first[QK].start()
    first[VALUE].start()
    dt_ref[...] = jnp.zeros_like(dt_ref)
    for n, w in enumerate((wq_ref, wk_ref, wv_ref)):
        cols = slice(n * 256, (n + 1) * 256)
        dt_ref[...] += dot(high[:, cols], w[...], (1, 1)) + dot(low[:, cols], w[...], (1, 1))
    vec_ref[0:8] = gf_ref[...]
    vec_ref[8:16] = gm_ref[...]
    vec_ref[16:32] = jnp.zeros((16, 1024), F32)

    def gain_rows(i):
        at = pl.ds(i, 32)
        x = obs_ref[at, :].astype(F32)
        vec_ref[16:24] += fold8(dt_ref[at, :] * x * inverse_rms(x))

    by_blocks(256, 32, gain_rows)
    place_at = (iota((32, 128), 1) == 17 + iota((32, 128), 0) // 8).astype(BF16)
    vec = vec_ref[...]
    high, low = halves(vec)
    lowest = (vec - high.astype(F32) - low.astype(F32)).astype(BF16)
    small = small_ref[...] + sum(dot(part, place_at, (0, 0)) for part in (high, low, lowest))
    small4[...] = small.reshape(4, 4, 64, 128)
    first[SMALL].start()

    first[OUT].middle()
    send_tail(UP_A)
    send_tail(UP_B)
    turn(DOWN_A)
    turn(DOWN_B)
    for i in (QK, VALUE, SMALL):
        first[i].middle()
    turn(OUT)
    second[DOWN_A].middle()
    second[DOWN_B].middle()
    for i in (QK, VALUE, SMALL):
        turn(i)
    send_tail(DOWN_A)
    send_tail(DOWN_B)
    second[OUT].middle()
    for i in (QK, VALUE, SMALL):
        second[i].middle()
    for i in (OUT, SMALL, QK, VALUE):
        send_tail(i)

    def total(i, put):
        res, ybuf, _ = ends[i]
        by_blocks(32, 8, lambda k: put(k, res[rows(yh * 32 + k, 8), :] + ybuf[pl.ds(k, 8), :]))

    def to_out(ref):
        def put(k, value):
            ref[pl.ds(k, 8), :] = value

        return put

    def to_mp(k, value):
        mp_buf[m, pl.ds(k, 8), :] = value

    shares = []
    for i in (UP_A, UP_B, DOWN_A, DOWN_B, OUT, SMALL, QK, VALUE):
        tails[i].wait_recv()
        if i == SMALL:
            total(i, to_mp)
            shares = [remote(mp_buf.at[m], mp_buf.at[m], mp_sem, (j,), dev) for j, dev in enumerate(peers)]
        else:
            total(i, to_out(outs[i]))
    for cp in shares:
        cp.wait_recv()
    outs[SMALL][...] = mp_buf[0] + mp_buf[1] + mp_buf[2] + mp_buf[3]
    for cp in [*shares, *tails.values()]:
        cp.wait_send()
    for ring in [*first.values(), *second]:
        ring.drain()


def tail(*args):
    vm, dma = pltpu.VMEM, pltpu.SemaphoreType.DMA
    scratch = [vm(shape, kind) for shape, kind in LOADS]
    scratch += [
        dma((len(LOADS),)), vm((4, 4, 64, 512), F32), vm((4, 4, 64, 256), F32), vm((4, 4, 64, 256), F32),
        vm((256, 768), F32), vm((256, 1024), F32), vm((32, 1024), F32), vm((4, 32, 128), F32), dma((2, 3)),
    ]
    for i in range(2, 8):
        scratch += one_scratch(WIDTH[i]) + [vm((4, 64, WIDTH[i]), F32)]
        if i == SMALL:
            scratch += [vm((4, 4, 64, 128), F32)]
    for i in range(8):
        scratch += two_scratch(WIDTH[i])
    return pl.pallas_call(
        tail_kernel,
        out_shape=tuple(jax.ShapeDtypeStruct((32, w), F32) for w in WIDTH),
        in_specs=[ANY] * len(LOADS),
        out_specs=tuple([VMEM] * 8),
        scratch_shapes=scratch,
        compiler_params=params(2),
        name="tail",
    )(*args)


def write_kernel(
    up_a, up_b, down_a, down_b, out_ref, qk_ref, value_ref, small_ref,
    o_q, o_k, o_v, o_out, o_up, o_down, o_actor, o_critic, o_final, o_mlp, o_attn,
):
    o_q[...] = qk_ref[:, :256]
    o_k[...] = qk_ref[:, 256:]
    o_v[...] = value_ref[...]
    o_up[:, :512] = up_a[...]
    o_up[:, 512:] = up_b[...]
    o_out[...] = out_ref[...]
    o_down[:, :512] = down_a[...]
    o_down[:, 512:] = down_b[...]
    flat = jnp.transpose(small_ref[...])
    o_actor[...] = flat[:16, :]
    o_critic[...] = flat[16:17, :]
    o_final[...] = flat[17:18, :]
    o_mlp[...] = flat[18:19, :]
    own = jnp.transpose(small_ref[rows(lax.axis_index("mp") * 8, 8), :])
    o_attn[...] = own[19:20, :]


def write_outputs(*parts):
    sd = jax.ShapeDtypeStruct
    shapes = [(32, 256)] * 4 + [(32, 1024)] * 2 + [(16, 32)] + [(1, 32)] * 3 + [(1, 8)]
    return pl.pallas_call(
        write_kernel,
        out_shape=tuple(sd(shape, F32) for shape in shapes),
        in_specs=[VMEM] * 8,
        out_specs=tuple([VMEM] * 11),
        name="write_outputs",
    )(*parts)


def per_device(
    initial_state,
    actions,
    next_state,
    reward_table,
    reward_scale,
    observe_table,
    gain_attn,
    w_query,
    w_key,
    w_value,
    w_out,
    gain_mlp,
    w_up,
    w_down,
    gain_final,
    actor_head,
    critic_head,
):
    token_total = actions.size * lax.axis_size("dp")

    def line(vector):
        return vector.reshape(1, -1)

    qkv, match, mixed, h_table, grad_down, dx_one_low, grad_heads, final_terms, mlp_terms, res_a, res_b = policy(
        token_total,
        line(initial_state), actions.T, line(reward_scale), next_state.T, reward_table.T, observe_table,
        line(gain_attn), w_query, w_key, w_value, w_out, line(gain_mlp), line(gain_final),
        actor_head.T, line(critic_head), w_up, w_down,
    )
    parts = tail(
        grad_down, dx_one_low, mixed, w_out, qkv, match, h_table, observe_table, w_query, w_key, w_value,
        grad_heads, final_terms, mlp_terms, res_a, res_b,
    )
    q, k, v, out, up, down, actor, critic, final, mlp, attn = write_outputs(*parts)
    return (
        q, k, v, out.T, up, down.T, attn.reshape(-1), mlp.reshape(-1), final.reshape(-1), actor.T,
        critic.reshape(-1),
    )


def solution(mesh):
    return jax.shard_map(
        per_device,
        mesh=mesh,
        in_specs=(
            P("dp"),
            P("dp", None),
            P(),
            P(),
            P("dp"),
            P(),
            P(),
            P(None, "mp"),
            P(None, "mp"),
            P(None, "mp"),
            P("mp", None),
            P(),
            P(None, "mp"),
            P("mp", None),
            P(),
            P(),
            P(),
        ),
        out_specs=(
            P("dp", "mp"),
            P("dp", "mp"),
            P("dp", "mp"),
            P("mp", "dp"),
            P("dp", "mp"),
            P("mp", "dp"),
            P(("dp", "mp")),
            P("dp"),
            P("dp"),
            P("dp", None),
            P("dp"),
        ),
        check_vma=False,
    )
```

```python
import functools
import math

import jax
import jax.numpy as jnp
from jax import lax
from jax.experimental import pallas as pl
from jax.experimental.pallas import tpu as pltpu
from jax.sharding import PartitionSpec as P

HEAD_DIM = 128
STEPS = 16
EPS = 1e-05
GAMMA = 0.9
VALUE_COEF = 0.5
ENTROPY_COEF = 0.1
SCALE = 1.0 / math.sqrt(HEAD_DIM)
MESH = pl.DeviceIdType.MESH
VMEM = pl.BlockSpec(memory_space=pltpu.VMEM)
WIDE = 1024
ANY = pl.BlockSpec(memory_space=pl.ANY)
F32 = jnp.float32
BF16 = jnp.bfloat16


def place():
    d, m = lax.axis_index("dp"), lax.axis_index("mp")
    return d, m, m % 2, m // 2


def axes_place():
    d, m, c, l = place()
    return d // 8, (d // 2) % 4, d % 2


def partners():
    d, m, c, l = place()
    over = m + 2 - 4 * l
    return (d, m + 1 - 2 * c), (d, over), (d + 1 - 2 * (d % 2), over)


def at_x(k):
    d, m, c, l = place()
    x, z, yh = axes_place()
    return (lax.rem(x + k, 4) * 8 + z * 2 + yh, m)


def at_z(k):
    d, m, c, l = place()
    x, z, yh = axes_place()
    return (x * 8 + lax.rem(z + k, 4) * 2 + yh, m)


def stats_devices():
    d, m, c, l = place()
    x, z, yh = axes_place()
    plane, column = [], []
    for j in range(1, 16):
        other = lax.rem(x * 4 + z + j, 16)
        plane.append(((other // 4) * 8 + (other % 4) * 2 + yh, m))
    for j in range(1, 8):
        other = lax.rem(yh * 4 + m + j, 8)
        column.append((x * 8 + z * 2 + other // 4, other % 4))
    return plane, column


def greet(devices):
    barrier = pltpu.get_barrier_semaphore()
    for dev in devices:
        pl.semaphore_signal(barrier, inc=1, device_id=dev, device_id_type=MESH)
    pl.semaphore_wait(barrier, len(devices))


def remote(src, dst, sems, at, dev):
    cp = pltpu.make_async_remote_copy(
        src_ref=src, dst_ref=dst, send_sem=sems.at[(0, *at)], recv_sem=sems.at[(1, *at)],
        device_id=dev, device_id_type=MESH,
    )
    cp.start()
    return cp


def rows(start, size):
    return pl.ds(pl.multiple_of(start, size), size)


def by_blocks(total, block, body):
    lax.fori_loop(0, total // block, lambda i, z: (body(pl.multiple_of(i * block, block)), z)[1], 0)


def dot(left, right, contract, **kw):
    return lax.dot_general(
        left, right, ((contract[:1], contract[1:]), ((), ())), preferred_element_type=F32, **kw
    )


def iota(shape, axis):
    return lax.broadcasted_iota(jnp.int32, shape, axis)


def fold8(term):
    total = term[0:8]
    for k in range(1, term.shape[0] // 8):
        total = total + term[8 * k : 8 * k + 8]
    return total


def inverse_rms(x):
    return lax.rsqrt(jnp.mean(x * x, axis=-1, keepdims=True) + EPS)


def norm_back(x, inv, gain, up):
    weighted = up * gain
    return inv * weighted - x * (inv * inv * inv) * jnp.mean(x * weighted, axis=-1, keepdims=True)


def block_at(h, core, low):
    return h * 512 + core * 256 + low * 128


CHUNKS = [(h, k) for k in range(2) for h in range(2)]


class Sums:
    def __init__(self, p, near_own, near_far, far, sems):
        d, m, self.c, self.l = place()
        self.core, *self.over = partners()
        self.p, self.near_own, self.near_far, self.far = p, near_own, near_far, far
        self.own_sem, self.near_sem, self.far_sem = sems
        self.own, self.near, self.sent = {}, {}, {}

    def give_own(self):
        for h in range(2):
            src = self.p.at[rows(block_at(h, 1 - self.c, self.l), 128)]
            self.own[h] = remote(src, self.near_own.at[h], self.own_sem, (h,), self.core)

    def give_far(self, k):
        for h in range(2):
            src = self.p.at[rows(block_at(h, 1 - self.c, 1 - self.l) + k * 64, 64)]
            self.near[h, k] = remote(src, self.near_far.at[h, k], self.near_sem, (h, k), self.core)

    def pass_far(self, k):
        for h in range(2):
            self.near[h, k].wait_recv()
            base = block_at(h, self.c, 1 - self.l) + k * 64

            def body(i, h=h, base=base):
                self.near_far[h, k, pl.ds(i, 32), :] += self.p[rows(base + i, 32), :]

            by_blocks(64, 32, body)
            self.sent[h, k] = remote(
                self.near_far.at[h, k], self.far.at[h, k], self.far_sem, (h, k), self.over[h]
            )

    def take_own(self):
        for h in range(2):
            self.own[h].wait_recv()

    def take(self, h, k):
        self.sent[h, k].wait_recv()

    def value(self, h, k, i):
        mine = self.p[rows(block_at(h, self.c, self.l) + k * 64 + i, 32), :]
        return mine + self.near_own[h, pl.ds(k * 64 + i, 32), :] + self.far[h, k, pl.ds(i, 32), :]

    def drain(self):
        for group in (self.own, self.near, self.sent):
            for cp in group.values():
                cp.wait_send()


class Gather:
    def __init__(self, q, whole, low, sems):
        d, m, self.c, self.l = place()
        self.core, *self.over = partners()
        self.q, self.whole, self.low = q, whole, low
        self.over_sem, self.core_sem, self.fwd_sem = sems
        self.far, self.near, self.fwd, self.left = {}, {}, {}, set()

    def keep(self, base, src=None, at=0):
        def body(i):
            value = self.whole[rows(base + i, 32), :] if src is None else src[pl.ds(at + i, 32), :]
            self.low[rows(base + i, 32), :] = value.astype(BF16)

        by_blocks(64, 32, body)

    def send(self, h, k):
        base = block_at(h, self.c, self.l) + k * 64
        src, dst = self.q.at[pl.ds(h * 128 + k * 64, 64)], self.whole.at[rows(base, 64)]
        self.far[h, k] = remote(src, dst, self.over_sem, (h, k), self.over[h])
        self.near[h, k] = remote(src, dst, self.core_sem, (h, k), self.core)
        self.keep(base, self.q, h * 128 + k * 64)

    def take_core(self, h, k):
        self.near[h, k].wait_recv()
        self.keep(block_at(h, 1 - self.c, self.l) + k * 64)

    def take_far(self, h, k):
        self.far[h, k].wait_recv()
        base = block_at(h, self.c, 1 - self.l) + k * 64
        at = self.whole.at[rows(base, 64)]
        self.fwd[h, k] = remote(at, at, self.fwd_sem, (h, k), self.core)
        self.keep(base)

    def forwarded(self, k):
        for h in range(2):
            self.fwd[h, k].wait_send()
        self.left.add(k)

    def take_fwd(self, h, k):
        self.fwd[h, k].wait_recv()
        self.keep(block_at(h, 1 - self.c, 1 - self.l) + k * 64)

    def drain(self):
        late = [cp for (h, k), cp in self.fwd.items() if k not in self.left]
        for cp in [*self.far.values(), *self.near.values(), *late]:
            cp.wait_send()


SUM_SEMS = [
    pltpu.SemaphoreType.DMA((2, 2)), pltpu.SemaphoreType.DMA((2, 2, 2)), pltpu.SemaphoreType.DMA((2, 2, 2)),
]
GATHER_SEMS = [pltpu.SemaphoreType.DMA((2, 2, 2))] * 3


def gather_work_sum(gather, sums, work):
    c, l = sums.c, sums.l
    work([(block_at(h, c, l), 128) for h in range(2)])
    for h, k in CHUNKS:
        gather.take_core(h, k)
    work([(block_at(h, 1 - c, l), 128) for h in range(2)])
    sums.give_own()
    for k in range(2):
        for h in range(2):
            gather.take_far(h, k)
        work([(block_at(h, c, 1 - l) + k * 64, 64) for h in range(2)])
        for h in range(2):
            gather.take_fwd(h, k)
        work([(block_at(h, 1 - c, 1 - l) + k * 64, 64) for h in range(2)])
        sums.give_far(k)
        gather.forwarded(k)
        sums.pass_far(k)
    sums.take_own()


def spans_of(ref, spans, cols=slice(None)):
    return jnp.concatenate([ref[rows(at, n), cols] for at, n in spans], axis=0)


def put_spans(ref, spans, cols, value):
    done = 0
    for at, n in spans:
        ref[rows(at, n), cols] = value[done : done + n]
        done += n


def sum_everywhere(value, between, ps, cs, psem, csem):
    d, m, c, l = place()
    x, z, yh = axes_place()
    plane, column = stats_devices()

    def stage(slots, sems, devs, me, value, between=None):
        slots[me] = value
        copies = [remote(slots.at[me], slots.at[me], sems, (j,), dev) for j, dev in enumerate(devs)]
        done = between() if between is not None else None
        for cp in copies:
            cp.wait_recv()
        total = slots[0]
        for k in range(1, len(devs) + 1):
            total = total + slots[k]
        for cp in copies:
            cp.wait_send()
        return total, done

    value, done = stage(ps, psem, plane, x * 4 + z, value, between)
    return stage(cs, csem, column, yh * 4 + m, value)[0], done


STATS_SCRATCH = [
    pltpu.VMEM((16, 8, 128), F32),
    pltpu.VMEM((8, 8, 128), F32),
    pltpu.SemaphoreType.DMA((2, 15)),
    pltpu.SemaphoreType.DMA((2, 7)),
]


class Ring:
    def __init__(self, src, bufs, sems, pos, right, left):
        self.src, self.pos, self.right, self.left = src, pos, right, left
        self.mid, self.fl, self.fr = bufs
        self.sems = sems
        self.copies = []

    def send(self, src, dst, dev):
        self.copies.append(remote(src, dst, self.sems, (len(self.copies),), dev))

    def start(self):
        p = self.pos
        self.r, self.l, opp = lax.rem(p + 1, 4), lax.rem(p + 3, 4), lax.rem(p + 2, 4)
        self.send(self.src(opp, 0), self.mid.at[0], self.right)
        self.send(self.src(opp, 1), self.mid.at[1], self.left)
        self.send(self.src(self.r, 1), self.fl.at[1], self.right)
        self.send(self.src(self.l, 0), self.fr.at[0], self.left)

    def middle(self):
        self.copies[0].wait_recv()
        add_into(self.mid.at[0], self.src(self.r, 0))
        self.send(self.mid.at[0], self.fl.at[0], self.right)
        self.copies[1].wait_recv()
        add_into(self.mid.at[1], self.src(self.l, 1))
        self.send(self.mid.at[1], self.fr.at[1], self.left)

    def finish(self, out):
        for k in (2, 3, 4, 5):
            self.copies[k].wait_recv()
        for half in range(2):
            add_three(out(half), self.src(self.pos, half), self.fl.at[half], self.fr.at[half])

    def drain(self):
        for cp in self.copies:
            cp.wait_send()


def each_block(ref, body):
    n = min(16, ref.shape[-2])
    if len(ref.shape) == 3:
        for k in range(ref.shape[0]):
            by_blocks(ref.shape[1], n, lambda i, k=k: body((k, pl.ds(i, n), slice(None))))
    else:
        by_blocks(ref.shape[0], n, lambda i: body((pl.ds(i, n), slice(None))))


def add_into(dst, src):
    def body(at):
        dst[at] += src[at]

    each_block(dst, body)


def add_three(dst, a, b, c):
    def body(at):
        dst[at] = a[at] + b[at] + c[at]

    each_block(dst, body)


def ring_one(order, src, bufs, sems, cols=slice(None)):
    x, z, yh = axes_place()
    every = slice(None)
    if order == "xz":
        return Ring(lambda j, h: src.at[j, pl.ds(h * 2, 2), every, cols], bufs, sems, x, at_x(1), at_x(3))
    return Ring(lambda j, h: src.at[pl.ds(h * 2, 2), j, every, cols], bufs, sems, z, at_z(1), at_z(3))


def ring_two(order, res, bufs, sems):
    x, z, yh = axes_place()

    half = res.shape[1] // 2

    def src(j, h):
        return res.at[j, pl.ds(h * half, half)]

    if order == "xz":
        return Ring(src, bufs, sems, z, at_z(1), at_z(3))
    return Ring(src, bufs, sems, x, at_x(1), at_x(3))


def one_scratch(w, part=64):
    return [pltpu.VMEM((2, 2, part, w), F32)] * 3 + [pltpu.SemaphoreType.DMA((2, 6))]


def two_scratch(w, part=64, kept=32):
    return [
        *[pltpu.VMEM((2, part // 2, w), F32)] * 3,
        pltpu.VMEM((part, w), F32),
        pltpu.VMEM((kept, w), F32),
        pltpu.SemaphoreType.DMA((2, 6)),
        pltpu.SemaphoreType.DMA((2,)),
    ]


def params(n):
    return pltpu.CompilerParams(
        collective_id=n, has_side_effects=True, vmem_limit_bytes=63 * 1024 * 1024
    )


def block_probs(q, k):
    r, s = iota((128, 128), 0), iota((128, 128), 1)
    seen = ((r // STEPS) == (s // STEPS)) & (r >= s)
    weights = jnp.where(seen, jnp.exp(dot(q, k, (1, 1)) * SCALE), 0.0)
    return weights / jnp.sum(weights, axis=-1, keepdims=True)


def policy_kernel(
    token_total,
    init_ref, act_ref, scale_ref, next_ref, rew_ref, obs_ref, gain_attn, wq_ref, wk_ref, wv_ref, wo_ref,
    gain_mlp, gain_fin, actor_ref, critic_ref, up_hbm, down_hbm,
    qkv_out, match_out, mixed_out, ht_out, down_out, low_one, gh_ref, g_fin, g_mlp, res_a, res_b,
    qkv_ref, match_ref, mixed_ref, ht_ref, flush_sem,
    r_init, r_act, r_scale, roll_sem, tables, st_ref, own_ref, head_f, heads,
    w_up, w_down, w_sem,
    p, near_own, near_far, far, whole, h_two, up_rows, hidden, low_two, d_up, x_one, dx_two, buf_a, buf_b,
    fin_ref, grad_up, grad_down, *rest,
):
    stats, rest = rest[:4], rest[4:]
    sems_a, sems_b, sems_d = rest[0:3], rest[3:6], rest[6:9]
    gs_b, gs_d, gs_e = rest[9:12], rest[12:15], rest[15:18]
    ring_a, ring_b = rest[18:22], rest[22:26]
    flushed = []

    def flush(src, dst):
        cp = pltpu.make_async_copy(src, dst, flush_sem.at[len(flushed)])
        cp.start()
        flushed.append(cp)

    d, m, c, l = place()
    weights = [
        pltpu.make_async_copy(up_hbm, w_up, w_sem.at[0]), pltpu.make_async_copy(down_hbm, w_down, w_sem.at[1]),
    ]
    for cp in weights:
        cp.start()
    plane, column = stats_devices()
    greet(plane + column)
    far_dev = partners()[2]
    copies = [
        remote(src, dst, roll_sem, (n,), far_dev)
        for n, (src, dst) in enumerate(((init_ref, r_init), (act_ref, r_act), (scale_ref, r_scale)))
    ]

    def table_rows(i):
        at = pl.ds(i, 32)
        x = obs_ref[at, :].astype(F32)
        ht_ref[at, :] = (x * inverse_rms(x) * gain_attn[...]).astype(BF16)

    by_blocks(256, 32, table_rows)
    flush(ht_ref, ht_out)
    for n, w in enumerate((wq_ref, wk_ref, wv_ref)):
        tables[:, n * 256 : (n + 1) * 256] = dot(ht_ref[...], w[...], (1, 0)).astype(BF16)
    head_f[...] = jnp.zeros_like(head_f)
    head_f[0:16, :] = actor_ref[...].astype(F32)
    head_f[16:17, :] = critic_ref[...].astype(F32)
    heads[...] = jnp.zeros_like(heads)
    heads[0:32, :] = head_f[...].astype(BF16)

    for cp in copies:
        cp.wait()
    swap = 32 + 64 * l
    lane = iota((1, 64), 1)
    state = jnp.where(lane >= swap, r_init[...], init_ref[...]).astype(F32)
    scale = jnp.where(lane >= swap, r_scale[...], scale_ref[...])
    act_t = jnp.where(iota((16, 64), 1) >= swap, r_act[...], act_ref[...]).astype(F32)
    nexts = next_ref[...].astype(F32).astype(BF16)
    ids, kinds = iota((256, 64), 0).astype(F32), iota((16, 64), 0).astype(F32)
    for t in range(STEPS):
        st_ref[pl.ds(t, 1), :] = state
        if t + 1 < STEPS:
            hit = jnp.where(ids == state, 1.0, 0.0).astype(BF16)
            found = dot(nexts, hit, (1, 0))
            state = jnp.sum(jnp.where(kinds == act_t[t : t + 1, :], found, 0.0), axis=0, keepdims=True)

    pick_t = (iota((128, 16), 0) % STEPS == iota((128, 16), 1)).astype(BF16)
    spread = jnp.ones((64, 128), BF16)
    lanes = iota((128, 128), 1).astype(F32)

    def per_token(rows_by_env, first_env):
        here = iota((128, 64), 1) == first_env + iota((128, 64), 0) // STEPS
        found = jnp.where(here, dot(pick_t, rows_by_env, (1, 0)), 0.0)
        return dot(found.astype(BF16), spread, (1, 0))

    def attend(core, low):
        def block(h, carry):
            at = rows(block_at(h, core, low), 128)
            ids_here = per_token(st_ref[...].astype(BF16), h * 32 + (core * 2 + low) * 8)
            match = jnp.concatenate(
                [jnp.where(ids_here == lanes, 1.0, 0.0), jnp.where(ids_here == lanes + 128.0, 1.0, 0.0)], axis=1
            ).astype(BF16)
            match_ref[at, :] = match
            qkv = dot(match, tables[...], (1, 0)).astype(BF16)
            qkv_ref[at, :] = qkv
            outs = []
            for n in range(2):
                q, k, v = (qkv[:, j * 256 + n * 128 : j * 256 + (n + 1) * 128] for j in range(3))
                outs.append(dot(block_probs(q, k).astype(BF16), v, (1, 0)).astype(BF16))
            mixed = jnp.concatenate(outs, axis=1)
            mixed_ref[at, :] = mixed
            p[at, :] = dot(mixed, wo_ref[...], (1, 0))
            return carry

        lax.fori_loop(0, 2, block, 0, unroll=True)

    sums = Sums(p, near_own, near_far, far, sems_a)
    attend(1 - c, 1 - l)
    sums.give_far(0)
    sums.give_far(1)
    attend(c, 1 - l)
    sums.pass_far(0)
    sums.pass_far(1)
    attend(1 - c, l)
    sums.give_own()
    attend(c, l)
    flush(qkv_ref, qkv_out)
    flush(match_ref, match_out)
    flush(mixed_ref, mixed_out)
    for h in range(2):
        at = pl.ds(h * 128, 128)
        mine = match_ref[rows(block_at(h, c, l), 128), :]
        x_one[at, :] = dot(mine, obs_ref[...], (1, 0))
        first_env = h * 32 + (c * 2 + l) * 8
        chosen = jnp.where(per_token(act_t.astype(BF16), first_env) == lanes, 1.0, 0.0)
        found = dot(mine.astype(F32), rew_ref[...], (1, 1), precision=lax.Precision.HIGHEST)
        here = iota((128, 64), 1) == first_env + iota((128, 64), 0) // STEPS
        factor = jnp.sum(jnp.where(here, scale, 0.0), axis=1, keepdims=True)
        reward = jnp.sum(chosen[:, :16] * found, axis=1, keepdims=True) * factor
        own_ref[at, :] = jnp.where(lanes == 16.0, reward, chosen)
    sums.take_own()

    gather = Gather(buf_a, whole, h_two, gs_b)
    for h, k in CHUNKS:
        sums.take(h, k)

        def body(i, h=h, k=k):
            at = pl.ds(h * 128 + k * 64 + i, 32)
            x = sums.value(h, k, i) + x_one[at, :]
            x_one[at, :] = x
            buf_a[at, :] = x * inverse_rms(x) * gain_mlp[...]

        by_blocks(64, 32, body)
        gather.send(h, k)
    sums.drain()
    for cp in weights:
        cp.wait()

    def forward(spans):
        def up(j):
            cols = pl.ds(j, WIDE)
            u = dot(spans_of(h_two, spans), w_up[:, cols], (1, 0))
            put_spans(up_rows, spans, cols, u)
            put_spans(hidden, spans, cols, (u / (1.0 + jnp.exp(-u))).astype(BF16))

        def down(j):
            cols = pl.ds(j, WIDE)
            put_spans(p, spans, cols, dot(spans_of(hidden, spans), w_down[:, cols], (1, 0)))

        by_blocks(1024, WIDE, up)
        by_blocks(1024, WIDE, down)

    sums = Sums(p, near_own, near_far, far, sems_b)
    gather_work_sum(gather, sums, forward)
    for h, k in CHUNKS:
        sums.take(h, k)

        def body(i, h=h, k=k):
            at = pl.ds(h * 128 + k * 64 + i, 32)
            x = sums.value(h, k, i) + x_one[at, :]
            buf_b[at, :] = x
            fin_ref[at, :] = (x * inverse_rms(x) * gain_fin[...]).astype(BF16)

        by_blocks(64, 32, body)
    gather.drain()
    sums.drain()

    lane = iota((256, 128), 1)
    both = dot(fin_ref[...], heads[...], (1, 1))
    critic = jnp.sum(jnp.where(lane == 16, both, 0.0), axis=1, keepdims=True)
    own = own_ref[...]
    reward = jnp.sum(jnp.where(lane == 16, own, 0.0), axis=1, keepdims=True)
    step = iota((256, 128), 0) % STEPS
    base = reward + jnp.where(step == STEPS - 1, GAMMA * critic, 0.0)
    r, s = iota((256, 256), 0), iota((256, 256), 1)
    ahead = ((r // STEPS) == (s // STEPS)) & (s >= r)
    decay = jnp.where(ahead, jnp.exp((s - r).astype(F32) * math.log(GAMMA)), 0.0)
    returns = dot(decay, base, (1, 0), precision=lax.Precision.HIGHEST)
    advantage = returns - critic
    tile = jnp.where(
        iota((8, 128), 0) == 0,
        jnp.sum(advantage, axis=0, keepdims=True),
        jnp.sum(advantage * advantage, axis=0, keepdims=True),
    )
    real = lane < 16
    factor = 1.0 / math.sqrt(token_total)

    def policy_terms():
        logits = jnp.where(real, both, 0.0)
        mass = jnp.sum(jnp.where(real, jnp.exp(logits), 0.0), axis=1, keepdims=True)
        logp = jnp.where(real, logits - jnp.log(mass), 0.0)
        chance = jnp.where(real, jnp.exp(logp), 0.0)
        entropy = -jnp.sum(chance * logp, axis=1, keepdims=True)
        picked = jnp.where(real, own, 0.0)
        d_value = (factor * VALUE_COEF) * (critic - returns)
        return picked - chance, ENTROPY_COEF * chance * (logp + entropy), d_value

    totals, (push, calm, d_value) = sum_everywhere(tile, policy_terms, *stats)
    mean = totals[0:1, :] * (1.0 / token_total)
    variance = totals[1:2, :] * (1.0 / token_total) - mean * mean
    normed = (advantage - mean) * lax.rsqrt(variance + EPS)
    d_logits = factor * (-normed * push + calm)
    d_both = jnp.where(real, d_logits, jnp.where(lane == 16, d_value, 0.0)).astype(BF16)
    buf_a[...] = dot(d_both, heads[...], (1, 0))
    g_fin[...] = jnp.zeros_like(g_fin)
    g_mlp[...] = jnp.zeros_like(g_mlp)

    gather = Gather(dx_two, whole, low_two, gs_d)
    for h, k in CHUNKS:

        def body(i, h=h, k=k):
            at = pl.ds(h * 128 + k * 64 + i, 32)
            x, up = buf_b[at, :], buf_a[at, :]
            inv = inverse_rms(x)
            dx_two[at, :] = norm_back(x, inv, gain_fin[...], up)
            g_fin[...] += fold8(up * x * inv)

        by_blocks(64, 32, body)
        gather.send(h, k)
    gh_ref[...] = dot(fin_ref[...], d_both, (0, 0))

    def backward(spans):
        def up(j):
            cols = pl.ds(j, WIDE)
            d_hidden = dot(spans_of(low_two, spans), w_down[cols, :], (1, 1)).astype(BF16).astype(F32)
            u = spans_of(up_rows, spans, cols)
            sig = 1.0 / (1.0 + jnp.exp(-u))
            put_spans(d_up, spans, cols, (d_hidden * sig * (1.0 + u * (1.0 - sig))).astype(BF16))

        def down(j):
            cols = pl.ds(j, WIDE)
            put_spans(p, spans, cols, dot(spans_of(d_up, spans), w_up[cols, :], (1, 1)))

        by_blocks(1024, WIDE, up)
        by_blocks(1024, WIDE, down)

    sums = Sums(p, near_own, near_far, far, sems_d)
    gather_work_sum(gather, sums, backward)

    def weight_grad(out, left, right):
        def tile(j, carry):
            cols = rows(j * 256, 256)
            out[j] = dot(left[:, cols], right[...], (0, 0)).reshape(4, 64, 1024)
            return carry

        lax.fori_loop(0, 4, tile, 0)

    rings = [
        ring_one("xz", grad_up, ring_a[:3], ring_a[3], pl.ds(0, 512)),
        ring_one("zx", grad_up, ring_b[:3], ring_b[3], pl.ds(512, 512)),
    ]
    weight_grad(grad_up, h_two, d_up)
    for ring in rings:
        ring.start()
    weight_grad(grad_down, low_two, hidden)
    flush(grad_down, down_out)
    gather.drain()

    gather = Gather(buf_b, whole, low_one, gs_e)
    for h, k in CHUNKS:
        sums.take(h, k)

        def body(i, h=h, k=k):
            at = pl.ds(h * 128 + k * 64 + i, 32)
            up, x = sums.value(h, k, i), x_one[at, :]
            inv = inverse_rms(x)
            buf_b[at, :] = dx_two[at, :] + norm_back(x, inv, gain_mlp[...], up)
            g_mlp[...] += fold8(up * x * inv)

        by_blocks(64, 32, body)
        gather.send(h, k)
    sums.drain()
    for h, k in CHUNKS:
        gather.take_core(h, k)
    for h in range(2):
        gather.take_far(h, 0)
    for ring in rings:
        ring.middle()
    for h in range(2):
        gather.take_far(h, 1)
    for h, k in CHUNKS:
        gather.take_fwd(h, k)
    gather.drain()
    for ring, res in zip(rings, (res_a, res_b)):
        ring.finish(lambda h, res=res: res.at[pl.ds(h * 2, 2)])
    for ring in rings:
        ring.drain()
    for cp in flushed:
        cp.wait()


def policy(token_total, *args):
    sd, vm = jax.ShapeDtypeStruct, pltpu.VMEM
    return pl.pallas_call(
        functools.partial(policy_kernel, token_total),
        out_shape=(
            sd((1024, 768), BF16), sd((1024, 256), BF16), sd((1024, 256), BF16), sd((256, 1024), BF16),
            sd((4, 4, 64, 1024), F32), sd((1024, 1024), BF16), sd((1024, 128), F32), sd((8, 1024), F32),
            sd((8, 1024), F32), sd((4, 64, 512), F32), sd((4, 64, 512), F32),
        ),
        in_specs=[VMEM] * 15 + [ANY] * 2,
        out_specs=tuple([ANY] * 5 + [VMEM] * 6),
        scratch_shapes=[
            vm((1024, 768), BF16), vm((1024, 256), BF16), vm((1024, 256), BF16), vm((256, 1024), BF16),
            pltpu.SemaphoreType.DMA((5,)),
            vm((1, 64), jnp.int32), vm((16, 64), jnp.int32), vm((1, 64), F32), pltpu.SemaphoreType.DMA((2, 3)),
            vm((256, 768), BF16), vm((16, 64), F32), vm((256, 128), F32), vm((32, 1024), F32), vm((128, 1024), BF16),
            vm((1024, 1024), BF16), vm((1024, 1024), BF16), pltpu.SemaphoreType.DMA((2,)),
            vm((1024, 1024), F32), vm((2, 128, 1024), F32), vm((2, 2, 64, 1024), F32), vm((2, 2, 64, 1024), F32),
            vm((1024, 1024), F32), vm((1024, 1024), BF16), vm((1024, 1024), F32), vm((1024, 1024), BF16),
            vm((1024, 1024), BF16), vm((1024, 1024), BF16),
            vm((256, 1024), F32), vm((256, 1024), F32), vm((256, 1024), F32), vm((256, 1024), F32),
            vm((256, 1024), BF16), vm((4, 4, 64, 1024), F32), vm((4, 4, 64, 1024), F32),
            *STATS_SCRATCH, *SUM_SEMS, *SUM_SEMS, *SUM_SEMS, *GATHER_SEMS, *GATHER_SEMS, *GATHER_SEMS,
            *one_scratch(512), *one_scratch(512),
        ],
        compiler_params=params(1),
        name="policy",
    )(*args)


def halves(value):
    high = value.astype(BF16)
    return high, (value - high.astype(F32)).astype(BF16)


UP_A, UP_B, DOWN_A, DOWN_B, OUT, SMALL, SUM_A, SUM_B = range(8)
ORDER = ("xz", "zx", "xz", "zx", "zx", "xz", "xz", "zx")
WIDTH = (512, 512, 512, 512, 256, 128, 384, 384)
PART = (64, 64, 64, 64, 64, 64, 16, 16)
LOADS = ((4, 4, 64, 1024), F32), ((1024, 1024), BF16), ((1024, 256), BF16), ((256, 1024), BF16), \
    ((1024, 768), BF16), ((1024, 256), BF16), ((256, 1024), BF16), ((256, 1024), BF16), \
    ((1024, 256), BF16), ((1024, 256), BF16), ((1024, 256), BF16), ((1024, 128), F32), \
    ((8, 1024), F32), ((8, 1024), F32), ((4, 64, 512), F32), ((4, 64, 512), F32)


def tail_kernel(*refs):
    n = len(LOADS)
    hbm, outs, held, rest = refs[:n], refs[n : n + 7], refs[n + 7 : 2 * n + 7], refs[2 * n + 7 :]
    load_sem, out_ref, sums, sums4, full_a, full_b, near_sem, far_sem, mine_ref, dt_ref, vec_ref, small4, mp_buf, mp_sem = rest[:14]
    rest = rest[14:]
    down_ref, dx_ref, mixed_ref, wo_ref, qkv_ref, match_ref, ht_ref, obs_ref = held[:8]
    wq_ref, wk_ref, wv_ref, small_ref, gf_ref, gm_ref, res_a, res_b = held[8:]
    loads = [pltpu.make_async_copy(a, b, load_sem.at[k]) for k, (a, b) in enumerate(zip(hbm, held))]
    for k in (14, 15, 0, *range(1, 14)):
        loads[k].start()
    d, m, c, l = place()
    x, z, yh = axes_place()
    yother = (d + 1 - 2 * yh, m)
    peers = [(d, lax.rem(m + j, 4)) for j in (1, 2, 3)]
    greet([at_x(1), at_x(3), at_z(1), at_z(3), yother] + peers)

    first, second, results, ends = {}, [], [res_a, res_b], []
    sources = {
        DOWN_A: (down_ref, pl.ds(0, 512)), DOWN_B: (down_ref, pl.ds(512, 512)), OUT: (out_ref, slice(None)),
        SMALL: (small4, slice(None)), SUM_A: (sums4, pl.ds(0, 384)), SUM_B: (sums4, pl.ds(384, 384)),
    }
    for i in range(2, 8):
        mid, fl, fr, sems, res = rest[:5]
        rest = rest[5:]
        src, cols = sources[i]
        first[i] = ring_one(ORDER[i], src, (mid, fl, fr), sems, cols)
        results.append(res)
    for i in range(8):
        mid, fl, fr, res, ybuf, sems, ysem = rest[:7]
        rest = rest[7:]
        second.append(ring_two(ORDER[i], results[i], (mid, fl, fr), sems))
        ends.append((res, ybuf, ysem))
    tails = {}

    def turn(i):
        first[i].finish(lambda h: results[i].at[pl.ds(h * 2, 2)])
        second[i].start()

    def send_tail(i):
        res, ybuf, ysem = ends[i]
        half = res.shape[0] // 2
        second[i].finish(lambda h: res.at[pl.ds(h * half, half)])
        src = res if i in (SUM_A, SUM_B) else res.at[rows((1 - yh) * 32, 32)]
        tails[i] = remote(src, ybuf, ysem, (), yother)

    loads[14].wait()
    loads[15].wait()
    second[UP_A].start()
    second[UP_B].start()
    loads[0].wait()
    first[DOWN_A].start()
    first[DOWN_B].start()
    for k in range(1, 14):
        loads[k].wait()

    def out_tile(j, carry):
        cols = rows(j * 256, 256)
        out_ref[j] = dot(dx_ref[:, cols], mixed_ref[...], (0, 0)).reshape(4, 64, 256)
        return carry

    sums[...] = jnp.zeros_like(sums)

    def block(b, carry):
        at = rows(b * 128, 128)
        d_mixed = dot(dx_ref[at, :], wo_ref[...], (1, 1)).astype(BF16)
        qkv = qkv_ref[at, :]
        parts = [[], [], []]
        for h in range(2):
            q, k, v = (qkv[:, n * 256 + h * 128 : n * 256 + (h + 1) * 128] for n in range(3))
            up = d_mixed[:, h * 128 : (h + 1) * 128]
            probs = block_probs(q, k)
            d_probs = dot(up, v, (1, 1))
            parts[2].append(dot(probs.astype(BF16), up, (0, 0)).astype(BF16))
            d_scores = (
                probs * (d_probs - jnp.sum(probs * d_probs, axis=-1, keepdims=True)) * SCALE
            ).astype(BF16)
            parts[0].append(dot(d_scores, k, (1, 0)).astype(BF16))
            parts[1].append(dot(d_scores, q, (0, 0)).astype(BF16))
        d_qkv = jnp.concatenate([*parts[0], *parts[1], *parts[2]], axis=1)
        sums[...] += dot(match_ref[at, :], d_qkv, (0, 0))
        return carry

    def pair(b, carry):
        return block(2 * b + 1, block(2 * b, carry))

    lax.fori_loop(0, 2, pair, 0)
    for i in (UP_A, UP_B):
        second[i].middle()
    for i in (DOWN_A, DOWN_B):
        first[i].middle()
    lax.fori_loop(2, 4, pair, 0)
    sums4[...] = sums[...].reshape(4, 4, 16, 768)
    first[SUM_A].start()
    first[SUM_B].start()
    lax.fori_loop(0, 4, out_tile, 0)
    first[OUT].start()
    high, low = halves(sums[...])

    dt_ref[...] = jnp.zeros_like(dt_ref)
    for n, w in enumerate((wq_ref, wk_ref, wv_ref)):
        cols = slice(n * 256, (n + 1) * 256)
        dt_ref[...] += dot(high[:, cols], w[...], (1, 1)) + dot(low[:, cols], w[...], (1, 1))
    vec_ref[0:8] = gf_ref[...]
    vec_ref[8:16] = gm_ref[...]
    vec_ref[16:32] = jnp.zeros((16, 1024), F32)

    def gain_rows(i):
        at = pl.ds(i, 32)
        x = obs_ref[at, :].astype(F32)
        vec_ref[16:24] += fold8(dt_ref[at, :] * x * inverse_rms(x))

    by_blocks(256, 32, gain_rows)
    place_at = (iota((32, 128), 1) == 17 + iota((32, 128), 0) // 8).astype(BF16)
    vec = vec_ref[...]
    high, low = halves(vec)
    lowest = (vec - high.astype(F32) - low.astype(F32)).astype(BF16)
    small = small_ref[...] + sum(dot(part, place_at, (0, 0)) for part in (high, low, lowest))
    small4[...] = small.reshape(4, 4, 64, 128)
    first[SMALL].start()

    first[SUM_A].middle()
    first[SUM_B].middle()
    send_tail(UP_A)
    send_tail(UP_B)
    turn(DOWN_A)
    turn(DOWN_B)
    turn(SUM_A)
    turn(SUM_B)
    first[OUT].middle()
    first[SMALL].middle()
    second[SUM_A].middle()
    second[SUM_B].middle()
    second[DOWN_A].middle()
    second[DOWN_B].middle()
    send_tail(SUM_A)
    send_tail(SUM_B)
    turn(OUT)
    turn(SMALL)
    for i in (SUM_A, SUM_B):
        tails[i].wait_recv()
    full_a[x, z] = ends[SUM_A][0][...] + ends[SUM_A][1][...]
    full_b[x, z] = ends[SUM_B][0][...] + ends[SUM_B][1][...]
    near = [remote(full_a.at[x, z], full_a.at[x, z], near_sem, (0, j - 1), at_z(j)) for j in (1, 2, 3)]
    near += [remote(full_b.at[x, z], full_b.at[x, z], near_sem, (1, j - 1), at_x(j)) for j in (1, 2, 3)]
    send_tail(DOWN_A)
    send_tail(DOWN_B)
    second[OUT].middle()
    second[SMALL].middle()
    for cp in near:
        cp.wait_recv()
    wide = [remote(full_a.at[x], full_a.at[x], far_sem, (0, j - 1), at_x(j)) for j in (1, 2, 3)]
    wide += [remote(full_b.at[:, z], full_b.at[:, z], far_sem, (1, j - 1), at_z(j)) for j in (1, 2, 3)]
    send_tail(OUT)
    send_tail(SMALL)

    def total(i, put):
        res, ybuf, _ = ends[i]
        by_blocks(32, 8, lambda k: put(k, res[rows(yh * 32 + k, 8), :] + ybuf[pl.ds(k, 8), :]))

    def to_out(ref):
        def put(k, value):
            ref[pl.ds(k, 8), :] = value

        return put

    def to_mp(k, value):
        mp_buf[m, pl.ds(k, 8), :] = value

    shares = []
    for i in (UP_A, UP_B, DOWN_A, DOWN_B, SMALL, OUT):
        tails[i].wait_recv()
        if i == SMALL:
            total(i, to_mp)
            shares = [remote(mp_buf.at[m], mp_buf.at[m], mp_sem, (j,), dev) for j, dev in enumerate(peers)]
        else:
            total(i, to_out(outs[i]))
    for cp in wide:
        cp.wait_recv()
    table = ht_ref[:, rows((d // 4) * 128, 128)]
    for n, ref in enumerate((full_a, full_b)):
        high, low = halves(ref[...].reshape(256, 384))
        mine_ref[:, n * 384 : (n + 1) * 384] = dot(table, high, (0, 0)) + dot(table, low, (0, 0))
    outs[6][...] = mine_ref[rows((d % 4) * 32, 32), :]
    for cp in shares:
        cp.wait_recv()
    outs[SMALL][...] = mp_buf[0] + mp_buf[1] + mp_buf[2] + mp_buf[3]
    for cp in [*shares, *tails.values(), *near, *wide]:
        cp.wait_send()
    for ring in [*first.values(), *second]:
        ring.drain()


def tail(*args):
    vm, dma = pltpu.VMEM, pltpu.SemaphoreType.DMA
    scratch = [vm(shape, kind) for shape, kind in LOADS]
    scratch += [
        dma((len(LOADS),)), vm((4, 4, 64, 256), F32), vm((256, 768), F32), vm((4, 4, 16, 768), F32),
        vm((4, 4, 16, 384), F32), vm((4, 4, 16, 384), F32), dma((2, 2, 3)), dma((2, 2, 3)), vm((128, 768), F32),
        vm((256, 1024), F32), vm((32, 1024), F32), vm((4, 4, 64, 128), F32), vm((4, 32, 128), F32), dma((2, 3)),
    ]
    for i in range(2, 8):
        scratch += one_scratch(WIDTH[i], PART[i]) + [vm((4, PART[i], WIDTH[i]), F32)]
    for i in range(8):
        scratch += two_scratch(WIDTH[i], PART[i], 16 if i in (SUM_A, SUM_B) else 32)
    return pl.pallas_call(
        tail_kernel,
        out_shape=tuple(jax.ShapeDtypeStruct((32, w), F32) for w in (*WIDTH[:6], 768)),
        in_specs=[ANY] * len(LOADS),
        out_specs=tuple([VMEM] * 7),
        scratch_shapes=scratch,
        compiler_params=params(2),
        name="tail",
    )(*args)


def write_kernel(
    up_a, up_b, down_a, down_b, out_ref, small_ref, qkv_ref,
    o_q, o_k, o_v, o_out, o_up, o_down, o_actor, o_critic, o_final, o_mlp, o_attn,
):
    o_q[...] = qkv_ref[:, :256]
    o_k[...] = qkv_ref[:, 256:512]
    o_v[...] = qkv_ref[:, 512:]
    o_up[:, :512] = up_a[...]
    o_up[:, 512:] = up_b[...]
    o_out[...] = out_ref[...]
    o_down[:, :512] = down_a[...]
    o_down[:, 512:] = down_b[...]
    flat = jnp.transpose(small_ref[...])
    o_actor[...] = flat[:16, :]
    o_critic[...] = flat[16:17, :]
    o_final[...] = flat[17:18, :]
    o_mlp[...] = flat[18:19, :]
    own = jnp.transpose(small_ref[rows(lax.axis_index("mp") * 8, 8), :])
    o_attn[...] = own[19:20, :]


def write_outputs(*parts):
    sd = jax.ShapeDtypeStruct
    shapes = [(32, 256)] * 4 + [(32, 1024)] * 2 + [(16, 32)] + [(1, 32)] * 3 + [(1, 8)]
    return pl.pallas_call(
        write_kernel,
        out_shape=tuple(sd(shape, F32) for shape in shapes),
        in_specs=[VMEM] * 7,
        out_specs=tuple([VMEM] * 11),
        name="write_outputs",
    )(*parts)


def per_device(
    initial_state,
    actions,
    next_state,
    reward_table,
    reward_scale,
    observe_table,
    gain_attn,
    w_query,
    w_key,
    w_value,
    w_out,
    gain_mlp,
    w_up,
    w_down,
    gain_final,
    actor_head,
    critic_head,
):
    token_total = actions.size * lax.axis_size("dp")

    def line(vector):
        return vector.reshape(1, -1)

    qkv, match, mixed, h_table, grad_down, dx_one_low, grad_heads, final_terms, mlp_terms, res_a, res_b = policy(
        token_total,
        line(initial_state), actions.T, line(reward_scale), next_state.T, reward_table.T, observe_table,
        line(gain_attn), w_query, w_key, w_value, w_out, line(gain_mlp), line(gain_final),
        actor_head.T, line(critic_head), w_up, w_down,
    )
    parts = tail(
        grad_down, dx_one_low, mixed, w_out, qkv, match, h_table, observe_table, w_query, w_key, w_value,
        grad_heads, final_terms, mlp_terms, res_a, res_b,
    )
    q, k, v, out, up, down, actor, critic, final, mlp, attn = write_outputs(*parts)
    return (
        q, k, v, out.T, up, down.T, attn.reshape(-1), mlp.reshape(-1), final.reshape(-1), actor.T,
        critic.reshape(-1),
    )


def solution(mesh):
    return jax.shard_map(
        per_device,
        mesh=mesh,
        in_specs=(
            P("dp"),
            P("dp", None),
            P(),
            P(),
            P("dp"),
            P(),
            P(),
            P(None, "mp"),
            P(None, "mp"),
            P(None, "mp"),
            P("mp", None),
            P(),
            P(None, "mp"),
            P("mp", None),
            P(),
            P(),
            P(),
        ),
        out_specs=(
            P("dp", "mp"),
            P("dp", "mp"),
            P("dp", "mp"),
            P("mp", "dp"),
            P("dp", "mp"),
            P("mp", "dp"),
            P(("dp", "mp")),
            P("dp"),
            P("dp"),
            P("dp", None),
            P("dp"),
        ),
        check_vma=False,
    )
```

```python
import functools
import math

import jax
import jax.numpy as jnp
from jax import lax
from jax.experimental import pallas as pl
from jax.experimental.pallas import tpu as pltpu
from jax.sharding import PartitionSpec as P

HEAD_DIM = 128
STEPS = 16
EPS = 1e-05
GAMMA = 0.9
VALUE_COEF = 0.5
ENTROPY_COEF = 0.1
SCALE = 1.0 / math.sqrt(HEAD_DIM)
MESH = pl.DeviceIdType.MESH
VMEM = pl.BlockSpec(memory_space=pltpu.VMEM)
WIDE = 1024
ANY = pl.BlockSpec(memory_space=pl.ANY)
F32 = jnp.float32
BF16 = jnp.bfloat16


def place():
    d, m = lax.axis_index("dp"), lax.axis_index("mp")
    return d, m, m % 2, m // 2


def axes_place():
    d, m, c, l = place()
    return d // 8, (d // 2) % 4, d % 2


def partners():
    d, m, c, l = place()
    over = m + 2 - 4 * l
    return (d, m + 1 - 2 * c), (d, over), (d + 1 - 2 * (d % 2), over)


def at_x(k):
    d, m, c, l = place()
    x, z, yh = axes_place()
    return (lax.rem(x + k, 4) * 8 + z * 2 + yh, m)


def at_z(k):
    d, m, c, l = place()
    x, z, yh = axes_place()
    return (x * 8 + lax.rem(z + k, 4) * 2 + yh, m)


def stats_devices():
    d, m, c, l = place()
    x, z, yh = axes_place()
    plane, column = [], []
    for j in range(1, 16):
        other = lax.rem(x * 4 + z + j, 16)
        plane.append(((other // 4) * 8 + (other % 4) * 2 + yh, m))
    for j in range(1, 8):
        other = lax.rem(yh * 4 + m + j, 8)
        column.append((x * 8 + z * 2 + other // 4, other % 4))
    return plane, column


def greet(devices):
    barrier = pltpu.get_barrier_semaphore()
    for dev in devices:
        pl.semaphore_signal(barrier, inc=1, device_id=dev, device_id_type=MESH)
    pl.semaphore_wait(barrier, len(devices))


def remote(src, dst, sems, at, dev):
    cp = pltpu.make_async_remote_copy(
        src_ref=src, dst_ref=dst, send_sem=sems.at[(0, *at)], recv_sem=sems.at[(1, *at)],
        device_id=dev, device_id_type=MESH,
    )
    cp.start()
    return cp


def rows(start, size):
    return pl.ds(pl.multiple_of(start, size), size)


def by_blocks(total, block, body):
    lax.fori_loop(0, total // block, lambda i, z: (body(pl.multiple_of(i * block, block)), z)[1], 0)


def dot(left, right, contract, **kw):
    return lax.dot_general(
        left, right, ((contract[:1], contract[1:]), ((), ())), preferred_element_type=F32, **kw
    )


def iota(shape, axis):
    return lax.broadcasted_iota(jnp.int32, shape, axis)


def fold8(term):
    total = term[0:8]
    for k in range(1, term.shape[0] // 8):
        total = total + term[8 * k : 8 * k + 8]
    return total


def inverse_rms(x):
    return lax.rsqrt(jnp.mean(x * x, axis=-1, keepdims=True) + EPS)


def norm_back(x, inv, gain, up):
    weighted = up * gain
    return inv * weighted - x * (inv * inv * inv) * jnp.mean(x * weighted, axis=-1, keepdims=True)


def block_at(h, core, low):
    return h * 512 + core * 256 + low * 128


CHUNKS = [(h, k) for k in range(2) for h in range(2)]


class Sums:
    def __init__(self, p, near_own, near_far, far, sems):
        d, m, self.c, self.l = place()
        self.core, *self.over = partners()
        self.p, self.near_own, self.near_far, self.far = p, near_own, near_far, far
        self.own_sem, self.near_sem, self.far_sem = sems
        self.own, self.near, self.sent = {}, {}, {}

    def give_own(self):
        for h in range(2):
            src = self.p.at[rows(block_at(h, 1 - self.c, self.l), 128)]
            self.own[h] = remote(src, self.near_own.at[h], self.own_sem, (h,), self.core)

    def give_far(self, k):
        for h in range(2):
            src = self.p.at[rows(block_at(h, 1 - self.c, 1 - self.l) + k * 64, 64)]
            self.near[h, k] = remote(src, self.near_far.at[h, k], self.near_sem, (h, k), self.core)

    def pass_far(self, k):
        for h in range(2):
            self.near[h, k].wait_recv()
            base = block_at(h, self.c, 1 - self.l) + k * 64

            def body(i, h=h, base=base):
                self.near_far[h, k, pl.ds(i, 32), :] += self.p[rows(base + i, 32), :]

            by_blocks(64, 32, body)
            self.sent[h, k] = remote(
                self.near_far.at[h, k], self.far.at[h, k], self.far_sem, (h, k), self.over[h]
            )

    def take_own(self):
        for h in range(2):
            self.own[h].wait_recv()

    def take(self, h, k):
        self.sent[h, k].wait_recv()

    def value(self, h, k, i):
        mine = self.p[rows(block_at(h, self.c, self.l) + k * 64 + i, 32), :]
        return mine + self.near_own[h, pl.ds(k * 64 + i, 32), :] + self.far[h, k, pl.ds(i, 32), :]

    def drain(self):
        for group in (self.own, self.near, self.sent):
            for cp in group.values():
                cp.wait_send()


class Gather:
    def __init__(self, q, whole, low, sems):
        d, m, self.c, self.l = place()
        self.core, *self.over = partners()
        self.q, self.whole, self.low = q, whole, low
        self.over_sem, self.core_sem, self.fwd_sem = sems
        self.far, self.near, self.fwd, self.left = {}, {}, {}, set()

    def keep(self, base, src=None, at=0):
        def body(i):
            value = self.whole[rows(base + i, 32), :] if src is None else src[pl.ds(at + i, 32), :]
            self.low[rows(base + i, 32), :] = value.astype(BF16)

        by_blocks(64, 32, body)

    def send(self, h, k):
        base = block_at(h, self.c, self.l) + k * 64
        src, dst = self.q.at[pl.ds(h * 128 + k * 64, 64)], self.whole.at[rows(base, 64)]
        self.far[h, k] = remote(src, dst, self.over_sem, (h, k), self.over[h])
        self.near[h, k] = remote(src, dst, self.core_sem, (h, k), self.core)
        self.keep(base, self.q, h * 128 + k * 64)

    def take_core(self, h, k):
        self.near[h, k].wait_recv()
        self.keep(block_at(h, 1 - self.c, self.l) + k * 64)

    def take_far(self, h, k):
        self.far[h, k].wait_recv()
        base = block_at(h, self.c, 1 - self.l) + k * 64
        at = self.whole.at[rows(base, 64)]
        self.fwd[h, k] = remote(at, at, self.fwd_sem, (h, k), self.core)
        self.keep(base)

    def forwarded(self, k):
        for h in range(2):
            self.fwd[h, k].wait_send()
        self.left.add(k)

    def take_fwd(self, h, k):
        self.fwd[h, k].wait_recv()
        self.keep(block_at(h, 1 - self.c, 1 - self.l) + k * 64)

    def drain(self):
        late = [cp for (h, k), cp in self.fwd.items() if k not in self.left]
        for cp in [*self.far.values(), *self.near.values(), *late]:
            cp.wait_send()


SUM_SEMS = [
    pltpu.SemaphoreType.DMA((2, 2)), pltpu.SemaphoreType.DMA((2, 2, 2)), pltpu.SemaphoreType.DMA((2, 2, 2)),
]
GATHER_SEMS = [pltpu.SemaphoreType.DMA((2, 2, 2))] * 3


def gather_work_sum(gather, sums, work):
    c, l = sums.c, sums.l
    work([(block_at(h, c, l), 128) for h in range(2)])
    for h, k in CHUNKS:
        gather.take_core(h, k)
    work([(block_at(h, 1 - c, l), 128) for h in range(2)])
    sums.give_own()
    for k in range(2):
        for h in range(2):
            gather.take_far(h, k)
        work([(block_at(h, c, 1 - l) + k * 64, 64) for h in range(2)])
        for h in range(2):
            gather.take_fwd(h, k)
        work([(block_at(h, 1 - c, 1 - l) + k * 64, 64) for h in range(2)])
        sums.give_far(k)
        gather.forwarded(k)
        sums.pass_far(k)
    sums.take_own()


def spans_of(ref, spans, cols=slice(None)):
    return jnp.concatenate([ref[rows(at, n), cols] for at, n in spans], axis=0)


def put_spans(ref, spans, cols, value):
    done = 0
    for at, n in spans:
        ref[rows(at, n), cols] = value[done : done + n]
        done += n


def sum_everywhere(value, between, ps, cs, psem, csem):
    d, m, c, l = place()
    x, z, yh = axes_place()
    plane, column = stats_devices()

    def stage(slots, sems, devs, me, value, between=None):
        slots[me] = value
        copies = [remote(slots.at[me], slots.at[me], sems, (j,), dev) for j, dev in enumerate(devs)]
        done = between() if between is not None else None
        for cp in copies:
            cp.wait_recv()
        total = slots[0]
        for k in range(1, len(devs) + 1):
            total = total + slots[k]
        for cp in copies:
            cp.wait_send()
        return total, done

    value, done = stage(ps, psem, plane, x * 4 + z, value, between)
    return stage(cs, csem, column, yh * 4 + m, value)[0], done


STATS_SCRATCH = [
    pltpu.VMEM((16, 8, 128), F32),
    pltpu.VMEM((8, 8, 128), F32),
    pltpu.SemaphoreType.DMA((2, 15)),
    pltpu.SemaphoreType.DMA((2, 7)),
]


class Ring:
    def __init__(self, src, bufs, sems, pos, right, left):
        self.src, self.pos, self.right, self.left = src, pos, right, left
        self.mid, self.fl, self.fr = bufs
        self.sems = sems
        self.copies = []

    def send(self, src, dst, dev):
        self.copies.append(remote(src, dst, self.sems, (len(self.copies),), dev))

    def start(self):
        p = self.pos
        self.r, self.l, opp = lax.rem(p + 1, 4), lax.rem(p + 3, 4), lax.rem(p + 2, 4)
        self.send(self.src(opp, 0), self.mid.at[0], self.right)
        self.send(self.src(opp, 1), self.mid.at[1], self.left)
        self.send(self.src(self.r, 1), self.fl.at[1], self.right)
        self.send(self.src(self.l, 0), self.fr.at[0], self.left)

    def middle(self):
        self.copies[0].wait_recv()
        add_into(self.mid.at[0], self.src(self.r, 0))
        self.send(self.mid.at[0], self.fl.at[0], self.right)
        self.copies[1].wait_recv()
        add_into(self.mid.at[1], self.src(self.l, 1))
        self.send(self.mid.at[1], self.fr.at[1], self.left)

    def finish(self, out):
        for k in (2, 3, 4, 5):
            self.copies[k].wait_recv()
        for half in range(2):
            add_three(out(half), self.src(self.pos, half), self.fl.at[half], self.fr.at[half])

    def drain(self):
        for cp in self.copies:
            cp.wait_send()


def each_block(ref, body):
    n = min(16, ref.shape[-2])
    if len(ref.shape) == 3:
        for k in range(ref.shape[0]):
            by_blocks(ref.shape[1], n, lambda i, k=k: body((k, pl.ds(i, n), slice(None))))
    else:
        by_blocks(ref.shape[0], n, lambda i: body((pl.ds(i, n), slice(None))))


def add_into(dst, src):
    def body(at):
        dst[at] += src[at]

    each_block(dst, body)


def add_three(dst, a, b, c):
    def body(at):
        dst[at] = a[at] + b[at] + c[at]

    each_block(dst, body)


def ring_one(order, src, bufs, sems, cols=slice(None)):
    x, z, yh = axes_place()
    every = slice(None)
    if order == "xz":
        return Ring(lambda j, h: src.at[j, pl.ds(h * 2, 2), every, cols], bufs, sems, x, at_x(1), at_x(3))
    return Ring(lambda j, h: src.at[pl.ds(h * 2, 2), j, every, cols], bufs, sems, z, at_z(1), at_z(3))


def ring_two(order, res, bufs, sems):
    x, z, yh = axes_place()

    half = res.shape[1] // 2

    def src(j, h):
        return res.at[j, pl.ds(h * half, half)]

    if order == "xz":
        return Ring(src, bufs, sems, z, at_z(1), at_z(3))
    return Ring(src, bufs, sems, x, at_x(1), at_x(3))


def one_scratch(w, part=64):
    return [pltpu.VMEM((2, 2, part, w), F32)] * 3 + [pltpu.SemaphoreType.DMA((2, 6))]


def two_scratch(w, part=64, kept=32):
    return [
        *[pltpu.VMEM((2, part // 2, w), F32)] * 3,
        pltpu.VMEM((part, w), F32),
        pltpu.VMEM((kept, w), F32),
        pltpu.SemaphoreType.DMA((2, 6)),
        pltpu.SemaphoreType.DMA((2,)),
    ]


def params(n):
    return pltpu.CompilerParams(
        collective_id=n, has_side_effects=True, vmem_limit_bytes=63 * 1024 * 1024
    )


def block_probs(q, k):
    r, s = iota((128, 128), 0), iota((128, 128), 1)
    seen = ((r // STEPS) == (s // STEPS)) & (r >= s)
    weights = jnp.where(seen, jnp.exp(dot(q, k, (1, 1)) * SCALE), 0.0)
    return weights / jnp.sum(weights, axis=-1, keepdims=True)


def policy_kernel(
    token_total,
    init_ref, act_ref, scale_ref, next_ref, rew_ref, obs_ref, gain_attn, wq_ref, wk_ref, wv_ref, wo_ref,
    gain_mlp, gain_fin, actor_ref, critic_ref, up_hbm, down_hbm,
    ht_out, down_out, gh_ref, g_fin, g_mlp, res_a, res_b, state_sums, out_ref,
    low_one, qkv_ref, match_ref, mixed_ref, ht_ref, flush_sem,
    r_init, r_act, r_scale, roll_sem, tables, st_ref, own_ref, head_f, heads,
    w_up, w_down, w_sem,
    p, near_own, near_far, far, whole, h_two, up_rows, hidden, low_two, d_up, x_one, dx_two, buf_a, buf_b,
    fin_ref, grad_up, grad_down, *rest,
):
    stats, rest = rest[:4], rest[4:]
    sems_a, sems_b, sems_d = rest[0:3], rest[3:6], rest[6:9]
    gs_b, gs_d, gs_e = rest[9:12], rest[12:15], rest[15:18]
    ring_a, ring_b = rest[18:22], rest[22:26]
    flushed = []

    def flush(src, dst):
        cp = pltpu.make_async_copy(src, dst, flush_sem.at[len(flushed)])
        cp.start()
        flushed.append(cp)

    d, m, c, l = place()
    weights = [
        pltpu.make_async_copy(up_hbm, w_up, w_sem.at[0]), pltpu.make_async_copy(down_hbm, w_down, w_sem.at[1]),
    ]
    for cp in weights:
        cp.start()
    plane, column = stats_devices()
    greet(plane + column)
    far_dev = partners()[2]
    copies = [
        remote(src, dst, roll_sem, (n,), far_dev)
        for n, (src, dst) in enumerate(((init_ref, r_init), (act_ref, r_act), (scale_ref, r_scale)))
    ]

    def table_rows(i):
        at = pl.ds(i, 32)
        x = obs_ref[at, :].astype(F32)
        ht_ref[at, :] = (x * inverse_rms(x) * gain_attn[...]).astype(BF16)

    by_blocks(256, 32, table_rows)
    flush(ht_ref, ht_out)
    for n, w in enumerate((wq_ref, wk_ref, wv_ref)):
        tables[:, n * 256 : (n + 1) * 256] = dot(ht_ref[...], w[...], (1, 0)).astype(BF16)
    head_f[...] = jnp.zeros_like(head_f)
    head_f[0:16, :] = actor_ref[...].astype(F32)
    head_f[16:17, :] = critic_ref[...].astype(F32)
    heads[...] = jnp.zeros_like(heads)
    heads[0:32, :] = head_f[...].astype(BF16)

    for cp in copies:
        cp.wait()
    swap = 32 + 64 * l
    lane = iota((1, 64), 1)
    state = jnp.where(lane >= swap, r_init[...], init_ref[...]).astype(F32)
    scale = jnp.where(lane >= swap, r_scale[...], scale_ref[...])
    act_t = jnp.where(iota((16, 64), 1) >= swap, r_act[...], act_ref[...]).astype(F32)
    nexts = next_ref[...].astype(F32).astype(BF16)
    ids, kinds = iota((256, 64), 0).astype(F32), iota((16, 64), 0).astype(F32)
    for t in range(STEPS):
        st_ref[pl.ds(t, 1), :] = state
        if t + 1 < STEPS:
            hit = jnp.where(ids == state, 1.0, 0.0).astype(BF16)
            found = dot(nexts, hit, (1, 0))
            state = jnp.sum(jnp.where(kinds == act_t[t : t + 1, :], found, 0.0), axis=0, keepdims=True)

    pick_t = (iota((128, 16), 0) % STEPS == iota((128, 16), 1)).astype(BF16)
    spread = jnp.ones((64, 128), BF16)
    lanes = iota((128, 128), 1).astype(F32)

    def per_token(rows_by_env, first_env):
        here = iota((128, 64), 1) == first_env + iota((128, 64), 0) // STEPS
        found = jnp.where(here, dot(pick_t, rows_by_env, (1, 0)), 0.0)
        return dot(found.astype(BF16), spread, (1, 0))

    def attend(core, low):
        def block(h, carry):
            at = rows(block_at(h, core, low), 128)
            ids_here = per_token(st_ref[...].astype(BF16), h * 32 + (core * 2 + low) * 8)
            match = jnp.concatenate(
                [jnp.where(ids_here == lanes, 1.0, 0.0), jnp.where(ids_here == lanes + 128.0, 1.0, 0.0)], axis=1
            ).astype(BF16)
            match_ref[at, :] = match
            qkv = dot(match, tables[...], (1, 0)).astype(BF16)
            qkv_ref[at, :] = qkv
            outs = []
            for n in range(2):
                q, k, v = (qkv[:, j * 256 + n * 128 : j * 256 + (n + 1) * 128] for j in range(3))
                outs.append(dot(block_probs(q, k).astype(BF16), v, (1, 0)).astype(BF16))
            mixed = jnp.concatenate(outs, axis=1)
            mixed_ref[at, :] = mixed
            p[at, :] = dot(mixed, wo_ref[...], (1, 0))
            return carry

        lax.fori_loop(0, 2, block, 0, unroll=True)

    sums = Sums(p, near_own, near_far, far, sems_a)
    attend(1 - c, 1 - l)
    sums.give_far(0)
    sums.give_far(1)
    attend(c, 1 - l)
    sums.pass_far(0)
    sums.pass_far(1)
    attend(1 - c, l)
    sums.give_own()
    attend(c, l)
    for h in range(2):
        at = pl.ds(h * 128, 128)
        mine = match_ref[rows(block_at(h, c, l), 128), :]
        x_one[at, :] = dot(mine, obs_ref[...], (1, 0))
        first_env = h * 32 + (c * 2 + l) * 8
        chosen = jnp.where(per_token(act_t.astype(BF16), first_env) == lanes, 1.0, 0.0)
        found = dot(mine.astype(F32), rew_ref[...], (1, 1), precision=lax.Precision.HIGHEST)
        here = iota((128, 64), 1) == first_env + iota((128, 64), 0) // STEPS
        factor = jnp.sum(jnp.where(here, scale, 0.0), axis=1, keepdims=True)
        reward = jnp.sum(chosen[:, :16] * found, axis=1, keepdims=True) * factor
        own_ref[at, :] = jnp.where(lanes == 16.0, reward, chosen)
    sums.take_own()

    gather = Gather(buf_a, whole, h_two, gs_b)
    for h, k in CHUNKS:
        sums.take(h, k)

        def body(i, h=h, k=k):
            at = pl.ds(h * 128 + k * 64 + i, 32)
            x = sums.value(h, k, i) + x_one[at, :]
            x_one[at, :] = x
            buf_a[at, :] = x * inverse_rms(x) * gain_mlp[...]

        by_blocks(64, 32, body)
        gather.send(h, k)
    sums.drain()
    for cp in weights:
        cp.wait()

    def forward(spans):
        def up(j):
            cols = pl.ds(j, WIDE)
            u = dot(spans_of(h_two, spans), w_up[:, cols], (1, 0))
            put_spans(up_rows, spans, cols, u)
            put_spans(hidden, spans, cols, (u / (1.0 + jnp.exp(-u))).astype(BF16))

        def down(j):
            cols = pl.ds(j, WIDE)
            put_spans(p, spans, cols, dot(spans_of(hidden, spans), w_down[:, cols], (1, 0)))

        by_blocks(1024, WIDE, up)
        by_blocks(1024, WIDE, down)

    sums = Sums(p, near_own, near_far, far, sems_b)
    gather_work_sum(gather, sums, forward)
    for h, k in CHUNKS:
        sums.take(h, k)

        def body(i, h=h, k=k):
            at = pl.ds(h * 128 + k * 64 + i, 32)
            x = sums.value(h, k, i) + x_one[at, :]
            buf_b[at, :] = x
            fin_ref[at, :] = (x * inverse_rms(x) * gain_fin[...]).astype(BF16)

        by_blocks(64, 32, body)
    gather.drain()
    sums.drain()

    lane = iota((256, 128), 1)
    both = dot(fin_ref[...], heads[...], (1, 1))
    critic = jnp.sum(jnp.where(lane == 16, both, 0.0), axis=1, keepdims=True)
    own = own_ref[...]
    reward = jnp.sum(jnp.where(lane == 16, own, 0.0), axis=1, keepdims=True)
    step = iota((256, 128), 0) % STEPS
    base = reward + jnp.where(step == STEPS - 1, GAMMA * critic, 0.0)
    r, s = iota((256, 256), 0), iota((256, 256), 1)
    ahead = ((r // STEPS) == (s // STEPS)) & (s >= r)
    decay = jnp.where(ahead, jnp.exp((s - r).astype(F32) * math.log(GAMMA)), 0.0)
    returns = dot(decay, base, (1, 0), precision=lax.Precision.HIGHEST)
    advantage = returns - critic
    tile = jnp.where(
        iota((8, 128), 0) == 0,
        jnp.sum(advantage, axis=0, keepdims=True),
        jnp.sum(advantage * advantage, axis=0, keepdims=True),
    )
    real = lane < 16
    factor = 1.0 / math.sqrt(token_total)

    def policy_terms():
        logits = jnp.where(real, both, 0.0)
        mass = jnp.sum(jnp.where(real, jnp.exp(logits), 0.0), axis=1, keepdims=True)
        logp = jnp.where(real, logits - jnp.log(mass), 0.0)
        chance = jnp.where(real, jnp.exp(logp), 0.0)
        entropy = -jnp.sum(chance * logp, axis=1, keepdims=True)
        picked = jnp.where(real, own, 0.0)
        d_value = (factor * VALUE_COEF) * (critic - returns)
        return picked - chance, ENTROPY_COEF * chance * (logp + entropy), d_value

    totals, (push, calm, d_value) = sum_everywhere(tile, policy_terms, *stats)
    mean = totals[0:1, :] * (1.0 / token_total)
    variance = totals[1:2, :] * (1.0 / token_total) - mean * mean
    normed = (advantage - mean) * lax.rsqrt(variance + EPS)
    d_logits = factor * (-normed * push + calm)
    d_both = jnp.where(real, d_logits, jnp.where(lane == 16, d_value, 0.0)).astype(BF16)
    buf_a[...] = dot(d_both, heads[...], (1, 0))
    g_fin[...] = jnp.zeros_like(g_fin)
    g_mlp[...] = jnp.zeros_like(g_mlp)

    gather = Gather(dx_two, whole, low_two, gs_d)
    for h, k in CHUNKS:

        def body(i, h=h, k=k):
            at = pl.ds(h * 128 + k * 64 + i, 32)
            x, up = buf_b[at, :], buf_a[at, :]
            inv = inverse_rms(x)
            dx_two[at, :] = norm_back(x, inv, gain_fin[...], up)
            g_fin[...] += fold8(up * x * inv)

        by_blocks(64, 32, body)
        gather.send(h, k)
    gh_ref[...] = dot(fin_ref[...], d_both, (0, 0))

    def backward(spans):
        def up(j):
            cols = pl.ds(j, WIDE)
            d_hidden = dot(spans_of(low_two, spans), w_down[cols, :], (1, 1)).astype(BF16).astype(F32)
            u = spans_of(up_rows, spans, cols)
            sig = 1.0 / (1.0 + jnp.exp(-u))
            put_spans(d_up, spans, cols, (d_hidden * sig * (1.0 + u * (1.0 - sig))).astype(BF16))

        def down(j):
            cols = pl.ds(j, WIDE)
            put_spans(p, spans, cols, dot(spans_of(d_up, spans), w_up[cols, :], (1, 1)))

        by_blocks(1024, WIDE, up)
        by_blocks(1024, WIDE, down)

    sums = Sums(p, near_own, near_far, far, sems_d)
    gather_work_sum(gather, sums, backward)

    def weight_grad(out, left, right):
        def tile(j, carry):
            cols = rows(j * 256, 256)
            out[j] = dot(left[:, cols], right[...], (0, 0)).reshape(4, 64, 1024)
            return carry

        lax.fori_loop(0, 4, tile, 0)

    rings = [
        ring_one("xz", grad_up, ring_a[:3], ring_a[3], pl.ds(0, 512)),
        ring_one("zx", grad_up, ring_b[:3], ring_b[3], pl.ds(512, 512)),
    ]
    weight_grad(grad_up, h_two, d_up)
    for ring in rings:
        ring.start()
    weight_grad(grad_down, low_two, hidden)
    flush(grad_down, down_out)
    gather.drain()

    def attend_back(core, low):
        lax.fori_loop(0, 2, functools.partial(back_block, core, low), 0, unroll=True)

    def back_block(core, low, h, carry):
        at = rows(block_at(h, core, low), 128)
        d_mixed = dot(low_one[at, :], wo_ref[...], (1, 1)).astype(BF16)
        qkv = qkv_ref[at, :]
        parts = [[], [], []]
        for n in range(2):
            q, k, v = (qkv[:, j * 256 + n * 128 : j * 256 + (n + 1) * 128] for j in range(3))
            up = d_mixed[:, n * 128 : (n + 1) * 128]
            probs = block_probs(q, k)
            d_probs = dot(up, v, (1, 1))
            parts[2].append(dot(probs.astype(BF16), up, (0, 0)).astype(BF16))
            d_scores = (
                probs * (d_probs - jnp.sum(probs * d_probs, axis=-1, keepdims=True)) * SCALE
            ).astype(BF16)
            parts[0].append(dot(d_scores, k, (1, 0)).astype(BF16))
            parts[1].append(dot(d_scores, q, (0, 0)).astype(BF16))
        d_qkv = jnp.concatenate([*parts[0], *parts[1], *parts[2]], axis=1)
        state_sums[...] += dot(match_ref[at, :], d_qkv, (0, 0))
        return carry

    state_sums[...] = jnp.zeros_like(state_sums)
    gather = Gather(buf_b, whole, low_one, gs_e)
    for h, k in CHUNKS:
        sums.take(h, k)

        def body(i, h=h, k=k):
            at = pl.ds(h * 128 + k * 64 + i, 32)
            up, x = sums.value(h, k, i), x_one[at, :]
            inv = inverse_rms(x)
            buf_b[at, :] = dx_two[at, :] + norm_back(x, inv, gain_mlp[...], up)
            g_mlp[...] += fold8(up * x * inv)

        by_blocks(64, 32, body)
        gather.send(h, k)
    sums.drain()
    attend_back(c, l)
    for h, k in CHUNKS:
        gather.take_core(h, k)
    for h in range(2):
        gather.take_far(h, 0)
    for ring in rings:
        ring.middle()
    attend_back(1 - c, l)
    for h in range(2):
        gather.take_far(h, 1)
    attend_back(c, 1 - l)
    for h, k in CHUNKS:
        gather.take_fwd(h, k)
    gather.drain()
    attend_back(1 - c, 1 - l)

    def out_tile(j, carry):
        cols = rows(j * 256, 256)
        out_ref[j] = dot(low_one[:, cols], mixed_ref[...], (0, 0)).reshape(4, 64, 256)
        return carry

    lax.fori_loop(0, 4, out_tile, 0)
    for ring, res in zip(rings, (res_a, res_b)):
        ring.finish(lambda h, res=res: res.at[pl.ds(h * 2, 2)])
    for ring in rings:
        ring.drain()
    for cp in flushed:
        cp.wait()


def policy(token_total, *args):
    sd, vm = jax.ShapeDtypeStruct, pltpu.VMEM
    return pl.pallas_call(
        functools.partial(policy_kernel, token_total),
        out_shape=(
            sd((256, 1024), BF16), sd((4, 4, 64, 1024), F32), sd((1024, 128), F32), sd((8, 1024), F32),
            sd((8, 1024), F32), sd((4, 64, 512), F32), sd((4, 64, 512), F32), sd((256, 768), F32),
            sd((4, 4, 64, 256), F32),
        ),
        in_specs=[VMEM] * 15 + [ANY] * 2,
        out_specs=tuple([ANY] * 2 + [VMEM] * 7),
        scratch_shapes=[
            vm((1024, 1024), BF16), vm((1024, 768), BF16), vm((1024, 256), BF16), vm((1024, 256), BF16), vm((256, 1024), BF16),
            pltpu.SemaphoreType.DMA((2,)),
            vm((1, 64), jnp.int32), vm((16, 64), jnp.int32), vm((1, 64), F32), pltpu.SemaphoreType.DMA((2, 3)),
            vm((256, 768), BF16), vm((16, 64), F32), vm((256, 128), F32), vm((32, 1024), F32), vm((128, 1024), BF16),
            vm((1024, 1024), BF16), vm((1024, 1024), BF16), pltpu.SemaphoreType.DMA((2,)),
            vm((1024, 1024), F32), vm((2, 128, 1024), F32), vm((2, 2, 64, 1024), F32), vm((2, 2, 64, 1024), F32),
            vm((1024, 1024), F32), vm((1024, 1024), BF16), vm((1024, 1024), F32), vm((1024, 1024), BF16),
            vm((1024, 1024), BF16), vm((1024, 1024), BF16),
            vm((256, 1024), F32), vm((256, 1024), F32), vm((256, 1024), F32), vm((256, 1024), F32),
            vm((256, 1024), BF16), vm((4, 4, 64, 1024), F32), vm((4, 4, 64, 1024), F32),
            *STATS_SCRATCH, *SUM_SEMS, *SUM_SEMS, *SUM_SEMS, *GATHER_SEMS, *GATHER_SEMS, *GATHER_SEMS,
            *one_scratch(512), *one_scratch(512),
        ],
        compiler_params=params(1),
        name="policy",
    )(*args)


def halves(value):
    high = value.astype(BF16)
    return high, (value - high.astype(F32)).astype(BF16)


UP_A, UP_B, DOWN_A, DOWN_B, OUT, SMALL, SUM_A, SUM_B = range(8)
ORDER = ("xz", "zx", "xz", "zx", "zx", "xz", "xz", "zx")
WIDTH = (512, 512, 512, 512, 256, 128, 384, 384)
PART = (64, 64, 64, 64, 64, 64, 16, 16)
LOADS = (
    ((4, 4, 16, 768), F32), ((4, 64, 512), F32), ((4, 64, 512), F32), ((4, 4, 64, 1024), F32),
    ((1024, 256), BF16), ((1024, 256), BF16), ((1024, 256), BF16), ((256, 1024), BF16), ((256, 1024), BF16),
    ((1024, 128), F32), ((8, 1024), F32), ((8, 1024), F32), ((4, 4, 64, 256), F32),
)


def tail_kernel(*refs):
    n = len(LOADS)
    hbm, outs, held, rest = refs[:n], refs[n : n + 7], refs[n + 7 : 2 * n + 7], refs[2 * n + 7 :]
    load_sem, full_a, full_b, near_sem, far_sem, mine_ref, dt_ref, vec_ref, small4, mp_buf, mp_sem = rest[:11]
    rest = rest[11:]
    sums4, res_a, res_b, down_ref, wq_ref, wk_ref, wv_ref, ht_ref, obs_ref, small_ref, gf_ref, gm_ref, out_ref = held
    loads = [pltpu.make_async_copy(a, b, load_sem.at[k]) for k, (a, b) in enumerate(zip(hbm, held))]
    for cp in loads:
        cp.start()
    d, m, c, l = place()
    x, z, yh = axes_place()
    yother = (d + 1 - 2 * yh, m)
    peers = [(d, lax.rem(m + j, 4)) for j in (1, 2, 3)]
    greet([at_x(1), at_x(3), at_z(1), at_z(3), yother] + peers)

    first, second, results, ends = {}, [], [res_a, res_b], []
    sources = {
        DOWN_A: (down_ref, pl.ds(0, 512)), DOWN_B: (down_ref, pl.ds(512, 512)), OUT: (out_ref, slice(None)),
        SMALL: (small4, slice(None)), SUM_A: (sums4, pl.ds(0, 384)), SUM_B: (sums4, pl.ds(384, 384)),
    }
    for i in range(2, 8):
        mid, fl, fr, sems, res = rest[:5]
        rest = rest[5:]
        src, cols = sources[i]
        first[i] = ring_one(ORDER[i], src, (mid, fl, fr), sems, cols)
        results.append(res)
    for i in range(8):
        mid, fl, fr, res, ybuf, sems, ysem = rest[:7]
        rest = rest[7:]
        second.append(ring_two(ORDER[i], results[i], (mid, fl, fr), sems))
        ends.append((res, ybuf, ysem))
    tails = {}

    def turn(i):
        first[i].finish(lambda h: results[i].at[pl.ds(h * 2, 2)])
        second[i].start()

    def send_tail(i):
        res, ybuf, ysem = ends[i]
        half = res.shape[0] // 2
        second[i].finish(lambda h: res.at[pl.ds(h * half, half)])
        src = res if i in (SUM_A, SUM_B) else res.at[rows((1 - yh) * 32, 32)]
        tails[i] = remote(src, ybuf, ysem, (), yother)

    loads[0].wait()
    first[SUM_A].start()
    first[SUM_B].start()
    loads[1].wait()
    loads[2].wait()
    second[UP_A].start()
    second[UP_B].start()
    loads[3].wait()
    first[DOWN_A].start()
    first[DOWN_B].start()
    for cp in loads[4:]:
        cp.wait()
    high, low = halves(sums4[...].reshape(256, 768))
    dt_ref[...] = jnp.zeros_like(dt_ref)
    for n, w in enumerate((wq_ref, wk_ref, wv_ref)):
        cols = slice(n * 256, (n + 1) * 256)
        dt_ref[...] += dot(high[:, cols], w[...], (1, 1)) + dot(low[:, cols], w[...], (1, 1))
    vec_ref[0:8] = gf_ref[...]
    vec_ref[8:16] = gm_ref[...]
    vec_ref[16:32] = jnp.zeros((16, 1024), F32)

    def gain_rows(i):
        at = pl.ds(i, 32)
        x = obs_ref[at, :].astype(F32)
        vec_ref[16:24] += fold8(dt_ref[at, :] * x * inverse_rms(x))

    by_blocks(256, 32, gain_rows)
    place_at = (iota((32, 128), 1) == 17 + iota((32, 128), 0) // 8).astype(BF16)
    vec = vec_ref[...]
    high, low = halves(vec)
    lowest = (vec - high.astype(F32) - low.astype(F32)).astype(BF16)
    small = small_ref[...] + sum(dot(part, place_at, (0, 0)) for part in (high, low, lowest))
    small4[...] = small.reshape(4, 4, 64, 128)
    for i in (SUM_A, SUM_B):
        first[i].middle()
    first[OUT].start()
    first[SMALL].start()
    for i in (SUM_A, SUM_B):
        turn(i)
    for i in (UP_A, UP_B, SUM_A, SUM_B):
        second[i].middle()
    for i in (DOWN_A, DOWN_B):
        first[i].middle()
    for i in (SUM_A, SUM_B, UP_A, UP_B):
        send_tail(i)
    for i in (SUM_A, SUM_B):
        tails[i].wait_recv()
    full_a[x, z] = ends[SUM_A][0][...] + ends[SUM_A][1][...]
    full_b[x, z] = ends[SUM_B][0][...] + ends[SUM_B][1][...]
    near = [remote(full_a.at[x, z], full_a.at[x, z], near_sem, (0, j - 1), at_z(j)) for j in (1, 2, 3)]
    near += [remote(full_b.at[x, z], full_b.at[x, z], near_sem, (1, j - 1), at_x(j)) for j in (1, 2, 3)]
    for i in (OUT, SMALL):
        first[i].middle()
    turn(DOWN_A)
    turn(DOWN_B)
    for cp in near:
        cp.wait_recv()
    wide = [remote(full_a.at[x], full_a.at[x], far_sem, (0, j - 1), at_x(j)) for j in (1, 2, 3)]
    wide += [remote(full_b.at[:, z], full_b.at[:, z], far_sem, (1, j - 1), at_z(j)) for j in (1, 2, 3)]
    turn(SMALL)
    turn(OUT)
    for i in (DOWN_A, DOWN_B, SMALL, OUT):
        second[i].middle()
    for i in (DOWN_A, DOWN_B, SMALL, OUT):
        send_tail(i)

    def total(i, put):
        res, ybuf, _ = ends[i]
        by_blocks(32, 8, lambda k: put(k, res[rows(yh * 32 + k, 8), :] + ybuf[pl.ds(k, 8), :]))

    def to_out(ref):
        def put(k, value):
            ref[pl.ds(k, 8), :] = value

        return put

    def to_mp(k, value):
        mp_buf[m, pl.ds(k, 8), :] = value

    shares = []
    for i in (UP_A, UP_B, DOWN_A, DOWN_B, SMALL, OUT):
        tails[i].wait_recv()
        if i == SMALL:
            total(i, to_mp)
            shares = [remote(mp_buf.at[m], mp_buf.at[m], mp_sem, (j,), dev) for j, dev in enumerate(peers)]
        else:
            total(i, to_out(outs[i]))
    for cp in wide:
        cp.wait_recv()
    table = ht_ref[:, rows((d // 4) * 128, 128)]
    for n, ref in enumerate((full_a, full_b)):
        high, low = halves(ref[...].reshape(256, 384))
        mine_ref[:, n * 384 : (n + 1) * 384] = dot(table, high, (0, 0)) + dot(table, low, (0, 0))
    outs[6][...] = mine_ref[rows((d % 4) * 32, 32), :]
    for cp in shares:
        cp.wait_recv()
    outs[SMALL][...] = mp_buf[0] + mp_buf[1] + mp_buf[2] + mp_buf[3]
    for cp in [*shares, *tails.values(), *near, *wide]:
        cp.wait_send()
    for ring in [*first.values(), *second]:
        ring.drain()


def tail(*args):
    vm, dma = pltpu.VMEM, pltpu.SemaphoreType.DMA
    scratch = [vm(shape, kind) for shape, kind in LOADS]
    scratch += [
        dma((len(LOADS),)), vm((4, 4, 16, 384), F32), vm((4, 4, 16, 384), F32), dma((2, 2, 3)), dma((2, 2, 3)), vm((128, 768), F32),
        vm((256, 1024), F32), vm((32, 1024), F32), vm((4, 4, 64, 128), F32), vm((4, 32, 128), F32), dma((2, 3)),
    ]
    for i in range(2, 8):
        scratch += one_scratch(WIDTH[i], PART[i]) + [vm((4, PART[i], WIDTH[i]), F32)]
    for i in range(8):
        scratch += two_scratch(WIDTH[i], PART[i], 16 if i in (SUM_A, SUM_B) else 32)
    return pl.pallas_call(
        tail_kernel,
        out_shape=tuple(jax.ShapeDtypeStruct((32, w), F32) for w in (*WIDTH[:6], 768)),
        in_specs=[ANY] * len(LOADS),
        out_specs=tuple([VMEM] * 7),
        scratch_shapes=scratch,
        compiler_params=params(2),
        name="tail",
    )(*args)


def write_kernel(
    up_a, up_b, down_a, down_b, out_ref, small_ref, qkv_ref,
    o_q, o_k, o_v, o_out, o_up, o_down, o_actor, o_critic, o_final, o_mlp, o_attn,
):
    o_q[...] = qkv_ref[:, :256]
    o_k[...] = qkv_ref[:, 256:512]
    o_v[...] = qkv_ref[:, 512:]
    o_up[:, :512] = up_a[...]
    o_up[:, 512:] = up_b[...]
    o_out[...] = out_ref[...]
    o_down[:, :512] = down_a[...]
    o_down[:, 512:] = down_b[...]
    flat = jnp.transpose(small_ref[...])
    o_actor[...] = flat[:16, :]
    o_critic[...] = flat[16:17, :]
    o_final[...] = flat[17:18, :]
    o_mlp[...] = flat[18:19, :]
    own = jnp.transpose(small_ref[rows(lax.axis_index("mp") * 8, 8), :])
    o_attn[...] = own[19:20, :]


def write_outputs(*parts):
    sd = jax.ShapeDtypeStruct
    shapes = [(32, 256)] * 4 + [(32, 1024)] * 2 + [(16, 32)] + [(1, 32)] * 3 + [(1, 8)]
    return pl.pallas_call(
        write_kernel,
        out_shape=tuple(sd(shape, F32) for shape in shapes),
        in_specs=[VMEM] * 7,
        out_specs=tuple([VMEM] * 11),
        name="write_outputs",
    )(*parts)


def per_device(
    initial_state,
    actions,
    next_state,
    reward_table,
    reward_scale,
    observe_table,
    gain_attn,
    w_query,
    w_key,
    w_value,
    w_out,
    gain_mlp,
    w_up,
    w_down,
    gain_final,
    actor_head,
    critic_head,
):
    token_total = actions.size * lax.axis_size("dp")

    def line(vector):
        return vector.reshape(1, -1)

    h_table, grad_down, grad_heads, final_terms, mlp_terms, res_a, res_b, state_sums, grad_out = policy(
        token_total,
        line(initial_state), actions.T, line(reward_scale), next_state.T, reward_table.T, observe_table,
        line(gain_attn), w_query, w_key, w_value, w_out, line(gain_mlp), line(gain_final),
        actor_head.T, line(critic_head), w_up, w_down,
    )
    parts = tail(
        state_sums.reshape(4, 4, 16, 768), res_a, res_b, grad_down, w_query, w_key, w_value, h_table,
        observe_table, grad_heads, final_terms, mlp_terms, grad_out,
    )
    q, k, v, out, up, down, actor, critic, final, mlp, attn = write_outputs(*parts)
    return (
        q, k, v, out.T, up, down.T, attn.reshape(-1), mlp.reshape(-1), final.reshape(-1), actor.T,
        critic.reshape(-1),
    )


def solution(mesh):
    return jax.shard_map(
        per_device,
        mesh=mesh,
        in_specs=(
            P("dp"),
            P("dp", None),
            P(),
            P(),
            P("dp"),
            P(),
            P(),
            P(None, "mp"),
            P(None, "mp"),
            P(None, "mp"),
            P("mp", None),
            P(),
            P(None, "mp"),
            P("mp", None),
            P(),
            P(),
            P(),
        ),
        out_specs=(
            P("dp", "mp"),
            P("dp", "mp"),
            P("dp", "mp"),
            P("mp", "dp"),
            P("dp", "mp"),
            P("mp", "dp"),
            P(("dp", "mp")),
            P("dp"),
            P("dp"),
            P("dp", None),
            P("dp"),
        ),
        check_vma=False,
    )
```

```python
import functools
import math

import jax
import jax.numpy as jnp
from jax import lax
from jax.experimental import pallas as pl
from jax.experimental.pallas import tpu as pltpu
from jax.sharding import PartitionSpec as P

HEAD_DIM = 128
STEPS = 16
EPS = 1e-05
GAMMA = 0.9
VALUE_COEF = 0.5
ENTROPY_COEF = 0.1
SCALE = 1.0 / math.sqrt(HEAD_DIM)
MESH = pl.DeviceIdType.MESH
VMEM = pl.BlockSpec(memory_space=pltpu.VMEM)
WIDE = 1024
ANY = pl.BlockSpec(memory_space=pl.ANY)
F32 = jnp.float32
BF16 = jnp.bfloat16


def place():
    d, m = lax.axis_index("dp"), lax.axis_index("mp")
    return d, m, m % 2, m // 2


def axes_place():
    d, m, c, l = place()
    return d // 8, (d // 2) % 4, d % 2


def partners():
    d, m, c, l = place()
    over = m + 2 - 4 * l
    return (d, m + 1 - 2 * c), (d, over), (d + 1 - 2 * (d % 2), over)


def at_x(k):
    d, m, c, l = place()
    x, z, yh = axes_place()
    return (lax.rem(x + k, 4) * 8 + z * 2 + yh, m)


def at_z(k):
    d, m, c, l = place()
    x, z, yh = axes_place()
    return (x * 8 + lax.rem(z + k, 4) * 2 + yh, m)


def stats_devices():
    d, m, c, l = place()
    x, z, yh = axes_place()
    plane, column = [], []
    for j in range(1, 16):
        other = lax.rem(x * 4 + z + j, 16)
        plane.append(((other // 4) * 8 + (other % 4) * 2 + yh, m))
    for j in range(1, 8):
        other = lax.rem(yh * 4 + m + j, 8)
        column.append((x * 8 + z * 2 + other // 4, other % 4))
    return plane, column


def greet(devices):
    barrier = pltpu.get_barrier_semaphore()
    for dev in devices:
        pl.semaphore_signal(barrier, inc=1, device_id=dev, device_id_type=MESH)
    pl.semaphore_wait(barrier, len(devices))


def remote(src, dst, sems, at, dev):
    cp = pltpu.make_async_remote_copy(
        src_ref=src, dst_ref=dst, send_sem=sems.at[(0, *at)], recv_sem=sems.at[(1, *at)],
        device_id=dev, device_id_type=MESH,
    )
    cp.start()
    return cp


def rows(start, size):
    return pl.ds(pl.multiple_of(start, size), size)


def by_blocks(total, block, body):
    lax.fori_loop(0, total // block, lambda i, z: (body(pl.multiple_of(i * block, block)), z)[1], 0)


def dot(left, right, contract, **kw):
    return lax.dot_general(
        left, right, ((contract[:1], contract[1:]), ((), ())), preferred_element_type=F32, **kw
    )


def iota(shape, axis):
    return lax.broadcasted_iota(jnp.int32, shape, axis)


def fold8(term):
    total = term[0:8]
    for k in range(1, term.shape[0] // 8):
        total = total + term[8 * k : 8 * k + 8]
    return total


def inverse_rms(x):
    return lax.rsqrt(jnp.mean(x * x, axis=-1, keepdims=True) + EPS)


def norm_back(x, inv, gain, up):
    weighted = up * gain
    return inv * weighted - x * (inv * inv * inv) * jnp.mean(x * weighted, axis=-1, keepdims=True)


def block_at(h, core, low):
    return h * 512 + core * 256 + low * 128


CHUNKS = [(h, k) for k in range(2) for h in range(2)]


class Sums:
    def __init__(self, p, near_own, near_far, far, sems):
        d, m, self.c, self.l = place()
        self.core, *self.over = partners()
        self.p, self.near_own, self.near_far, self.far = p, near_own, near_far, far
        self.own_sem, self.near_sem, self.far_sem = sems
        self.own, self.near, self.sent = {}, {}, {}

    def give_own(self):
        for h in range(2):
            src = self.p.at[rows(block_at(h, 1 - self.c, self.l), 128)]
            self.own[h] = remote(src, self.near_own.at[h], self.own_sem, (h,), self.core)

    def give_far(self, k):
        for h in range(2):
            src = self.p.at[rows(block_at(h, 1 - self.c, 1 - self.l) + k * 64, 64)]
            self.near[h, k] = remote(src, self.near_far.at[h, k], self.near_sem, (h, k), self.core)

    def pass_far(self, k):
        for h in range(2):
            self.near[h, k].wait_recv()
            base = block_at(h, self.c, 1 - self.l) + k * 64

            def body(i, h=h, base=base):
                self.near_far[h, k, pl.ds(i, 32), :] += self.p[rows(base + i, 32), :]

            by_blocks(64, 32, body)
            self.sent[h, k] = remote(
                self.near_far.at[h, k], self.far.at[h, k], self.far_sem, (h, k), self.over[h]
            )

    def take_own(self):
        for h in range(2):
            self.own[h].wait_recv()

    def take(self, h, k):
        self.sent[h, k].wait_recv()

    def value(self, h, k, i):
        mine = self.p[rows(block_at(h, self.c, self.l) + k * 64 + i, 32), :]
        return mine + self.near_own[h, pl.ds(k * 64 + i, 32), :] + self.far[h, k, pl.ds(i, 32), :]

    def drain(self):
        for group in (self.own, self.near, self.sent):
            for cp in group.values():
                cp.wait_send()


class Gather:
    def __init__(self, q, whole, low, sems):
        d, m, self.c, self.l = place()
        self.core, *self.over = partners()
        self.q, self.whole, self.low = q, whole, low
        self.over_sem, self.core_sem, self.fwd_sem = sems
        self.far, self.near, self.fwd, self.left = {}, {}, {}, set()

    def keep(self, base, src=None, at=0):
        def body(i):
            value = self.whole[rows(base + i, 32), :] if src is None else src[pl.ds(at + i, 32), :]
            self.low[rows(base + i, 32), :] = value.astype(BF16)

        by_blocks(64, 32, body)

    def send(self, h, k):
        base = block_at(h, self.c, self.l) + k * 64
        src, dst = self.q.at[pl.ds(h * 128 + k * 64, 64)], self.whole.at[rows(base, 64)]
        self.far[h, k] = remote(src, dst, self.over_sem, (h, k), self.over[h])
        self.near[h, k] = remote(src, dst, self.core_sem, (h, k), self.core)
        self.keep(base, self.q, h * 128 + k * 64)

    def take_core(self, h, k):
        self.near[h, k].wait_recv()
        self.keep(block_at(h, 1 - self.c, self.l) + k * 64)

    def take_far(self, h, k):
        self.far[h, k].wait_recv()
        base = block_at(h, self.c, 1 - self.l) + k * 64
        at = self.whole.at[rows(base, 64)]
        self.fwd[h, k] = remote(at, at, self.fwd_sem, (h, k), self.core)
        self.keep(base)

    def forwarded(self, k):
        for h in range(2):
            self.fwd[h, k].wait_send()
        self.left.add(k)

    def take_fwd(self, h, k):
        self.fwd[h, k].wait_recv()
        self.keep(block_at(h, 1 - self.c, 1 - self.l) + k * 64)

    def drain(self):
        late = [cp for (h, k), cp in self.fwd.items() if k not in self.left]
        for cp in [*self.far.values(), *self.near.values(), *late]:
            cp.wait_send()


SUM_SEMS = [
    pltpu.SemaphoreType.DMA((2, 2)), pltpu.SemaphoreType.DMA((2, 2, 2)), pltpu.SemaphoreType.DMA((2, 2, 2)),
]
GATHER_SEMS = [pltpu.SemaphoreType.DMA((2, 2, 2))] * 3


def gather_work_sum(gather, sums, work):
    c, l = sums.c, sums.l
    work([(block_at(h, c, l), 128) for h in range(2)])
    for h, k in CHUNKS:
        gather.take_core(h, k)
    work([(block_at(h, 1 - c, l), 128) for h in range(2)])
    sums.give_own()
    for k in range(2):
        for h in range(2):
            gather.take_far(h, k)
        work([(block_at(h, c, 1 - l) + k * 64, 64) for h in range(2)])
        for h in range(2):
            gather.take_fwd(h, k)
        work([(block_at(h, 1 - c, 1 - l) + k * 64, 64) for h in range(2)])
        sums.give_far(k)
        gather.forwarded(k)
        sums.pass_far(k)
    sums.take_own()


def spans_of(ref, spans, cols=slice(None)):
    return jnp.concatenate([ref[rows(at, n), cols] for at, n in spans], axis=0)


def put_spans(ref, spans, cols, value):
    done = 0
    for at, n in spans:
        ref[rows(at, n), cols] = value[done : done + n]
        done += n


def sum_everywhere(value, between, ps, cs, psem, csem):
    d, m, c, l = place()
    x, z, yh = axes_place()
    plane, column = stats_devices()

    def stage(slots, sems, devs, me, value, between=None):
        slots[me] = value
        copies = [remote(slots.at[me], slots.at[me], sems, (j,), dev) for j, dev in enumerate(devs)]
        done = between() if between is not None else None
        for cp in copies:
            cp.wait_recv()
        total = slots[0]
        for k in range(1, len(devs) + 1):
            total = total + slots[k]
        for cp in copies:
            cp.wait_send()
        return total, done

    value, done = stage(ps, psem, plane, x * 4 + z, value, between)
    return stage(cs, csem, column, yh * 4 + m, value)[0], done


STATS_SCRATCH = [
    pltpu.VMEM((16, 8, 128), F32),
    pltpu.VMEM((8, 8, 128), F32),
    pltpu.SemaphoreType.DMA((2, 15)),
    pltpu.SemaphoreType.DMA((2, 7)),
]


class Ring:
    def __init__(self, src, bufs, sems, pos, right, left):
        self.src, self.pos, self.right, self.left = src, pos, right, left
        self.mid, self.fl, self.fr = bufs
        self.sems = sems
        self.copies = []

    def send(self, src, dst, dev):
        self.copies.append(remote(src, dst, self.sems, (len(self.copies),), dev))

    def start(self):
        p = self.pos
        self.r, self.l, opp = lax.rem(p + 1, 4), lax.rem(p + 3, 4), lax.rem(p + 2, 4)
        self.send(self.src(opp, 0), self.mid.at[0], self.right)
        self.send(self.src(opp, 1), self.mid.at[1], self.left)
        self.send(self.src(self.r, 1), self.fl.at[1], self.right)
        self.send(self.src(self.l, 0), self.fr.at[0], self.left)

    def middle(self):
        self.copies[0].wait_recv()
        add_into(self.mid.at[0], self.src(self.r, 0))
        self.send(self.mid.at[0], self.fl.at[0], self.right)
        self.copies[1].wait_recv()
        add_into(self.mid.at[1], self.src(self.l, 1))
        self.send(self.mid.at[1], self.fr.at[1], self.left)

    def finish(self, out):
        for k in (2, 3, 4, 5):
            self.copies[k].wait_recv()
        for half in range(2):
            add_three(out(half), self.src(self.pos, half), self.fl.at[half], self.fr.at[half])

    def drain(self):
        for cp in self.copies:
            cp.wait_send()


def each_block(ref, body):
    n = min(16, ref.shape[-2])
    if len(ref.shape) == 3:
        for k in range(ref.shape[0]):
            by_blocks(ref.shape[1], n, lambda i, k=k: body((k, pl.ds(i, n), slice(None))))
    else:
        by_blocks(ref.shape[0], n, lambda i: body((pl.ds(i, n), slice(None))))


def add_into(dst, src):
    def body(at):
        dst[at] += src[at]

    each_block(dst, body)


def add_three(dst, a, b, c):
    def body(at):
        dst[at] = a[at] + b[at] + c[at]

    each_block(dst, body)


def ring_one(order, src, bufs, sems, cols=slice(None)):
    x, z, yh = axes_place()
    every = slice(None)
    if order == "xz":
        return Ring(lambda j, h: src.at[j, pl.ds(h * 2, 2), every, cols], bufs, sems, x, at_x(1), at_x(3))
    return Ring(lambda j, h: src.at[pl.ds(h * 2, 2), j, every, cols], bufs, sems, z, at_z(1), at_z(3))


def ring_two(order, res, bufs, sems):
    x, z, yh = axes_place()

    half = res.shape[1] // 2

    def src(j, h):
        return res.at[j, pl.ds(h * half, half)]

    if order == "xz":
        return Ring(src, bufs, sems, z, at_z(1), at_z(3))
    return Ring(src, bufs, sems, x, at_x(1), at_x(3))


def one_scratch(w, part=64):
    return [pltpu.VMEM((2, 2, part, w), F32)] * 3 + [pltpu.SemaphoreType.DMA((2, 6))]


def two_scratch(w, part=64, kept=32):
    return [
        *[pltpu.VMEM((2, part // 2, w), F32)] * 3,
        pltpu.VMEM((part, w), F32),
        pltpu.VMEM((kept, w), F32),
        pltpu.SemaphoreType.DMA((2, 6)),
        pltpu.SemaphoreType.DMA((2,)),
    ]


def params(n):
    return pltpu.CompilerParams(
        collective_id=n, has_side_effects=True, vmem_limit_bytes=63 * 1024 * 1024
    )


def block_probs(q, k):
    r, s = iota((128, 128), 0), iota((128, 128), 1)
    seen = ((r // STEPS) == (s // STEPS)) & (r >= s)
    weights = jnp.where(seen, jnp.exp(dot(q, k, (1, 1)) * SCALE), 0.0)
    return weights / jnp.sum(weights, axis=-1, keepdims=True)


def policy_kernel(
    token_total,
    init_ref, act_ref, scale_ref, next_ref, rew_ref, obs_ref, gain_attn, wq_ref, wk_ref, wv_ref, wo_ref,
    gain_mlp, gain_fin, actor_ref, critic_ref, up_hbm, down_hbm,
    ht_out, down_out, gh_ref, g_fin, g_mlp, res_a, res_b, state_sums, out_ref,
    low_one, qkv_ref, match_ref, mixed_ref, ht_ref, flush_sem,
    r_init, r_act, r_scale, roll_sem, tables, st_ref, own_ref, head_f, heads,
    w_up, w_down, w_sem,
    p, near_own, near_far, far, whole, h_two, up_rows, hidden, low_two, d_up, x_one, dx_two, buf_a, buf_b,
    fin_ref, grad_up, grad_down, *rest,
):
    stats, rest = rest[:4], rest[4:]
    sems_a, sems_b, sems_d = rest[0:3], rest[3:6], rest[6:9]
    gs_b, gs_d, gs_e = rest[9:12], rest[12:15], rest[15:18]
    ring_a, ring_b = rest[18:22], rest[22:26]
    flushed = []

    def flush(src, dst):
        cp = pltpu.make_async_copy(src, dst, flush_sem.at[len(flushed)])
        cp.start()
        flushed.append(cp)

    d, m, c, l = place()
    weights = [
        pltpu.make_async_copy(up_hbm, w_up, w_sem.at[0]), pltpu.make_async_copy(down_hbm, w_down, w_sem.at[1]),
    ]
    for cp in weights:
        cp.start()
    plane, column = stats_devices()
    greet(plane + column)
    far_dev = partners()[2]
    copies = [
        remote(src, dst, roll_sem, (n,), far_dev)
        for n, (src, dst) in enumerate(((init_ref, r_init), (act_ref, r_act), (scale_ref, r_scale)))
    ]

    def table_rows(i):
        at = pl.ds(i, 32)
        x = obs_ref[at, :].astype(F32)
        ht_ref[at, :] = (x * inverse_rms(x) * gain_attn[...]).astype(BF16)

    by_blocks(256, 32, table_rows)
    flush(ht_ref, ht_out)
    for n, w in enumerate((wq_ref, wk_ref, wv_ref)):
        tables[:, n * 256 : (n + 1) * 256] = dot(ht_ref[...], w[...], (1, 0)).astype(BF16)
    head_f[...] = jnp.zeros_like(head_f)
    head_f[0:16, :] = actor_ref[...].astype(F32)
    head_f[16:17, :] = critic_ref[...].astype(F32)
    heads[...] = jnp.zeros_like(heads)
    heads[0:32, :] = head_f[...].astype(BF16)

    for cp in copies:
        cp.wait()
    swap = 32 + 64 * l
    lane = iota((1, 64), 1)
    state = jnp.where(lane >= swap, r_init[...], init_ref[...]).astype(F32)
    scale = jnp.where(lane >= swap, r_scale[...], scale_ref[...])
    act_t = jnp.where(iota((16, 64), 1) >= swap, r_act[...], act_ref[...]).astype(F32)
    nexts = next_ref[...].astype(F32).astype(BF16)
    ids, kinds = iota((256, 64), 0).astype(F32), iota((16, 64), 0).astype(F32)
    for t in range(STEPS):
        st_ref[pl.ds(t, 1), :] = state
        if t + 1 < STEPS:
            hit = jnp.where(ids == state, 1.0, 0.0).astype(BF16)
            found = dot(nexts, hit, (1, 0))
            state = jnp.sum(jnp.where(kinds == act_t[t : t + 1, :], found, 0.0), axis=0, keepdims=True)

    pick_t = (iota((128, 16), 0) % STEPS == iota((128, 16), 1)).astype(BF16)
    spread = jnp.ones((64, 128), BF16)
    lanes = iota((128, 128), 1).astype(F32)

    def per_token(rows_by_env, first_env):
        here = iota((128, 64), 1) == first_env + iota((128, 64), 0) // STEPS
        found = jnp.where(here, dot(pick_t, rows_by_env, (1, 0)), 0.0)
        return dot(found.astype(BF16), spread, (1, 0))

    def attend(core, low):
        def block(h, carry):
            at = rows(block_at(h, core, low), 128)
            ids_here = per_token(st_ref[...].astype(BF16), h * 32 + (core * 2 + low) * 8)
            match = jnp.concatenate(
                [jnp.where(ids_here == lanes, 1.0, 0.0), jnp.where(ids_here == lanes + 128.0, 1.0, 0.0)], axis=1
            ).astype(BF16)
            match_ref[at, :] = match
            qkv = dot(match, tables[...], (1, 0)).astype(BF16)
            qkv_ref[at, :] = qkv
            outs = []
            for n in range(2):
                q, k, v = (qkv[:, j * 256 + n * 128 : j * 256 + (n + 1) * 128] for j in range(3))
                outs.append(dot(block_probs(q, k).astype(BF16), v, (1, 0)).astype(BF16))
            mixed = jnp.concatenate(outs, axis=1)
            mixed_ref[at, :] = mixed
            p[at, :] = dot(mixed, wo_ref[...], (1, 0))
            return carry

        lax.fori_loop(0, 2, block, 0, unroll=True)

    sums = Sums(p, near_own, near_far, far, sems_a)
    attend(1 - c, 1 - l)
    sums.give_far(0)
    sums.give_far(1)
    attend(c, 1 - l)
    sums.pass_far(0)
    sums.pass_far(1)
    attend(1 - c, l)
    sums.give_own()
    attend(c, l)
    for h in range(2):
        at = pl.ds(h * 128, 128)
        mine = match_ref[rows(block_at(h, c, l), 128), :]
        x_one[at, :] = dot(mine, obs_ref[...], (1, 0))
        first_env = h * 32 + (c * 2 + l) * 8
        chosen = jnp.where(per_token(act_t.astype(BF16), first_env) == lanes, 1.0, 0.0)
        found = dot(mine.astype(F32), rew_ref[...], (1, 1), precision=lax.Precision.HIGHEST)
        here = iota((128, 64), 1) == first_env + iota((128, 64), 0) // STEPS
        factor = jnp.sum(jnp.where(here, scale, 0.0), axis=1, keepdims=True)
        reward = jnp.sum(chosen[:, :16] * found, axis=1, keepdims=True) * factor
        own_ref[at, :] = jnp.where(lanes == 16.0, reward, chosen)
    sums.take_own()

    gather = Gather(buf_a, whole, h_two, gs_b)
    for h, k in CHUNKS:
        sums.take(h, k)

        def body(i, h=h, k=k):
            at = pl.ds(h * 128 + k * 64 + i, 32)
            x = sums.value(h, k, i) + x_one[at, :]
            x_one[at, :] = x
            buf_a[at, :] = x * inverse_rms(x) * gain_mlp[...]

        by_blocks(64, 32, body)
        gather.send(h, k)
    sums.drain()
    for cp in weights:
        cp.wait()

    def forward(spans):
        def up(j):
            cols = pl.ds(j, WIDE)
            u = dot(spans_of(h_two, spans), w_up[:, cols], (1, 0))
            put_spans(up_rows, spans, cols, u)
            put_spans(hidden, spans, cols, (u / (1.0 + jnp.exp(-u))).astype(BF16))

        def down(j):
            cols = pl.ds(j, WIDE)
            put_spans(p, spans, cols, dot(spans_of(hidden, spans), w_down[:, cols], (1, 0)))

        by_blocks(1024, WIDE, up)
        by_blocks(1024, WIDE, down)

    sums = Sums(p, near_own, near_far, far, sems_b)
    gather_work_sum(gather, sums, forward)
    for h, k in CHUNKS:
        sums.take(h, k)

        def body(i, h=h, k=k):
            at = pl.ds(h * 128 + k * 64 + i, 32)
            x = sums.value(h, k, i) + x_one[at, :]
            buf_b[at, :] = x
            fin_ref[at, :] = (x * inverse_rms(x) * gain_fin[...]).astype(BF16)

        by_blocks(64, 32, body)
    gather.drain()
    sums.drain()

    lane = iota((256, 128), 1)
    both = dot(fin_ref[...], heads[...], (1, 1))
    critic = jnp.sum(jnp.where(lane == 16, both, 0.0), axis=1, keepdims=True)
    own = own_ref[...]
    reward = jnp.sum(jnp.where(lane == 16, own, 0.0), axis=1, keepdims=True)
    step = iota((256, 128), 0) % STEPS
    base = reward + jnp.where(step == STEPS - 1, GAMMA * critic, 0.0)
    r, s = iota((256, 256), 0), iota((256, 256), 1)
    ahead = ((r // STEPS) == (s // STEPS)) & (s >= r)
    decay = jnp.where(ahead, jnp.exp((s - r).astype(F32) * math.log(GAMMA)), 0.0)
    returns = dot(decay, base, (1, 0), precision=lax.Precision.HIGHEST)
    advantage = returns - critic
    tile = jnp.where(
        iota((8, 128), 0) == 0,
        jnp.sum(advantage, axis=0, keepdims=True),
        jnp.sum(advantage * advantage, axis=0, keepdims=True),
    )
    real = lane < 16
    factor = 1.0 / math.sqrt(token_total)

    def policy_terms():
        logits = jnp.where(real, both, 0.0)
        mass = jnp.sum(jnp.where(real, jnp.exp(logits), 0.0), axis=1, keepdims=True)
        logp = jnp.where(real, logits - jnp.log(mass), 0.0)
        chance = jnp.where(real, jnp.exp(logp), 0.0)
        entropy = -jnp.sum(chance * logp, axis=1, keepdims=True)
        picked = jnp.where(real, own, 0.0)
        d_value = (factor * VALUE_COEF) * (critic - returns)
        return picked - chance, ENTROPY_COEF * chance * (logp + entropy), d_value

    totals, (push, calm, d_value) = sum_everywhere(tile, policy_terms, *stats)
    mean = totals[0:1, :] * (1.0 / token_total)
    variance = totals[1:2, :] * (1.0 / token_total) - mean * mean
    normed = (advantage - mean) * lax.rsqrt(variance + EPS)
    d_logits = factor * (-normed * push + calm)
    d_both = jnp.where(real, d_logits, jnp.where(lane == 16, d_value, 0.0)).astype(BF16)
    buf_a[...] = dot(d_both, heads[...], (1, 0))
    g_fin[...] = jnp.zeros_like(g_fin)
    g_mlp[...] = jnp.zeros_like(g_mlp)

    gather = Gather(dx_two, whole, low_two, gs_d)
    for h, k in CHUNKS:

        def body(i, h=h, k=k):
            at = pl.ds(h * 128 + k * 64 + i, 32)
            x, up = buf_b[at, :], buf_a[at, :]
            inv = inverse_rms(x)
            dx_two[at, :] = norm_back(x, inv, gain_fin[...], up)
            g_fin[...] += fold8(up * x * inv)

        by_blocks(64, 32, body)
        gather.send(h, k)
    gh_ref[...] = dot(fin_ref[...], d_both, (0, 0))

    def backward(spans):
        def up(j):
            cols = pl.ds(j, WIDE)
            d_hidden = dot(spans_of(low_two, spans), w_down[cols, :], (1, 1)).astype(BF16).astype(F32)
            u = spans_of(up_rows, spans, cols)
            sig = 1.0 / (1.0 + jnp.exp(-u))
            put_spans(d_up, spans, cols, (d_hidden * sig * (1.0 + u * (1.0 - sig))).astype(BF16))

        def down(j):
            cols = pl.ds(j, WIDE)
            put_spans(p, spans, cols, dot(spans_of(d_up, spans), w_up[cols, :], (1, 1)))

        by_blocks(1024, WIDE, up)
        by_blocks(1024, WIDE, down)

    sums = Sums(p, near_own, near_far, far, sems_d)
    gather_work_sum(gather, sums, backward)

    def weight_grad(out, left, right):
        def tile(j, carry):
            cols = rows(j * 256, 256)
            out[j] = dot(left[:, cols], right[...], (0, 0)).reshape(4, 64, 1024)
            return carry

        lax.fori_loop(0, 4, tile, 0)

    rings = [
        ring_one("xz", grad_up, ring_a[:3], ring_a[3], pl.ds(0, 512)),
        ring_one("zx", grad_up, ring_b[:3], ring_b[3], pl.ds(512, 512)),
    ]
    weight_grad(grad_up, h_two, d_up)
    for ring in rings:
        ring.start()
    weight_grad(grad_down, low_two, hidden)
    flush(grad_down, down_out)
    gather.drain()

    def attend_back(spans):
        d_mixed = dot(spans_of(low_one, spans), wo_ref[...], (1, 1)).astype(BF16)
        qkv = spans_of(qkv_ref, spans)
        parts = [[], [], []]
        for n in range(2):
            q, k, v = (qkv[:, j * 256 + n * 128 : j * 256 + (n + 1) * 128] for j in range(3))
            up = d_mixed[:, n * 128 : (n + 1) * 128]
            probs = block_probs(q, k)
            d_probs = dot(up, v, (1, 1))
            parts[2].append(dot(probs.astype(BF16), up, (0, 0)).astype(BF16))
            d_scores = (
                probs * (d_probs - jnp.sum(probs * d_probs, axis=-1, keepdims=True)) * SCALE
            ).astype(BF16)
            parts[0].append(dot(d_scores, k, (1, 0)).astype(BF16))
            parts[1].append(dot(d_scores, q, (0, 0)).astype(BF16))
        d_qkv = jnp.concatenate([*parts[0], *parts[1], *parts[2]], axis=1)
        state_sums[...] += dot(spans_of(match_ref, spans), d_qkv, (0, 0))

    state_sums[...] = jnp.zeros_like(state_sums)
    gather = Gather(buf_b, whole, low_one, gs_e)
    for h, k in CHUNKS:
        sums.take(h, k)

        def body(i, h=h, k=k):
            at = pl.ds(h * 128 + k * 64 + i, 32)
            up, x = sums.value(h, k, i), x_one[at, :]
            inv = inverse_rms(x)
            buf_b[at, :] = dx_two[at, :] + norm_back(x, inv, gain_mlp[...], up)
            g_mlp[...] += fold8(up * x * inv)

        by_blocks(64, 32, body)
        gather.send(h, k)
    sums.drain()
    for h in range(2):
        attend_back([(block_at(h, c, l), 128)])
    for h, k in CHUNKS:
        gather.take_core(h, k)
    for h in range(2):
        gather.take_far(h, 0)
    for ring in rings:
        ring.middle()
    for h in range(2):
        attend_back([(block_at(h, 1 - c, l), 128)])
    for h in range(2):
        gather.take_fwd(h, 0)
    attend_back([(block_at(h, c, 1 - l), 64) for h in range(2)])
    attend_back([(block_at(h, 1 - c, 1 - l), 64) for h in range(2)])
    for h in range(2):
        gather.take_far(h, 1)
    attend_back([(block_at(h, c, 1 - l) + 64, 64) for h in range(2)])
    for h in range(2):
        gather.take_fwd(h, 1)
    attend_back([(block_at(h, 1 - c, 1 - l) + 64, 64) for h in range(2)])
    gather.drain()

    def out_tile(j, carry):
        cols = rows(j * 256, 256)
        out_ref[j] = dot(low_one[:, cols], mixed_ref[...], (0, 0)).reshape(4, 64, 256)
        return carry

    lax.fori_loop(0, 4, out_tile, 0)
    for ring, res in zip(rings, (res_a, res_b)):
        ring.finish(lambda h, res=res: res.at[pl.ds(h * 2, 2)])
    for ring in rings:
        ring.drain()
    for cp in flushed:
        cp.wait()


def policy(token_total, *args):
    sd, vm = jax.ShapeDtypeStruct, pltpu.VMEM
    return pl.pallas_call(
        functools.partial(policy_kernel, token_total),
        out_shape=(
            sd((256, 1024), BF16), sd((4, 4, 64, 1024), F32), sd((1024, 128), F32), sd((8, 1024), F32),
            sd((8, 1024), F32), sd((4, 64, 512), F32), sd((4, 64, 512), F32), sd((256, 768), F32),
            sd((4, 4, 64, 256), F32),
        ),
        in_specs=[VMEM] * 15 + [ANY] * 2,
        out_specs=tuple([ANY] * 2 + [VMEM] * 7),
        scratch_shapes=[
            vm((1024, 1024), BF16), vm((1024, 768), BF16), vm((1024, 256), BF16), vm((1024, 256), BF16), vm((256, 1024), BF16),
            pltpu.SemaphoreType.DMA((2,)),
            vm((1, 64), jnp.int32), vm((16, 64), jnp.int32), vm((1, 64), F32), pltpu.SemaphoreType.DMA((2, 3)),
            vm((256, 768), BF16), vm((16, 64), F32), vm((256, 128), F32), vm((32, 1024), F32), vm((128, 1024), BF16),
            vm((1024, 1024), BF16), vm((1024, 1024), BF16), pltpu.SemaphoreType.DMA((2,)),
            vm((1024, 1024), F32), vm((2, 128, 1024), F32), vm((2, 2, 64, 1024), F32), vm((2, 2, 64, 1024), F32),
            vm((1024, 1024), F32), vm((1024, 1024), BF16), vm((1024, 1024), F32), vm((1024, 1024), BF16),
            vm((1024, 1024), BF16), vm((1024, 1024), BF16),
            vm((256, 1024), F32), vm((256, 1024), F32), vm((256, 1024), F32), vm((256, 1024), F32),
            vm((256, 1024), BF16), vm((4, 4, 64, 1024), F32), vm((4, 4, 64, 1024), F32),
            *STATS_SCRATCH, *SUM_SEMS, *SUM_SEMS, *SUM_SEMS, *GATHER_SEMS, *GATHER_SEMS, *GATHER_SEMS,
            *one_scratch(512), *one_scratch(512),
        ],
        compiler_params=params(1),
        name="policy",
    )(*args)


def halves(value):
    high = value.astype(BF16)
    return high, (value - high.astype(F32)).astype(BF16)


UP_A, UP_B, DOWN_A, DOWN_B, OUT, SMALL, SUM_A, SUM_B = range(8)
ORDER = ("xz", "zx", "xz", "zx", "zx", "xz", "xz", "zx")
WIDTH = (512, 512, 512, 512, 256, 128, 384, 384)
PART = (64, 64, 64, 64, 64, 64, 16, 16)
LOADS = (
    ((4, 4, 16, 768), F32), ((4, 64, 512), F32), ((4, 64, 512), F32), ((4, 4, 64, 1024), F32),
    ((1024, 256), BF16), ((1024, 256), BF16), ((1024, 256), BF16), ((256, 1024), BF16), ((256, 1024), BF16),
    ((1024, 128), F32), ((8, 1024), F32), ((8, 1024), F32), ((4, 4, 64, 256), F32),
)


def tail_kernel(*refs):
    n = len(LOADS)
    hbm, outs, held, rest = refs[:n], refs[n : n + 7], refs[n + 7 : 2 * n + 7], refs[2 * n + 7 :]
    load_sem, full_a, full_b, near_sem, far_sem, mine_ref, dt_ref, vec_ref, small4, mp_buf, mp_sem = rest[:11]
    rest = rest[11:]
    sums4, res_a, res_b, down_ref, wq_ref, wk_ref, wv_ref, ht_ref, obs_ref, small_ref, gf_ref, gm_ref, out_ref = held
    loads = [pltpu.make_async_copy(a, b, load_sem.at[k]) for k, (a, b) in enumerate(zip(hbm, held))]
    for cp in loads:
        cp.start()
    d, m, c, l = place()
    x, z, yh = axes_place()
    yother = (d + 1 - 2 * yh, m)
    peers = [(d, lax.rem(m + j, 4)) for j in (1, 2, 3)]
    greet([at_x(1), at_x(3), at_z(1), at_z(3), yother] + peers)

    first, second, results, ends = {}, [], [res_a, res_b], []
    sources = {
        DOWN_A: (down_ref, pl.ds(0, 512)), DOWN_B: (down_ref, pl.ds(512, 512)), OUT: (out_ref, slice(None)),
        SMALL: (small4, slice(None)), SUM_A: (sums4, pl.ds(0, 384)), SUM_B: (sums4, pl.ds(384, 384)),
    }
    for i in range(2, 8):
        mid, fl, fr, sems, res = rest[:5]
        rest = rest[5:]
        src, cols = sources[i]
        first[i] = ring_one(ORDER[i], src, (mid, fl, fr), sems, cols)
        results.append(res)
    for i in range(8):
        mid, fl, fr, res, ybuf, sems, ysem = rest[:7]
        rest = rest[7:]
        second.append(ring_two(ORDER[i], results[i], (mid, fl, fr), sems))
        ends.append((res, ybuf, ysem))
    tails = {}

    def turn(i):
        first[i].finish(lambda h: results[i].at[pl.ds(h * 2, 2)])
        second[i].start()

    def send_tail(i):
        res, ybuf, ysem = ends[i]
        half = res.shape[0] // 2
        second[i].finish(lambda h: res.at[pl.ds(h * half, half)])
        src = res if i in (SUM_A, SUM_B) else res.at[rows((1 - yh) * 32, 32)]
        tails[i] = remote(src, ybuf, ysem, (), yother)

    loads[0].wait()
    first[SUM_A].start()
    first[SUM_B].start()
    loads[1].wait()
    loads[2].wait()
    second[UP_A].start()
    second[UP_B].start()
    loads[3].wait()
    first[DOWN_A].start()
    first[DOWN_B].start()
    for cp in loads[4:]:
        cp.wait()
    high, low = halves(sums4[...].reshape(256, 768))
    dt_ref[...] = jnp.zeros_like(dt_ref)
    for n, w in enumerate((wq_ref, wk_ref, wv_ref)):
        cols = slice(n * 256, (n + 1) * 256)
        dt_ref[...] += dot(high[:, cols], w[...], (1, 1)) + dot(low[:, cols], w[...], (1, 1))
    vec_ref[0:8] = gf_ref[...]
    vec_ref[8:16] = gm_ref[...]
    vec_ref[16:32] = jnp.zeros((16, 1024), F32)

    def gain_rows(i):
        at = pl.ds(i, 32)
        x = obs_ref[at, :].astype(F32)
        vec_ref[16:24] += fold8(dt_ref[at, :] * x * inverse_rms(x))

    by_blocks(256, 32, gain_rows)
    place_at = (iota((32, 128), 1) == 17 + iota((32, 128), 0) // 8).astype(BF16)
    vec = vec_ref[...]
    high, low = halves(vec)
    lowest = (vec - high.astype(F32) - low.astype(F32)).astype(BF16)
    small = small_ref[...] + sum(dot(part, place_at, (0, 0)) for part in (high, low, lowest))
    small4[...] = small.reshape(4, 4, 64, 128)
    for i in (SUM_A, SUM_B):
        first[i].middle()
    for i in (UP_A, UP_B):
        second[i].middle()
    for i in (DOWN_A, DOWN_B):
        first[i].middle()
    for i in (UP_A, UP_B):
        send_tail(i)
    for i in (SUM_A, SUM_B):
        turn(i)
    first[OUT].start()
    first[SMALL].start()
    for i in (DOWN_A, DOWN_B):
        turn(i)
    for i in (SUM_A, SUM_B):
        second[i].middle()
    for i in (SUM_A, SUM_B):
        send_tail(i)
    for i in (DOWN_A, DOWN_B):
        second[i].middle()
    for i in (OUT, SMALL):
        first[i].middle()
    for i in (SUM_A, SUM_B):
        tails[i].wait_recv()
    full_a[x, z] = ends[SUM_A][0][...] + ends[SUM_A][1][...]
    full_b[x, z] = ends[SUM_B][0][...] + ends[SUM_B][1][...]
    near = [remote(full_a.at[x, z], full_a.at[x, z], near_sem, (0, j - 1), at_z(j)) for j in (1, 2, 3)]
    near += [remote(full_b.at[x, z], full_b.at[x, z], near_sem, (1, j - 1), at_x(j)) for j in (1, 2, 3)]
    for i in (DOWN_A, DOWN_B):
        send_tail(i)
    for cp in near:
        cp.wait_recv()
    wide = [remote(full_a.at[x], full_a.at[x], far_sem, (0, j - 1), at_x(j)) for j in (1, 2, 3)]
    wide += [remote(full_b.at[:, z], full_b.at[:, z], far_sem, (1, j - 1), at_z(j)) for j in (1, 2, 3)]
    for i in (SMALL, OUT):
        turn(i)
    for i in (SMALL, OUT):
        second[i].middle()
    for i in (SMALL, OUT):
        send_tail(i)

    def total(i, put):
        res, ybuf, _ = ends[i]
        by_blocks(32, 8, lambda k: put(k, res[rows(yh * 32 + k, 8), :] + ybuf[pl.ds(k, 8), :]))

    def to_out(ref):
        def put(k, value):
            ref[pl.ds(k, 8), :] = value

        return put

    def to_mp(k, value):
        mp_buf[m, pl.ds(k, 8), :] = value

    shares = []
    for i in (UP_A, UP_B, DOWN_A, DOWN_B, SMALL, OUT):
        tails[i].wait_recv()
        if i == SMALL:
            total(i, to_mp)
            shares = [remote(mp_buf.at[m], mp_buf.at[m], mp_sem, (j,), dev) for j, dev in enumerate(peers)]
        else:
            total(i, to_out(outs[i]))
    for cp in wide:
        cp.wait_recv()
    table = ht_ref[:, rows((d // 4) * 128, 128)]
    for n, ref in enumerate((full_a, full_b)):
        high, low = halves(ref[...].reshape(256, 384))
        mine_ref[:, n * 384 : (n + 1) * 384] = dot(table, high, (0, 0)) + dot(table, low, (0, 0))
    outs[6][...] = mine_ref[rows((d % 4) * 32, 32), :]
    for cp in shares:
        cp.wait_recv()
    outs[SMALL][...] = mp_buf[0] + mp_buf[1] + mp_buf[2] + mp_buf[3]
    for cp in [*shares, *tails.values(), *near, *wide]:
        cp.wait_send()
    for ring in [*first.values(), *second]:
        ring.drain()


def tail(*args):
    vm, dma = pltpu.VMEM, pltpu.SemaphoreType.DMA
    scratch = [vm(shape, kind) for shape, kind in LOADS]
    scratch += [
        dma((len(LOADS),)), vm((4, 4, 16, 384), F32), vm((4, 4, 16, 384), F32), dma((2, 2, 3)), dma((2, 2, 3)), vm((128, 768), F32),
        vm((256, 1024), F32), vm((32, 1024), F32), vm((4, 4, 64, 128), F32), vm((4, 32, 128), F32), dma((2, 3)),
    ]
    for i in range(2, 8):
        scratch += one_scratch(WIDTH[i], PART[i]) + [vm((4, PART[i], WIDTH[i]), F32)]
    for i in range(8):
        scratch += two_scratch(WIDTH[i], PART[i], 16 if i in (SUM_A, SUM_B) else 32)
    return pl.pallas_call(
        tail_kernel,
        out_shape=tuple(jax.ShapeDtypeStruct((32, w), F32) for w in (*WIDTH[:6], 768)),
        in_specs=[ANY] * len(LOADS),
        out_specs=tuple([VMEM] * 7),
        scratch_shapes=scratch,
        compiler_params=params(2),
        name="tail",
    )(*args)


def write_kernel(
    up_a, up_b, down_a, down_b, out_ref, small_ref, qkv_ref,
    o_q, o_k, o_v, o_out, o_up, o_down, o_actor, o_critic, o_final, o_mlp, o_attn,
):
    o_q[...] = qkv_ref[:, :256]
    o_k[...] = qkv_ref[:, 256:512]
    o_v[...] = qkv_ref[:, 512:]
    o_up[:, :512] = up_a[...]
    o_up[:, 512:] = up_b[...]
    o_out[...] = out_ref[...]
    o_down[:, :512] = down_a[...]
    o_down[:, 512:] = down_b[...]
    flat = jnp.transpose(small_ref[...])
    o_actor[...] = flat[:16, :]
    o_critic[...] = flat[16:17, :]
    o_final[...] = flat[17:18, :]
    o_mlp[...] = flat[18:19, :]
    own = jnp.transpose(small_ref[rows(lax.axis_index("mp") * 8, 8), :])
    o_attn[...] = own[19:20, :]


def write_outputs(*parts):
    sd = jax.ShapeDtypeStruct
    shapes = [(32, 256)] * 4 + [(32, 1024)] * 2 + [(16, 32)] + [(1, 32)] * 3 + [(1, 8)]
    return pl.pallas_call(
        write_kernel,
        out_shape=tuple(sd(shape, F32) for shape in shapes),
        in_specs=[VMEM] * 7,
        out_specs=tuple([VMEM] * 11),
        name="write_outputs",
    )(*parts)


def per_device(
    initial_state,
    actions,
    next_state,
    reward_table,
    reward_scale,
    observe_table,
    gain_attn,
    w_query,
    w_key,
    w_value,
    w_out,
    gain_mlp,
    w_up,
    w_down,
    gain_final,
    actor_head,
    critic_head,
):
    token_total = actions.size * lax.axis_size("dp")

    def line(vector):
        return vector.reshape(1, -1)

    h_table, grad_down, grad_heads, final_terms, mlp_terms, res_a, res_b, state_sums, grad_out = policy(
        token_total,
        line(initial_state), actions.T, line(reward_scale), next_state.T, reward_table.T, observe_table,
        line(gain_attn), w_query, w_key, w_value, w_out, line(gain_mlp), line(gain_final),
        actor_head.T, line(critic_head), w_up, w_down,
    )
    parts = tail(
        state_sums.reshape(4, 4, 16, 768), res_a, res_b, grad_down, w_query, w_key, w_value, h_table,
        observe_table, grad_heads, final_terms, mlp_terms, grad_out,
    )
    q, k, v, out, up, down, actor, critic, final, mlp, attn = write_outputs(*parts)
    return (
        q, k, v, out.T, up, down.T, attn.reshape(-1), mlp.reshape(-1), final.reshape(-1), actor.T,
        critic.reshape(-1),
    )


def solution(mesh):
    return jax.shard_map(
        per_device,
        mesh=mesh,
        in_specs=(
            P("dp"),
            P("dp", None),
            P(),
            P(),
            P("dp"),
            P(),
            P(),
            P(None, "mp"),
            P(None, "mp"),
            P(None, "mp"),
            P("mp", None),
            P(),
            P(None, "mp"),
            P("mp", None),
            P(),
            P(),
            P(),
        ),
        out_specs=(
            P("dp", "mp"),
            P("dp", "mp"),
            P("dp", "mp"),
            P("mp", "dp"),
            P("dp", "mp"),
            P("mp", "dp"),
            P(("dp", "mp")),
            P("dp"),
            P("dp"),
            P("dp", None),
            P("dp"),
        ),
        check_vma=False,
    )
```

```python
import functools
import math

import jax
import jax.numpy as jnp
from jax import lax
from jax.experimental import pallas as pl
from jax.experimental.pallas import tpu as pltpu
from jax.sharding import PartitionSpec as P

HEAD_DIM = 128
STEPS = 16
EPS = 1e-05
GAMMA = 0.9
VALUE_COEF = 0.5
ENTROPY_COEF = 0.1
SCALE = 1.0 / math.sqrt(HEAD_DIM)
MESH = pl.DeviceIdType.MESH
VMEM = pl.BlockSpec(memory_space=pltpu.VMEM)
WIDE = 1024
ANY = pl.BlockSpec(memory_space=pl.ANY)
F32 = jnp.float32
BF16 = jnp.bfloat16


def place():
    d, m = lax.axis_index("dp"), lax.axis_index("mp")
    return d, m, m % 2, m // 2


def axes_place():
    d, m, c, l = place()
    return d // 8, (d // 2) % 4, d % 2


def partners():
    d, m, c, l = place()
    over = m + 2 - 4 * l
    return (d, m + 1 - 2 * c), (d, over), (d + 1 - 2 * (d % 2), over)


def at_x(k):
    d, m, c, l = place()
    x, z, yh = axes_place()
    return (lax.rem(x + k, 4) * 8 + z * 2 + yh, m)


def at_z(k):
    d, m, c, l = place()
    x, z, yh = axes_place()
    return (x * 8 + lax.rem(z + k, 4) * 2 + yh, m)


def stats_devices():
    d, m, c, l = place()
    x, z, yh = axes_place()
    plane, column = [], []
    for j in range(1, 16):
        other = lax.rem(x * 4 + z + j, 16)
        plane.append(((other // 4) * 8 + (other % 4) * 2 + yh, m))
    for j in range(1, 8):
        other = lax.rem(yh * 4 + m + j, 8)
        column.append((x * 8 + z * 2 + other // 4, other % 4))
    return plane, column


def greet(devices):
    barrier = pltpu.get_barrier_semaphore()
    for dev in devices:
        pl.semaphore_signal(barrier, inc=1, device_id=dev, device_id_type=MESH)
    pl.semaphore_wait(barrier, len(devices))


def remote(src, dst, sems, at, dev):
    cp = pltpu.make_async_remote_copy(
        src_ref=src, dst_ref=dst, send_sem=sems.at[(0, *at)], recv_sem=sems.at[(1, *at)],
        device_id=dev, device_id_type=MESH,
    )
    cp.start()
    return cp


def rows(start, size):
    return pl.ds(pl.multiple_of(start, size), size)


def by_blocks(total, block, body):
    lax.fori_loop(0, total // block, lambda i, z: (body(pl.multiple_of(i * block, block)), z)[1], 0)


def dot(left, right, contract, **kw):
    return lax.dot_general(
        left, right, ((contract[:1], contract[1:]), ((), ())), preferred_element_type=F32, **kw
    )


def iota(shape, axis):
    return lax.broadcasted_iota(jnp.int32, shape, axis)


def fold8(term):
    total = term[0:8]
    for k in range(1, term.shape[0] // 8):
        total = total + term[8 * k : 8 * k + 8]
    return total


def inverse_rms(x):
    return lax.rsqrt(jnp.mean(x * x, axis=-1, keepdims=True) + EPS)


def norm_back(x, inv, gain, up):
    weighted = up * gain
    return inv * weighted - x * (inv * inv * inv) * jnp.mean(x * weighted, axis=-1, keepdims=True)


def block_at(h, core, low):
    return h * 512 + core * 256 + low * 128


CHUNKS = [(h, k) for k in range(2) for h in range(2)]


class Sums:
    def __init__(self, p, near_own, near_far, far, sems):
        d, m, self.c, self.l = place()
        self.core, *self.over = partners()
        self.p, self.near_own, self.near_far, self.far = p, near_own, near_far, far
        self.own_sem, self.near_sem, self.far_sem = sems
        self.own, self.near, self.sent = {}, {}, {}

    def give_own(self):
        for h in range(2):
            src = self.p.at[rows(block_at(h, 1 - self.c, self.l), 128)]
            self.own[h] = remote(src, self.near_own.at[h], self.own_sem, (h,), self.core)

    def give_far(self, k):
        for h in range(2):
            src = self.p.at[rows(block_at(h, 1 - self.c, 1 - self.l) + k * 64, 64)]
            self.near[h, k] = remote(src, self.near_far.at[h, k], self.near_sem, (h, k), self.core)

    def pass_far(self, k):
        for h in range(2):
            self.near[h, k].wait_recv()
            base = block_at(h, self.c, 1 - self.l) + k * 64

            def body(i, h=h, base=base):
                self.near_far[h, k, pl.ds(i, 32), :] += self.p[rows(base + i, 32), :]

            by_blocks(64, 32, body)
            self.sent[h, k] = remote(
                self.near_far.at[h, k], self.far.at[h, k], self.far_sem, (h, k), self.over[h]
            )

    def take_own(self):
        for h in range(2):
            self.own[h].wait_recv()

    def take(self, h, k):
        self.sent[h, k].wait_recv()

    def value(self, h, k, i):
        mine = self.p[rows(block_at(h, self.c, self.l) + k * 64 + i, 32), :]
        return mine + self.near_own[h, pl.ds(k * 64 + i, 32), :] + self.far[h, k, pl.ds(i, 32), :]

    def drain(self):
        for group in (self.own, self.near, self.sent):
            for cp in group.values():
                cp.wait_send()


class Gather:
    def __init__(self, q, whole, low, sems):
        d, m, self.c, self.l = place()
        self.core, *self.over = partners()
        self.q, self.whole, self.low = q, whole, low
        self.over_sem, self.core_sem, self.fwd_sem = sems
        self.far, self.near, self.fwd, self.left = {}, {}, {}, set()

    def keep(self, base, src=None, at=0):
        def body(i):
            value = self.whole[rows(base + i, 32), :] if src is None else src[pl.ds(at + i, 32), :]
            self.low[rows(base + i, 32), :] = value.astype(BF16)

        by_blocks(64, 32, body)

    def send(self, h, k):
        base = block_at(h, self.c, self.l) + k * 64
        src, dst = self.q.at[pl.ds(h * 128 + k * 64, 64)], self.whole.at[rows(base, 64)]
        self.far[h, k] = remote(src, dst, self.over_sem, (h, k), self.over[h])
        self.near[h, k] = remote(src, dst, self.core_sem, (h, k), self.core)
        self.keep(base, self.q, h * 128 + k * 64)

    def take_core(self, h, k):
        self.near[h, k].wait_recv()
        self.keep(block_at(h, 1 - self.c, self.l) + k * 64)

    def take_far(self, h, k):
        self.far[h, k].wait_recv()
        base = block_at(h, self.c, 1 - self.l) + k * 64
        at = self.whole.at[rows(base, 64)]
        self.fwd[h, k] = remote(at, at, self.fwd_sem, (h, k), self.core)
        self.keep(base)

    def forwarded(self, k):
        for h in range(2):
            self.fwd[h, k].wait_send()
        self.left.add(k)

    def take_fwd(self, h, k):
        self.fwd[h, k].wait_recv()
        self.keep(block_at(h, 1 - self.c, 1 - self.l) + k * 64)

    def drain(self):
        late = [cp for (h, k), cp in self.fwd.items() if k not in self.left]
        for cp in [*self.far.values(), *self.near.values(), *late]:
            cp.wait_send()


SUM_SEMS = [
    pltpu.SemaphoreType.DMA((2, 2)), pltpu.SemaphoreType.DMA((2, 2, 2)), pltpu.SemaphoreType.DMA((2, 2, 2)),
]
GATHER_SEMS = [pltpu.SemaphoreType.DMA((2, 2, 2))] * 3


def gather_work_sum(gather, sums, work):
    c, l = sums.c, sums.l
    work([(block_at(h, c, l), 128) for h in range(2)])
    for h, k in CHUNKS:
        gather.take_core(h, k)
    work([(block_at(h, 1 - c, l), 128) for h in range(2)])
    sums.give_own()
    for k in range(2):
        for h in range(2):
            gather.take_far(h, k)
        work([(block_at(h, c, 1 - l) + k * 64, 64) for h in range(2)])
        for h in range(2):
            gather.take_fwd(h, k)
        work([(block_at(h, 1 - c, 1 - l) + k * 64, 64) for h in range(2)])
        sums.give_far(k)
        gather.forwarded(k)
        sums.pass_far(k)
    sums.take_own()


def spans_of(ref, spans, cols=slice(None)):
    return jnp.concatenate([ref[rows(at, n), cols] for at, n in spans], axis=0)


def put_spans(ref, spans, cols, value):
    done = 0
    for at, n in spans:
        ref[rows(at, n), cols] = value[done : done + n]
        done += n


def sum_everywhere(value, between, ps, cs, psem, csem):
    d, m, c, l = place()
    x, z, yh = axes_place()
    plane, column = stats_devices()

    def stage(slots, sems, devs, me, value, between=None):
        slots[me] = value
        copies = [remote(slots.at[me], slots.at[me], sems, (j,), dev) for j, dev in enumerate(devs)]
        done = between() if between is not None else None
        for cp in copies:
            cp.wait_recv()
        total = slots[0]
        for k in range(1, len(devs) + 1):
            total = total + slots[k]
        for cp in copies:
            cp.wait_send()
        return total, done

    value, done = stage(ps, psem, plane, x * 4 + z, value, between)
    return stage(cs, csem, column, yh * 4 + m, value)[0], done


STATS_SCRATCH = [
    pltpu.VMEM((16, 8, 128), F32),
    pltpu.VMEM((8, 8, 128), F32),
    pltpu.SemaphoreType.DMA((2, 15)),
    pltpu.SemaphoreType.DMA((2, 7)),
]


class Ring:
    def __init__(self, src, bufs, sems, pos, right, left):
        self.src, self.pos, self.right, self.left = src, pos, right, left
        self.mid, self.fl, self.fr = bufs
        self.sems = sems
        self.copies = []

    def send(self, src, dst, dev):
        self.copies.append(remote(src, dst, self.sems, (len(self.copies),), dev))

    def start(self):
        p = self.pos
        self.r, self.l, opp = lax.rem(p + 1, 4), lax.rem(p + 3, 4), lax.rem(p + 2, 4)
        self.send(self.src(opp, 0), self.mid.at[0], self.right)
        self.send(self.src(opp, 1), self.mid.at[1], self.left)
        self.send(self.src(self.r, 1), self.fl.at[1], self.right)
        self.send(self.src(self.l, 0), self.fr.at[0], self.left)

    def middle(self):
        self.copies[0].wait_recv()
        add_into(self.mid.at[0], self.src(self.r, 0))
        self.send(self.mid.at[0], self.fl.at[0], self.right)
        self.copies[1].wait_recv()
        add_into(self.mid.at[1], self.src(self.l, 1))
        self.send(self.mid.at[1], self.fr.at[1], self.left)

    def finish(self, out):
        for k in (2, 3, 4, 5):
            self.copies[k].wait_recv()
        for half in range(2):
            add_three(out(half), self.src(self.pos, half), self.fl.at[half], self.fr.at[half])

    def drain(self):
        for cp in self.copies:
            cp.wait_send()


def each_block(ref, body):
    n = min(16, ref.shape[-2])
    if len(ref.shape) == 3:
        for k in range(ref.shape[0]):
            by_blocks(ref.shape[1], n, lambda i, k=k: body((k, pl.ds(i, n), slice(None))))
    else:
        by_blocks(ref.shape[0], n, lambda i: body((pl.ds(i, n), slice(None))))


def add_into(dst, src):
    def body(at):
        dst[at] += src[at]

    each_block(dst, body)


def add_three(dst, a, b, c):
    def body(at):
        dst[at] = a[at] + b[at] + c[at]

    each_block(dst, body)


def ring_one(order, src, bufs, sems, cols=slice(None)):
    x, z, yh = axes_place()
    every = slice(None)
    if order == "xz":
        return Ring(lambda j, h: src.at[j, pl.ds(h * 2, 2), every, cols], bufs, sems, x, at_x(1), at_x(3))
    return Ring(lambda j, h: src.at[pl.ds(h * 2, 2), j, every, cols], bufs, sems, z, at_z(1), at_z(3))


def ring_two(order, res, bufs, sems):
    x, z, yh = axes_place()

    half = res.shape[1] // 2

    def src(j, h):
        return res.at[j, pl.ds(h * half, half)]

    if order == "xz":
        return Ring(src, bufs, sems, z, at_z(1), at_z(3))
    return Ring(src, bufs, sems, x, at_x(1), at_x(3))


def one_scratch(w, part=64):
    return [pltpu.VMEM((2, 2, part, w), F32)] * 3 + [pltpu.SemaphoreType.DMA((2, 6))]


def two_scratch(w, part=64, kept=32):
    return [
        *[pltpu.VMEM((2, part // 2, w), F32)] * 3,
        pltpu.VMEM((part, w), F32),
        pltpu.VMEM((kept, w), F32),
        pltpu.SemaphoreType.DMA((2, 6)),
        pltpu.SemaphoreType.DMA((2,)),
    ]


def params(n):
    return pltpu.CompilerParams(
        collective_id=n, has_side_effects=True, vmem_limit_bytes=63 * 1024 * 1024
    )


def block_probs(q, k):
    r, s = iota((128, 128), 0), iota((128, 128), 1)
    seen = ((r // STEPS) == (s // STEPS)) & (r >= s)
    weights = jnp.where(seen, jnp.exp(dot(q, k, (1, 1)) * SCALE), 0.0)
    return weights / jnp.sum(weights, axis=-1, keepdims=True)


def policy_kernel(
    token_total,
    init_ref, act_ref, scale_ref, next_ref, rew_ref, obs_ref, gain_attn, wq_ref, wk_ref, wv_ref, wo_ref,
    gain_mlp, gain_fin, actor_ref, critic_ref, up_hbm, down_hbm,
    ht_out, down_out, gh_ref, g_fin, g_mlp, res_a, res_b, state_sums, out_ref,
    low_one, qkv_ref, match_ref, mixed_ref, ht_ref, flush_sem,
    r_init, r_act, r_scale, roll_sem, tables, st_ref, own_ref, head_f, heads,
    w_up, w_down, w_sem,
    p, near_own, near_far, far, whole, h_two, up_rows, hidden, low_two, d_up, x_one, dx_two, buf_a, buf_b,
    fin_ref, grad_up, grad_down, *rest,
):
    stats, rest = rest[:4], rest[4:]
    sems_a, sems_b, sems_d = rest[0:3], rest[3:6], rest[6:9]
    gs_b, gs_d, gs_e = rest[9:12], rest[12:15], rest[15:18]
    ring_a, ring_b = rest[18:22], rest[22:26]
    flushed = []

    def flush(src, dst):
        cp = pltpu.make_async_copy(src, dst, flush_sem.at[len(flushed)])
        cp.start()
        flushed.append(cp)

    d, m, c, l = place()
    weights = [
        pltpu.make_async_copy(up_hbm, w_up, w_sem.at[0]), pltpu.make_async_copy(down_hbm, w_down, w_sem.at[1]),
    ]
    for cp in weights:
        cp.start()
    plane, column = stats_devices()
    greet(plane + column)
    far_dev = partners()[2]
    copies = [
        remote(src, dst, roll_sem, (n,), far_dev)
        for n, (src, dst) in enumerate(((init_ref, r_init), (act_ref, r_act), (scale_ref, r_scale)))
    ]

    def table_rows(i):
        at = pl.ds(i, 32)
        x = obs_ref[at, :].astype(F32)
        ht_ref[at, :] = (x * inverse_rms(x) * gain_attn[...]).astype(BF16)

    by_blocks(256, 32, table_rows)
    flush(ht_ref, ht_out)
    for n, w in enumerate((wq_ref, wk_ref, wv_ref)):
        tables[:, n * 256 : (n + 1) * 256] = dot(ht_ref[...], w[...], (1, 0)).astype(BF16)
    head_f[...] = jnp.zeros_like(head_f)
    head_f[0:16, :] = actor_ref[...].astype(F32)
    head_f[16:17, :] = critic_ref[...].astype(F32)
    heads[...] = jnp.zeros_like(heads)
    heads[0:32, :] = head_f[...].astype(BF16)

    for cp in copies:
        cp.wait()
    swap = 32 + 64 * l
    lane = iota((1, 64), 1)
    state = jnp.where(lane >= swap, r_init[...], init_ref[...]).astype(F32)
    scale = jnp.where(lane >= swap, r_scale[...], scale_ref[...])
    act_t = jnp.where(iota((16, 64), 1) >= swap, r_act[...], act_ref[...]).astype(F32)
    nexts = next_ref[...].astype(F32).astype(BF16)
    ids, kinds = iota((256, 64), 0).astype(F32), iota((16, 64), 0).astype(F32)
    for t in range(STEPS):
        st_ref[pl.ds(t, 1), :] = state
        if t + 1 < STEPS:
            hit = jnp.where(ids == state, 1.0, 0.0).astype(BF16)
            found = dot(nexts, hit, (1, 0))
            state = jnp.sum(jnp.where(kinds == act_t[t : t + 1, :], found, 0.0), axis=0, keepdims=True)

    pick_t = (iota((128, 16), 0) % STEPS == iota((128, 16), 1)).astype(BF16)
    spread = jnp.ones((64, 128), BF16)
    lanes = iota((128, 128), 1).astype(F32)

    def per_token(rows_by_env, first_env):
        here = iota((128, 64), 1) == first_env + iota((128, 64), 0) // STEPS
        found = jnp.where(here, dot(pick_t, rows_by_env, (1, 0)), 0.0)
        return dot(found.astype(BF16), spread, (1, 0))

    def attend(core, low):
        def block(h, carry):
            at = rows(block_at(h, core, low), 128)
            ids_here = per_token(st_ref[...].astype(BF16), h * 32 + (core * 2 + low) * 8)
            match = jnp.concatenate(
                [jnp.where(ids_here == lanes, 1.0, 0.0), jnp.where(ids_here == lanes + 128.0, 1.0, 0.0)], axis=1
            ).astype(BF16)
            match_ref[at, :] = match
            qkv = dot(match, tables[...], (1, 0)).astype(BF16)
            qkv_ref[at, :] = qkv
            outs = []
            for n in range(2):
                q, k, v = (qkv[:, j * 256 + n * 128 : j * 256 + (n + 1) * 128] for j in range(3))
                outs.append(dot(block_probs(q, k).astype(BF16), v, (1, 0)).astype(BF16))
            mixed = jnp.concatenate(outs, axis=1)
            mixed_ref[at, :] = mixed
            p[at, :] = dot(mixed, wo_ref[...], (1, 0))
            return carry

        lax.fori_loop(0, 2, block, 0, unroll=True)

    sums = Sums(p, near_own, near_far, far, sems_a)
    attend(1 - c, 1 - l)
    sums.give_far(0)
    sums.give_far(1)
    attend(c, 1 - l)
    sums.pass_far(0)
    sums.pass_far(1)
    attend(1 - c, l)
    sums.give_own()
    attend(c, l)
    for h in range(2):
        at = pl.ds(h * 128, 128)
        mine = match_ref[rows(block_at(h, c, l), 128), :]
        x_one[at, :] = dot(mine, obs_ref[...], (1, 0))
        first_env = h * 32 + (c * 2 + l) * 8
        chosen = jnp.where(per_token(act_t.astype(BF16), first_env) == lanes, 1.0, 0.0)
        found = dot(mine.astype(F32), rew_ref[...], (1, 1), precision=lax.Precision.HIGHEST)
        here = iota((128, 64), 1) == first_env + iota((128, 64), 0) // STEPS
        factor = jnp.sum(jnp.where(here, scale, 0.0), axis=1, keepdims=True)
        reward = jnp.sum(chosen[:, :16] * found, axis=1, keepdims=True) * factor
        own_ref[at, :] = jnp.where(lanes == 16.0, reward, chosen)
    sums.take_own()

    gather = Gather(buf_a, whole, h_two, gs_b)
    for h, k in CHUNKS:
        sums.take(h, k)

        def body(i, h=h, k=k):
            at = pl.ds(h * 128 + k * 64 + i, 32)
            x = sums.value(h, k, i) + x_one[at, :]
            x_one[at, :] = x
            buf_a[at, :] = x * inverse_rms(x) * gain_mlp[...]

        by_blocks(64, 32, body)
        gather.send(h, k)
    sums.drain()
    for cp in weights:
        cp.wait()

    def forward(spans):
        def up(j):
            cols = pl.ds(j, WIDE)
            u = dot(spans_of(h_two, spans), w_up[:, cols], (1, 0))
            put_spans(up_rows, spans, cols, u)
            put_spans(hidden, spans, cols, (u / (1.0 + jnp.exp(-u))).astype(BF16))

        def down(j):
            cols = pl.ds(j, WIDE)
            put_spans(p, spans, cols, dot(spans_of(hidden, spans), w_down[:, cols], (1, 0)))

        by_blocks(1024, WIDE, up)
        by_blocks(1024, WIDE, down)

    sums = Sums(p, near_own, near_far, far, sems_b)
    gather_work_sum(gather, sums, forward)
    for h, k in CHUNKS:
        sums.take(h, k)

        def body(i, h=h, k=k):
            at = pl.ds(h * 128 + k * 64 + i, 32)
            x = sums.value(h, k, i) + x_one[at, :]
            buf_b[at, :] = x
            fin_ref[at, :] = (x * inverse_rms(x) * gain_fin[...]).astype(BF16)

        by_blocks(64, 32, body)
    gather.drain()
    sums.drain()

    lane = iota((256, 128), 1)
    both = dot(fin_ref[...], heads[...], (1, 1))
    critic = jnp.sum(jnp.where(lane == 16, both, 0.0), axis=1, keepdims=True)
    own = own_ref[...]
    reward = jnp.sum(jnp.where(lane == 16, own, 0.0), axis=1, keepdims=True)
    step = iota((256, 128), 0) % STEPS
    base = reward + jnp.where(step == STEPS - 1, GAMMA * critic, 0.0)
    r, s = iota((256, 256), 0), iota((256, 256), 1)
    ahead = ((r // STEPS) == (s // STEPS)) & (s >= r)
    decay = jnp.where(ahead, jnp.exp((s - r).astype(F32) * math.log(GAMMA)), 0.0)
    returns = dot(decay, base, (1, 0), precision=lax.Precision.HIGHEST)
    advantage = returns - critic
    tile = jnp.where(
        iota((8, 128), 0) == 0,
        jnp.sum(advantage, axis=0, keepdims=True),
        jnp.sum(advantage * advantage, axis=0, keepdims=True),
    )
    real = lane < 16
    factor = 1.0 / math.sqrt(token_total)

    def policy_terms():
        logits = jnp.where(real, both, 0.0)
        mass = jnp.sum(jnp.where(real, jnp.exp(logits), 0.0), axis=1, keepdims=True)
        logp = jnp.where(real, logits - jnp.log(mass), 0.0)
        chance = jnp.where(real, jnp.exp(logp), 0.0)
        entropy = -jnp.sum(chance * logp, axis=1, keepdims=True)
        picked = jnp.where(real, own, 0.0)
        d_value = (factor * VALUE_COEF) * (critic - returns)
        return picked - chance, ENTROPY_COEF * chance * (logp + entropy), d_value

    totals, (push, calm, d_value) = sum_everywhere(tile, policy_terms, *stats)
    mean = totals[0:1, :] * (1.0 / token_total)
    variance = totals[1:2, :] * (1.0 / token_total) - mean * mean
    normed = (advantage - mean) * lax.rsqrt(variance + EPS)
    d_logits = factor * (-normed * push + calm)
    d_both = jnp.where(real, d_logits, jnp.where(lane == 16, d_value, 0.0)).astype(BF16)
    buf_a[...] = dot(d_both, heads[...], (1, 0))
    g_fin[...] = jnp.zeros_like(g_fin)
    g_mlp[...] = jnp.zeros_like(g_mlp)

    gather = Gather(dx_two, whole, low_two, gs_d)
    for h, k in CHUNKS:

        def body(i, h=h, k=k):
            at = pl.ds(h * 128 + k * 64 + i, 32)
            x, up = buf_b[at, :], buf_a[at, :]
            inv = inverse_rms(x)
            dx_two[at, :] = norm_back(x, inv, gain_fin[...], up)
            g_fin[...] += fold8(up * x * inv)

        by_blocks(64, 32, body)
        gather.send(h, k)
    gh_ref[...] = dot(fin_ref[...], d_both, (0, 0))

    def backward(spans):
        def up(j):
            cols = pl.ds(j, WIDE)
            d_hidden = dot(spans_of(low_two, spans), w_down[cols, :], (1, 1)).astype(BF16).astype(F32)
            u = spans_of(up_rows, spans, cols)
            sig = 1.0 / (1.0 + jnp.exp(-u))
            put_spans(d_up, spans, cols, (d_hidden * sig * (1.0 + u * (1.0 - sig))).astype(BF16))

        def down(j):
            cols = pl.ds(j, WIDE)
            put_spans(p, spans, cols, dot(spans_of(d_up, spans), w_up[cols, :], (1, 1)))

        by_blocks(1024, WIDE, up)
        by_blocks(1024, WIDE, down)

    sums = Sums(p, near_own, near_far, far, sems_d)
    gather_work_sum(gather, sums, backward)

    def weight_grad(out, left, right):
        def tile(j, carry):
            cols = rows(j * 256, 256)
            out[j] = dot(left[:, cols], right[...], (0, 0)).reshape(4, 64, 1024)
            return carry

        lax.fori_loop(0, 4, tile, 0)

    rings = [
        ring_one("xz", grad_up, ring_a[:3], ring_a[3], pl.ds(0, 512)),
        ring_one("zx", grad_up, ring_b[:3], ring_b[3], pl.ds(512, 512)),
    ]
    weight_grad(grad_up, h_two, d_up)
    for ring in rings:
        ring.start()
    weight_grad(grad_down, low_two, hidden)
    flush(grad_down, down_out)
    gather.drain()

    def attend_back(spans):
        d_mixed = dot(spans_of(low_one, spans), wo_ref[...], (1, 1)).astype(BF16)
        qkv = spans_of(qkv_ref, spans)
        parts = [[], [], []]
        for n in range(2):
            q, k, v = (qkv[:, j * 256 + n * 128 : j * 256 + (n + 1) * 128] for j in range(3))
            up = d_mixed[:, n * 128 : (n + 1) * 128]
            probs = block_probs(q, k)
            d_probs = dot(up, v, (1, 1))
            parts[2].append(dot(probs.astype(BF16), up, (0, 0)).astype(BF16))
            d_scores = (
                probs * (d_probs - jnp.sum(probs * d_probs, axis=-1, keepdims=True)) * SCALE
            ).astype(BF16)
            parts[0].append(dot(d_scores, k, (1, 0)).astype(BF16))
            parts[1].append(dot(d_scores, q, (0, 0)).astype(BF16))
        d_qkv = jnp.concatenate([*parts[0], *parts[1], *parts[2]], axis=1)
        state_sums[...] += dot(spans_of(match_ref, spans), d_qkv, (0, 0))

    state_sums[...] = jnp.zeros_like(state_sums)
    gather = Gather(buf_b, whole, low_one, gs_e)
    for h, k in CHUNKS:
        sums.take(h, k)

        def body(i, h=h, k=k):
            at = pl.ds(h * 128 + k * 64 + i, 32)
            up, x = sums.value(h, k, i), x_one[at, :]
            inv = inverse_rms(x)
            buf_b[at, :] = dx_two[at, :] + norm_back(x, inv, gain_mlp[...], up)
            g_mlp[...] += fold8(up * x * inv)

        by_blocks(64, 32, body)
        gather.send(h, k)
    sums.drain()
    for h in range(2):
        attend_back([(block_at(h, c, l), 128)])
    for h, k in CHUNKS:
        gather.take_core(h, k)
    for h in range(2):
        gather.take_far(h, 0)
    for ring in rings:
        ring.middle()
    for h in range(2):
        attend_back([(block_at(h, 1 - c, l), 128)])
    for h in range(2):
        gather.take_fwd(h, 0)
    attend_back([(block_at(h, c, 1 - l), 64) for h in range(2)])
    attend_back([(block_at(h, 1 - c, 1 - l), 64) for h in range(2)])
    for h in range(2):
        gather.take_far(h, 1)
    attend_back([(block_at(h, c, 1 - l) + 64, 64) for h in range(2)])
    for h in range(2):
        gather.take_fwd(h, 1)
    attend_back([(block_at(h, 1 - c, 1 - l) + 64, 64) for h in range(2)])
    gather.drain()

    def out_tile(j, carry):
        cols = rows(j * 256, 256)
        out_ref[j] = dot(low_one[:, cols], mixed_ref[...], (0, 0)).reshape(4, 64, 256)
        return carry

    lax.fori_loop(0, 4, out_tile, 0)
    for ring, res in zip(rings, (res_a, res_b)):
        ring.finish(lambda h, res=res: res.at[pl.ds(h * 2, 2)])
    for ring in rings:
        ring.drain()
    for cp in flushed:
        cp.wait()


def policy(token_total, *args):
    sd, vm = jax.ShapeDtypeStruct, pltpu.VMEM
    return pl.pallas_call(
        functools.partial(policy_kernel, token_total),
        out_shape=(
            sd((256, 1024), BF16), sd((4, 4, 64, 1024), F32), sd((1024, 128), F32), sd((8, 1024), F32),
            sd((8, 1024), F32), sd((4, 64, 512), F32), sd((4, 64, 512), F32), sd((256, 768), F32),
            sd((4, 4, 64, 256), F32),
        ),
        in_specs=[VMEM] * 15 + [ANY] * 2,
        out_specs=tuple([ANY] * 2 + [VMEM] * 7),
        scratch_shapes=[
            vm((1024, 1024), BF16), vm((1024, 768), BF16), vm((1024, 256), BF16), vm((1024, 256), BF16), vm((256, 1024), BF16),
            pltpu.SemaphoreType.DMA((2,)),
            vm((1, 64), jnp.int32), vm((16, 64), jnp.int32), vm((1, 64), F32), pltpu.SemaphoreType.DMA((2, 3)),
            vm((256, 768), BF16), vm((16, 64), F32), vm((256, 128), F32), vm((32, 1024), F32), vm((128, 1024), BF16),
            vm((1024, 1024), BF16), vm((1024, 1024), BF16), pltpu.SemaphoreType.DMA((2,)),
            vm((1024, 1024), F32), vm((2, 128, 1024), F32), vm((2, 2, 64, 1024), F32), vm((2, 2, 64, 1024), F32),
            vm((1024, 1024), F32), vm((1024, 1024), BF16), vm((1024, 1024), F32), vm((1024, 1024), BF16),
            vm((1024, 1024), BF16), vm((1024, 1024), BF16),
            vm((256, 1024), F32), vm((256, 1024), F32), vm((256, 1024), F32), vm((256, 1024), F32),
            vm((256, 1024), BF16), vm((4, 4, 64, 1024), F32), vm((4, 4, 64, 1024), F32),
            *STATS_SCRATCH, *SUM_SEMS, *SUM_SEMS, *SUM_SEMS, *GATHER_SEMS, *GATHER_SEMS, *GATHER_SEMS,
            *one_scratch(512), *one_scratch(512),
        ],
        compiler_params=params(1),
        name="policy",
    )(*args)


def halves(value):
    high = value.astype(BF16)
    return high, (value - high.astype(F32)).astype(BF16)


UP_A, UP_B, DOWN_A, DOWN_B, OUT, SMALL, SUM_A, SUM_B = range(8)
ORDER = ("xz", "zx", "xz", "zx", "zx", "xz", "xz", "zx")
WIDTH = (512, 512, 512, 512, 256, 128, 384, 384)
PART = (64, 64, 64, 64, 64, 64, 16, 16)
LOADS = (
    ((4, 4, 16, 768), F32), ((4, 64, 512), F32), ((4, 64, 512), F32), ((4, 4, 64, 1024), F32),
    ((1024, 256), BF16), ((1024, 256), BF16), ((1024, 256), BF16), ((256, 1024), BF16), ((256, 1024), BF16),
    ((1024, 128), F32), ((8, 1024), F32), ((8, 1024), F32), ((4, 4, 64, 256), F32),
)


def tail_kernel(*refs):
    n = len(LOADS)
    hbm, outs, held, rest = refs[:n], refs[n : n + 7], refs[n + 7 : 2 * n + 7], refs[2 * n + 7 :]
    load_sem, full_a, full_b, near_sem, far_sem, mine_ref, dt_ref, vec_ref, small4, mp_buf, mp_sem = rest[:11]
    rest = rest[11:]
    sums4, res_a, res_b, down_ref, wq_ref, wk_ref, wv_ref, ht_ref, obs_ref, small_ref, gf_ref, gm_ref, out_ref = held
    loads = [pltpu.make_async_copy(a, b, load_sem.at[k]) for k, (a, b) in enumerate(zip(hbm, held))]
    for cp in loads:
        cp.start()
    d, m, c, l = place()
    x, z, yh = axes_place()
    yother = (d + 1 - 2 * yh, m)
    peers = [(d, lax.rem(m + j, 4)) for j in (1, 2, 3)]
    greet([at_x(1), at_x(3), at_z(1), at_z(3), yother] + peers)

    first, second, results, ends = {}, [], [res_a, res_b], []
    sources = {
        DOWN_A: (down_ref, pl.ds(0, 512)), DOWN_B: (down_ref, pl.ds(512, 512)), OUT: (out_ref, slice(None)),
        SMALL: (small4, slice(None)), SUM_A: (sums4, pl.ds(0, 384)), SUM_B: (sums4, pl.ds(384, 384)),
    }
    for i in range(2, 8):
        mid, fl, fr, sems, res = rest[:5]
        rest = rest[5:]
        src, cols = sources[i]
        first[i] = ring_one(ORDER[i], src, (mid, fl, fr), sems, cols)
        results.append(res)
    for i in range(8):
        mid, fl, fr, res, ybuf, sems, ysem = rest[:7]
        rest = rest[7:]
        second.append(ring_two(ORDER[i], results[i], (mid, fl, fr), sems))
        ends.append((res, ybuf, ysem))
    tails = {}

    def turn(i):
        first[i].finish(lambda h: results[i].at[pl.ds(h * 2, 2)])
        second[i].start()

    def send_tail(i):
        res, ybuf, ysem = ends[i]
        half = res.shape[0] // 2
        second[i].finish(lambda h: res.at[pl.ds(h * half, half)])
        src = res if i in (SUM_A, SUM_B) else res.at[rows((1 - yh) * 32, 32)]
        tails[i] = remote(src, ybuf, ysem, (), yother)

    loads[0].wait()
    first[SUM_A].start()
    first[SUM_B].start()
    loads[1].wait()
    loads[2].wait()
    second[UP_A].start()
    second[UP_B].start()
    for cp in loads[3:]:
        cp.wait()
    high, low = halves(sums4[...].reshape(256, 768))
    dt_ref[...] = jnp.zeros_like(dt_ref)
    for n, w in enumerate((wq_ref, wk_ref, wv_ref)):
        cols = slice(n * 256, (n + 1) * 256)
        dt_ref[...] += dot(high[:, cols], w[...], (1, 1)) + dot(low[:, cols], w[...], (1, 1))
    vec_ref[0:8] = gf_ref[...]
    vec_ref[8:16] = gm_ref[...]
    vec_ref[16:32] = jnp.zeros((16, 1024), F32)

    def gain_rows(i):
        at = pl.ds(i, 32)
        x = obs_ref[at, :].astype(F32)
        vec_ref[16:24] += fold8(dt_ref[at, :] * x * inverse_rms(x))

    by_blocks(256, 32, gain_rows)
    place_at = (iota((32, 128), 1) == 17 + iota((32, 128), 0) // 8).astype(BF16)
    vec = vec_ref[...]
    high, low = halves(vec)
    lowest = (vec - high.astype(F32) - low.astype(F32)).astype(BF16)
    small = small_ref[...] + sum(dot(part, place_at, (0, 0)) for part in (high, low, lowest))
    small4[...] = small.reshape(4, 4, 64, 128)
    for i in (SUM_A, SUM_B):
        first[i].middle()
    for i in (UP_A, UP_B):
        second[i].middle()
    for i in (DOWN_A, DOWN_B, OUT, SMALL):
        first[i].start()
    for i in (SUM_A, SUM_B):
        turn(i)
    for i in (UP_A, UP_B):
        send_tail(i)
    for i in (DOWN_A, DOWN_B, OUT, SMALL):
        first[i].middle()
    for i in (SUM_A, SUM_B):
        second[i].middle()
    for i in (DOWN_A, DOWN_B):
        turn(i)
    for i in (SUM_A, SUM_B):
        send_tail(i)
    for i in (DOWN_A, DOWN_B):
        second[i].middle()
    for i in (SMALL, OUT):
        turn(i)
    for i in (SUM_A, SUM_B):
        tails[i].wait_recv()
    full_a[x, z] = ends[SUM_A][0][...] + ends[SUM_A][1][...]
    full_b[x, z] = ends[SUM_B][0][...] + ends[SUM_B][1][...]
    near = [remote(full_a.at[x, z], full_a.at[x, z], near_sem, (0, j - 1), at_z(j)) for j in (1, 2, 3)]
    near += [remote(full_b.at[x, z], full_b.at[x, z], near_sem, (1, j - 1), at_x(j)) for j in (1, 2, 3)]
    for i in (DOWN_A, DOWN_B):
        send_tail(i)
    for cp in near:
        cp.wait_recv()
    wide = [remote(full_a.at[x], full_a.at[x], far_sem, (0, j - 1), at_x(j)) for j in (1, 2, 3)]
    wide += [remote(full_b.at[:, z], full_b.at[:, z], far_sem, (1, j - 1), at_z(j)) for j in (1, 2, 3)]
    for i in (SMALL, OUT):
        second[i].middle()
    for i in (SMALL, OUT):
        send_tail(i)

    def total(i, put):
        res, ybuf, _ = ends[i]
        by_blocks(32, 8, lambda k: put(k, res[rows(yh * 32 + k, 8), :] + ybuf[pl.ds(k, 8), :]))

    def to_out(ref):
        def put(k, value):
            ref[pl.ds(k, 8), :] = value

        return put

    def to_mp(k, value):
        mp_buf[m, pl.ds(k, 8), :] = value

    shares = []
    for i in (UP_A, UP_B, DOWN_A, DOWN_B, SMALL, OUT):
        tails[i].wait_recv()
        if i == SMALL:
            total(i, to_mp)
            shares = [remote(mp_buf.at[m], mp_buf.at[m], mp_sem, (j,), dev) for j, dev in enumerate(peers)]
        else:
            total(i, to_out(outs[i]))
    for cp in wide:
        cp.wait_recv()
    table = ht_ref[:, rows((d // 4) * 128, 128)]
    for n, ref in enumerate((full_a, full_b)):
        high, low = halves(ref[...].reshape(256, 384))
        mine_ref[:, n * 384 : (n + 1) * 384] = dot(table, high, (0, 0)) + dot(table, low, (0, 0))
    outs[6][...] = mine_ref[rows((d % 4) * 32, 32), :]
    for cp in shares:
        cp.wait_recv()
    outs[SMALL][...] = mp_buf[0] + mp_buf[1] + mp_buf[2] + mp_buf[3]
    for cp in [*shares, *tails.values(), *near, *wide]:
        cp.wait_send()
    for ring in [*first.values(), *second]:
        ring.drain()


def tail(*args):
    vm, dma = pltpu.VMEM, pltpu.SemaphoreType.DMA
    scratch = [vm(shape, kind) for shape, kind in LOADS]
    scratch += [
        dma((len(LOADS),)), vm((4, 4, 16, 384), F32), vm((4, 4, 16, 384), F32), dma((2, 2, 3)), dma((2, 2, 3)), vm((128, 768), F32),
        vm((256, 1024), F32), vm((32, 1024), F32), vm((4, 4, 64, 128), F32), vm((4, 32, 128), F32), dma((2, 3)),
    ]
    for i in range(2, 8):
        scratch += one_scratch(WIDTH[i], PART[i]) + [vm((4, PART[i], WIDTH[i]), F32)]
    for i in range(8):
        scratch += two_scratch(WIDTH[i], PART[i], 16 if i in (SUM_A, SUM_B) else 32)
    return pl.pallas_call(
        tail_kernel,
        out_shape=tuple(jax.ShapeDtypeStruct((32, w), F32) for w in (*WIDTH[:6], 768)),
        in_specs=[ANY] * len(LOADS),
        out_specs=tuple([VMEM] * 7),
        scratch_shapes=scratch,
        compiler_params=params(2),
        name="tail",
    )(*args)


def write_kernel(
    up_a, up_b, down_a, down_b, out_ref, small_ref, qkv_ref,
    o_q, o_k, o_v, o_out, o_up, o_down, o_actor, o_critic, o_final, o_mlp, o_attn,
):
    o_q[...] = qkv_ref[:, :256]
    o_k[...] = qkv_ref[:, 256:512]
    o_v[...] = qkv_ref[:, 512:]
    o_up[:, :512] = up_a[...]
    o_up[:, 512:] = up_b[...]
    o_out[...] = out_ref[...]
    o_down[:, :512] = down_a[...]
    o_down[:, 512:] = down_b[...]
    flat = jnp.transpose(small_ref[...])
    o_actor[...] = flat[:16, :]
    o_critic[...] = flat[16:17, :]
    o_final[...] = flat[17:18, :]
    o_mlp[...] = flat[18:19, :]
    own = jnp.transpose(small_ref[rows(lax.axis_index("mp") * 8, 8), :])
    o_attn[...] = own[19:20, :]


def write_outputs(*parts):
    sd = jax.ShapeDtypeStruct
    shapes = [(32, 256)] * 4 + [(32, 1024)] * 2 + [(16, 32)] + [(1, 32)] * 3 + [(1, 8)]
    return pl.pallas_call(
        write_kernel,
        out_shape=tuple(sd(shape, F32) for shape in shapes),
        in_specs=[VMEM] * 7,
        out_specs=tuple([VMEM] * 11),
        name="write_outputs",
    )(*parts)


def per_device(
    initial_state,
    actions,
    next_state,
    reward_table,
    reward_scale,
    observe_table,
    gain_attn,
    w_query,
    w_key,
    w_value,
    w_out,
    gain_mlp,
    w_up,
    w_down,
    gain_final,
    actor_head,
    critic_head,
):
    token_total = actions.size * lax.axis_size("dp")

    def line(vector):
        return vector.reshape(1, -1)

    h_table, grad_down, grad_heads, final_terms, mlp_terms, res_a, res_b, state_sums, grad_out = policy(
        token_total,
        line(initial_state), actions.T, line(reward_scale), next_state.T, reward_table.T, observe_table,
        line(gain_attn), w_query, w_key, w_value, w_out, line(gain_mlp), line(gain_final),
        actor_head.T, line(critic_head), w_up, w_down,
    )
    parts = tail(
        state_sums.reshape(4, 4, 16, 768), res_a, res_b, grad_down, w_query, w_key, w_value, h_table,
        observe_table, grad_heads, final_terms, mlp_terms, grad_out,
    )
    q, k, v, out, up, down, actor, critic, final, mlp, attn = write_outputs(*parts)
    return (
        q, k, v, out.T, up, down.T, attn.reshape(-1), mlp.reshape(-1), final.reshape(-1), actor.T,
        critic.reshape(-1),
    )


def solution(mesh):
    return jax.shard_map(
        per_device,
        mesh=mesh,
        in_specs=(
            P("dp"),
            P("dp", None),
            P(),
            P(),
            P("dp"),
            P(),
            P(),
            P(None, "mp"),
            P(None, "mp"),
            P(None, "mp"),
            P("mp", None),
            P(),
            P(None, "mp"),
            P("mp", None),
            P(),
            P(),
            P(),
        ),
        out_specs=(
            P("dp", "mp"),
            P("dp", "mp"),
            P("dp", "mp"),
            P("mp", "dp"),
            P("dp", "mp"),
            P("mp", "dp"),
            P(("dp", "mp")),
            P("dp"),
            P("dp"),
            P("dp", None),
            P("dp"),
        ),
        check_vma=False,
    )
```
